128 devices in a mesh: dp: 1, ty: 16 (over z, y), tx: 8 (over x, core).
Axes of the slice: x: 4, y: 4, z: 4, core: 2. Of those that a mesh axis runs over, the one named last changes fastest.
Arguments:
- x_in: bfloat16 [3072, 6144], P('dp', 'tx')
- seq_lens: int32 [3072], P('dp')
- k_cache: bfloat16 [3072, 128, 128], P(('dp', 'ty', 'tx'))
- v_cache: bfloat16 [3072, 128, 128], P(('dp', 'ty', 'tx'))
- ln_gamma: float32 [6144], P('tx')
- w_query: bfloat16 [6144, 6144], P('tx', 'ty')
- w_key: bfloat16 [6144, 128], P('tx')
- w_value: bfloat16 [6144, 128], P('tx')
- w_gate: bfloat16 [6144, 24576], P('tx', 'ty')
- w_up: bfloat16 [6144, 24576], P('tx', 'ty')
- w_out: bfloat16 [6144, 6144], P('ty', 'tx')
- w_down: bfloat16 [24576, 6144], P('ty', 'tx')
Outputs:
- output 1: bfloat16 [3072, 6144], P('dp', 'tx')
- output 2: bfloat16 [3072, 128, 128], P(('dp', 'ty', 'tx'))
- output 3: bfloat16 [3072, 128, 128], P(('dp', 'ty', 'tx'))
All inputs are finite; a program needn't handle non-finite values.
Results may differ from the reference program's by a relative error of at most 0.0177021.
Values are sent between devices in bfloat16 or wider.
A program may use at most 1 GiB of HBM per device.

```python
import jax
import jax.numpy as jnp
from jax import lax

D_MODEL = 6144
NUM_HEADS = 48
HEAD_DIM = 128
FFN_DIM = 24576
BATCH = 3072
SEQ_BLOCK = 24
CTX_LEN = 128

EPSILON = 1e-6
ROPE_BASE = 10000.0


def setup_inputs(seed: int = 0, part: int = 0) -> dict:
    part_keys = jax.random.split(jax.random.fold_in(jax.random.key(seed), part), 6)
    shared_keys = jax.random.split(jax.random.key(seed + 1), 8)
    x_in = jax.random.normal(part_keys[0], (BATCH, D_MODEL), jnp.float32).astype(jnp.bfloat16)
    block_caps = jax.random.randint(part_keys[1], (BATCH // SEQ_BLOCK,), 1, CTX_LEN + 1)
    raw_lens = jax.random.randint(part_keys[2], (BATCH,), 0, jnp.repeat(block_caps, SEQ_BLOCK))
    pick_order = jax.random.permutation(part_keys[3], BATCH)
    seq_lens = raw_lens.at[pick_order[0]].set(CTX_LEN - 1).at[pick_order[1]].set(0).astype(jnp.int32)
    k_cache = jax.random.normal(part_keys[4], (BATCH, CTX_LEN, HEAD_DIM), jnp.float32).astype(jnp.bfloat16)
    v_cache = jax.random.normal(part_keys[5], (BATCH, CTX_LEN, HEAD_DIM), jnp.float32).astype(jnp.bfloat16)
    ln_gamma = 1.0 + 0.4 * jax.random.normal(shared_keys[0], (D_MODEL,), jnp.float32)
    w_query = (jax.random.normal(shared_keys[1], (D_MODEL, NUM_HEADS * HEAD_DIM), jnp.float32) * (2.0 * D_MODEL ** -0.5)).astype(jnp.bfloat16)
    w_key = (jax.random.normal(shared_keys[2], (D_MODEL, HEAD_DIM), jnp.float32) * D_MODEL ** -0.5).astype(jnp.bfloat16)
    w_value = (jax.random.normal(shared_keys[3], (D_MODEL, HEAD_DIM), jnp.float32) * D_MODEL ** -0.5).astype(jnp.bfloat16)
    w_gate = (jax.random.normal(shared_keys[4], (D_MODEL, FFN_DIM), jnp.float32) * D_MODEL ** -0.5).astype(jnp.bfloat16)
    w_up = (jax.random.normal(shared_keys[5], (D_MODEL, FFN_DIM), jnp.float32) * D_MODEL ** -0.5).astype(jnp.bfloat16)
    w_out = (jax.random.normal(shared_keys[6], (NUM_HEADS * HEAD_DIM, D_MODEL), jnp.float32) * (NUM_HEADS * HEAD_DIM) ** -0.5).astype(jnp.bfloat16)
    w_down = (jax.random.normal(shared_keys[7], (FFN_DIM, D_MODEL), jnp.float32) * FFN_DIM ** -0.5).astype(jnp.bfloat16)
    return {"x_in": x_in, "seq_lens": seq_lens, "k_cache": k_cache, "v_cache": v_cache, "ln_gamma": ln_gamma, "w_query": w_query, "w_key": w_key, "w_value": w_value, "w_gate": w_gate, "w_up": w_up, "w_out": w_out, "w_down": w_down}


def rope_tables(positions, head_dim):
    half_dim = head_dim // 2
    inv_freqs = ROPE_BASE ** (-(jnp.arange(half_dim, dtype=jnp.float32) * 2.0) / head_dim)
    angles = positions.astype(jnp.float32)[:, None] * inv_freqs[None, :]
    return jnp.cos(angles), jnp.sin(angles)


def rope_apply(vals, cosines, sines):
    half_dim = vals.shape[-1] // 2
    first = vals[..., :half_dim]
    second = vals[..., half_dim:]
    return jnp.concatenate([first * cosines - second * sines, second * cosines + first * sines], axis=-1)


def reference(x_in, seq_lens, k_cache, v_cache, ln_gamma, w_query, w_key, w_value, w_gate, w_up, w_out, w_down):
    x_f32 = x_in.astype(jnp.float32)
    row_mean = jnp.sum(x_f32, axis=-1) / D_MODEL
    row_var = jnp.sum(x_f32 * x_f32, axis=-1) / D_MODEL - row_mean * row_mean
    normed = ((x_f32 - row_mean[:, None]) * lax.rsqrt(row_var[:, None] + EPSILON) * ln_gamma[None, :]).astype(jnp.bfloat16)
    q_proj = jnp.dot(normed, w_query, preferred_element_type=jnp.float32).reshape(BATCH, NUM_HEADS, HEAD_DIM)
    k_proj = jnp.dot(normed, w_key, preferred_element_type=jnp.float32)
    v_new = jnp.dot(normed, w_value, preferred_element_type=jnp.float32).astype(jnp.bfloat16)
    gate = jnp.dot(normed, w_gate, preferred_element_type=jnp.float32).astype(jnp.bfloat16)
    up_proj = jnp.dot(normed, w_up, preferred_element_type=jnp.float32).astype(jnp.bfloat16)
    cosines, sines = rope_tables(seq_lens, HEAD_DIM)
    queries = rope_apply(q_proj, cosines[:, None, :], sines[:, None, :]).astype(jnp.bfloat16)
    k_new = rope_apply(k_proj, cosines, sines).astype(jnp.bfloat16)
    positions = jnp.arange(CTX_LEN)
    at_slot = positions[None, :, None] == seq_lens[:, None, None]
    k_out = jnp.where(at_slot, k_new[:, None, :], k_cache)
    v_out = jnp.where(at_slot, v_new[:, None, :], v_cache)

    def one_sequence(item):
        q_row, k_rows, v_rows, length = item
        scores = jnp.dot(q_row, k_rows.T, preferred_element_type=jnp.float32) * (HEAD_DIM ** -0.5)
        in_range = positions[None, :] <= length
        scores = jnp.where(in_range, scores, -1e30)
        att_probs = jax.nn.softmax(scores, axis=-1).astype(jnp.bfloat16)
        return jnp.dot(att_probs, v_rows, preferred_element_type=jnp.float32).astype(jnp.bfloat16)

    att_heads = lax.map(one_sequence, (queries, k_out, v_out, seq_lens))
    mlp_act = (jax.nn.silu(gate.astype(jnp.float32)) * up_proj.astype(jnp.float32)).astype(jnp.bfloat16)
    attn_part = jnp.dot(att_heads.reshape(BATCH, NUM_HEADS * HEAD_DIM), w_out, preferred_element_type=jnp.float32)
    mlp_part = jnp.dot(mlp_act, w_down, preferred_element_type=jnp.float32)
    y_out = (x_f32 + attn_part + mlp_part).astype(jnp.bfloat16)
    return (y_out, k_out, v_out)
```

```python
import functools

import jax
import jax.numpy as jnp
from jax import lax
from jax.experimental import pallas as pl
from jax.experimental.pallas import tpu as pltpu
from jax.sharding import PartitionSpec as P

EPSILON = 1e-6
ROPE_BASE = 10000.0
MESH = pl.DeviceIdType.MESH
RING = 4
F32 = jnp.float32
BF16 = jnp.bfloat16


def rope_tables(positions, head_dim):
    half_dim = head_dim // 2
    inv_freqs = ROPE_BASE ** (-(jnp.arange(half_dim, dtype=F32) * 2.0) / head_dim)
    angles = positions.astype(F32)[:, None] * inv_freqs[None, :]
    cosines, sines = jnp.cos(angles), jnp.sin(angles)
    return jnp.concatenate([cosines, cosines], axis=-1), jnp.concatenate([-sines, sines], axis=-1)


def remote(src, dst, send_sem, recv_sem, ty, tx):
    return pltpu.make_async_remote_copy(
        src_ref=src, dst_ref=dst, send_sem=send_sem, recv_sem=recv_sem,
        device_id={"ty": ty, "tx": tx}, device_id_type=MESH,
    )


def project_kernel(
    ty_size, tile, d_model,
    x_main, x_kv, wq, wkv, wg, wu, gamma, cos_q, sin_q, cos_kv, sin_kv,
    act_out, q_out, kv_out,
    xs, ws, wkvs, gam, st, sr, p2, sd, sb, ra, rb, act, kvs, kvr, kvf, qs, qr,
    load_sem, pair_send, pair_recv, st_send, st_recv, ssem, rsem, kv_ssem, kv_rsem, kvf_sem, q_ssem, q_rsem, out_sem,
):
    row_idx = lax.axis_index("ty")
    col_idx = lax.axis_index("tx")
    ring_pos, core = col_idx // 2, col_idx % 2
    other = 1 - core
    half_ty = ty_size // 2
    group = xs.shape[1]
    seq_block = group // 2
    rows = half_ty * group
    hrows = rows // 2
    hg = half_ty // 2
    kdim = xs.shape[2]
    kblk = kdim // 2
    steps = wg.shape[1] // tile
    head_dim = cos_q.shape[1]
    q_width = wq.shape[1]
    pos_p, pos_m, pos_o = (ring_pos + 1) % RING, (ring_pos + RING - 1) % RING, (ring_pos + 2) % RING
    tx_p, tx_m, tx_o = pos_p * 2 + core, pos_m * 2 + core, pos_o * 2 + core
    tx_pair = ring_pos * 2 + other
    lanes = pl.ds(pl.multiple_of(core * kblk, 128), kblk)
    krows = pl.ds(pl.multiple_of(core * kblk, 128), kblk)

    pieces = []
    for d in range(RING):
        pieces.append((lambda c, d=d: x_main.at[c, :, d], xs.at[pl.ds(d * half_ty, half_ty), :, lanes]))
    pieces.append((lambda c: x_kv.at[row_idx], xs.at[pl.ds(RING * half_ty, RING), :, lanes]))
    pieces.append((lambda c: gamma, gam.at[:, lanes]))
    pieces.append((lambda c: wq, ws.at[0, krows, pl.ds(0, q_width)]))
    pieces.append((lambda c: wkv.at[c], wkvs.at[krows]))
    for t in range(steps):
        pieces.append((lambda c, t=t: wg.at[:, pl.ds(t * tile, tile)], ws.at[t + 1, krows, pl.ds(0, tile)]))
        pieces.append((lambda c, t=t: wu.at[:, pl.ds(t * tile, tile)], ws.at[t + 1, krows, pl.ds(tile, tile)]))
    loads = [pltpu.make_async_copy(src(core), dst, load_sem.at[n]) for n, (src, dst) in enumerate(pieces)]
    swaps = [remote(src(other), dst, pair_send.at[n], pair_recv.at[n], row_idx, tx_pair) for n, (src, dst) in enumerate(pieces)]
    for load in loads:
        load.start()
    st[...] = jnp.zeros_like(st)

    barrier = pltpu.get_barrier_semaphore()
    pl.semaphore_signal(barrier, inc=1, device_id={"ty": row_idx, "tx": tx_pair}, device_id_type=MESH)
    for tx in (tx_p, tx_m, tx_o):
        pl.semaphore_signal(barrier, inc=1, device_id={"ty": row_idx, "tx": tx}, device_id_type=MESH)
    for off in range(1, ty_size):
        for cc in range(2):
            pl.semaphore_signal(
                barrier, inc=1, device_id={"ty": (row_idx + off) % ty_size, "tx": ring_pos * 2 + cc}, device_id_type=MESH
            )
    pl.semaphore_wait(barrier, 4 + 2 * (ty_size - 1))
    for swap in swaps:
        swap.start()
    for n in range(6):
        loads[n].wait()
        swaps[n].wait_recv()

    blk = 2 * group
    blocks = (RING * half_ty + RING) // 2
    lane_tiles = kdim // 128

    def stat_block(b, _):
        def lane_tile(j, sums):
            part = xs[pl.ds(2 * b, 2), :, pl.ds(pl.multiple_of(j * 128, 128), 128)].reshape(blk, 128).astype(F32)
            return sums[0] + part, sums[1] + part * part
        zero = jnp.zeros((blk, 128), F32)
        s1, s2 = lax.fori_loop(0, lane_tiles, lane_tile, (zero, zero))
        st[pl.ds(b, 1), pl.ds(0, blk)] = jnp.sum(s1.T, axis=0, keepdims=True)
        st[pl.ds(b + st.shape[0] // 2, 1), pl.ds(0, blk)] = jnp.sum(s2.T, axis=0, keepdims=True)
        return 0

    lax.fori_loop(0, blocks, stat_block, 0)
    stat_copies = [
        remote(st, sr.at[n], st_send.at[n], st_recv.at[n], row_idx, tx) for n, tx in enumerate((tx_p, tx_m, tx_o))
    ]
    for copy in stat_copies:
        copy.start()
    for copy in stat_copies:
        copy.wait()
    total = ((st[...] + sr[0]) + (sr[1] + sr[2]))
    mean = total[: st.shape[0] // 2] / d_model
    var = total[st.shape[0] // 2 :] / d_model - mean * mean
    sr[0, : st.shape[0] // 2, :] = mean
    sr[1, : st.shape[0] // 2, :] = lax.rsqrt(var + EPSILON)

    def norm_block(b, _):
        mean_b = jnp.broadcast_to(sr[0, pl.ds(b, 1), :], (128, 128)).T[:blk]
        rstd_b = jnp.broadcast_to(sr[1, pl.ds(b, 1), :], (128, 128)).T[:blk]
        for j in range(lane_tiles):
            cols = slice(j * 128, (j + 1) * 128)
            part = xs[pl.ds(2 * b, 2), :, cols].reshape(blk, 128).astype(F32)
            normed = ((part - mean_b) * rstd_b * gam[0:1, cols]).astype(BF16)
            xs[pl.ds(2 * b, 2), :, cols] = normed.reshape(2, group, 128)
        return 0

    lax.fori_loop(0, blocks, norm_block, 0)

    def left(start, count):
        return xs[pl.ds(start, count)].reshape(count * group, kdim)

    def mm(start, count, w):
        return jnp.dot(left(start, count), w, preferred_element_type=F32)

    def hop(s, n, kind, side):
        cols = pl.ds(0, n)
        src, dst = (
            (p2.at[s, pl.ds(side * hrows, hrows), cols], ra.at[s, side, :, cols]),
            (sd.at[s, side, :, cols], rb.at[s, side, 0, :, cols]),
            (sb.at[s, side, :, cols], rb.at[s, side, 1, :, cols]),
        )[kind]
        return remote(src, dst, ssem.at[s, kind, side], rsem.at[s, kind, side], row_idx, (tx_p, tx_m)[side])

    def stage_a(s, n):
        w = ws[s, :, 0:n]
        p2[s, :, 0:n] = mm(pos_o * half_ty, half_ty, w).astype(BF16)
        hop(s, n, 0, 0).start()
        hop(s, n, 0, 1).start()
        sd[s, 0, :, 0:n] = mm(pos_p * half_ty + hg, hg, w).astype(BF16)
        hop(s, n, 1, 0).start()
        sd[s, 1, :, 0:n] = mm(pos_m * half_ty, hg, w).astype(BF16)
        hop(s, n, 1, 1).start()

    def stage_b(s, n):
        w = ws[s, :, 0:n]
        for side, start in ((0, pos_p * half_ty), (1, pos_m * half_ty + hg)):
            own = mm(start, hg, w)
            hop(s, n, 0, side).wait_recv()
            sb[s, side, :, 0:n] = (own + ra[s, side, :, 0:n].astype(F32)).astype(BF16)
            hop(s, n, 2, side).start()

    def stage_c(s, n, finish):
        w = ws[s, :, 0:n]
        for half in range(2):
            own = mm(ring_pos * half_ty + half * hg, hg, w)
            hop(s, n, 2, half).wait_recv()
            hop(s, n, 1, 1 - half).wait_recv()
            finish(half, own + rb[s, half, 1, :, 0:n].astype(F32) + rb[s, 1 - half, 0, :, 0:n].astype(F32))

    def turn(vals, cos2, sin2):
        return vals * cos2 + pltpu.roll(vals, head_dim // 2, 1) * sin2

    def finish_q(half, vals):
        tab = pl.ds(half * hrows, hrows)
        for h in range(q_width // head_dim):
            cols = slice(h * head_dim, (h + 1) * head_dim)
            turned = turn(vals[:, cols], cos_q[tab, :], sin_q[tab, :])
            for k in range(2 * hg):
                qs[half * 2 * hg + k, :, cols] = turned[k * seq_block : (k + 1) * seq_block].astype(BF16)

    def finish_mlp(s):
        def finish(half, vals):
            gate = vals[:, :tile].astype(BF16).astype(F32)
            up = vals[:, tile:].astype(BF16).astype(F32)
            act[pl.ds(half * hrows, hrows), pl.ds(pl.multiple_of((s - 1) * tile, tile), tile)] = (
                gate * jax.nn.sigmoid(gate) * up
            ).astype(BF16)
        return finish

    def q_copy(k):
        return remote(
            qs.at[k], qr.at[row_idx], q_ssem.at[k], q_rsem.at[row_idx],
            core * half_ty + k // 2, ring_pos * 2 + k % 2,
        )

    def q_is_self(k):
        return jnp.logical_and(core * half_ty + k // 2 == row_idx, core == k % 2)

    def kv_copy(n, pos):
        return remote(kvs.at[pos], kvr.at[n], kv_ssem.at[n], kv_rsem.at[n], row_idx, pos * 2 + core)

    wide = 2 * tile
    loads[6].wait()
    swaps[6].wait_recv()
    stage_a(0, q_width)
    loads[7].wait()
    swaps[7].wait_recv()
    kvs[...] = mm(RING * half_ty, RING, wkvs[...]).reshape(kvs.shape)
    for n, pos in enumerate((pos_p, pos_m, pos_o)):
        kv_copy(n, pos).start()
    for n in range(8, len(loads)):
        loads[n].wait()
        swaps[n].wait_recv()
    stage_a(1, wide)
    stage_b(0, q_width)
    for n, pos in enumerate((pos_p, pos_m, pos_o)):
        kv_copy(n, pos).wait_recv()
    new_row = (kvs[ring_pos] + kvr[0]) + (kvr[1] + kvr[2])
    kvf[core] = turn(new_row, cos_kv[...], sin_kv[...]).astype(BF16)
    kv_pair = remote(kvf.at[core], kvf.at[core], kvf_sem.at[0], kvf_sem.at[1], row_idx, tx_pair)
    kv_pair.start()
    stage_a(2, wide)
    stage_b(1, wide)
    stage_c(0, q_width, finish_q)
    for k in range(ty_size):
        @pl.when(q_is_self(k))
        def _():
            pltpu.make_async_copy(qs.at[k], qr.at[row_idx], q_rsem.at[row_idx]).start()

        @pl.when(jnp.logical_not(q_is_self(k)))
        def _():
            q_copy(k).start()

    def middle(s, _):
        stage_a(s, wide)
        stage_b(s - 1, wide)
        stage_c(s - 2, wide, finish_mlp(s - 2))
        return 0

    lax.fori_loop(3, steps + 1, middle, 0)
    stage_b(steps, wide)
    stage_c(steps - 1, wide, finish_mlp(steps - 1))
    stage_c(steps, wide, finish_mlp(steps))

    outs = [
        pltpu.make_async_copy(act, act_out, out_sem.at[0]),
        pltpu.make_async_copy(qr, q_out, out_sem.at[1]),
        pltpu.make_async_copy(kvf, kv_out, out_sem.at[2]),
    ]
    outs[0].start()
    for k in range(ty_size):
        remote(qs.at[0], qr.at[k], q_ssem.at[0], q_rsem.at[k], row_idx, tx_pair).wait_recv()
    outs[1].start()
    kv_pair.wait_send()
    remote(kvf.at[other], kvf.at[other], kvf_sem.at[0], kvf_sem.at[1], row_idx, tx_pair).wait_recv()
    outs[2].start()
    for k in range(ty_size):
        @pl.when(jnp.logical_not(q_is_self(k)))
        def _():
            q_copy(k).wait_send()
    for n, pos in enumerate((pos_p, pos_m, pos_o)):
        kv_copy(n, pos).wait_send()
    for swap in swaps:
        swap.wait_send()
    for kind in range(3):
        for side in range(2):
            hop(0, q_width, kind, side).wait_send()

    def drain(s, _):
        for kind in range(3):
            for side in range(2):
                hop(s, wide, kind, side).wait_send()
        return 0

    lax.fori_loop(1, steps + 1, drain, 0)
    for out in outs:
        out.wait()


def project(x_blk, gamma_blk, wq, wk, wv, wg, wu, cos_q, sin_q, cos_kv, sin_kv, ty_size, seq_block, d_model, tile):
    rows_all, kblk = x_blk.shape
    half_ty, group = ty_size // 2, 2 * seq_block
    rows = half_ty * group
    q_width, ffn = wq.shape[1], wg.shape[1]
    kv_width = wk.shape[1]
    steps = ffn // tile
    wide = 2 * tile
    kdim = 2 * kblk
    x_main = x_blk.reshape(2, half_ty, RING, group, kblk)
    x_kv = x_blk.reshape(ty_size, RING, group, kblk)
    wkv = jnp.stack([wk, wv])
    gamma = jnp.broadcast_to(gamma_blk[None, :], (8, kblk))
    pieces = RING + 4 + 2 * steps
    stat_lines = 2 * (-(-((RING * half_ty + RING) // 2) // 8) * 8)
    any_spec = pl.BlockSpec(memory_space=pl.ANY)
    vmem_spec = pl.BlockSpec(memory_space=pltpu.VMEM)
    return pl.pallas_call(
        functools.partial(project_kernel, ty_size, tile, d_model),
        out_shape=(
            jax.ShapeDtypeStruct((rows, ffn), BF16),
            jax.ShapeDtypeStruct((ty_size, seq_block, q_width), BF16),
            jax.ShapeDtypeStruct((2, group, kv_width), BF16),
        ),
        in_specs=[any_spec] * 7 + [vmem_spec] * 4,
        out_specs=(any_spec,) * 3,
        scratch_shapes=[
            pltpu.VMEM((RING * half_ty + RING, group, kdim), BF16),
            pltpu.VMEM((steps + 1, kdim, wide), BF16),
            pltpu.VMEM((kdim, kv_width), BF16),
            pltpu.VMEM((8, kdim), F32),
            pltpu.VMEM((stat_lines, 128), F32),
            pltpu.VMEM((3, stat_lines, 128), F32),
            pltpu.VMEM((steps + 1, rows, wide), BF16),
            pltpu.VMEM((steps + 1, 2, rows // 2, wide), BF16),
            pltpu.VMEM((steps + 1, 2, rows // 2, wide), BF16),
            pltpu.VMEM((steps + 1, 2, rows // 2, wide), BF16),
            pltpu.VMEM((steps + 1, 2, 2, rows // 2, wide), BF16),
            pltpu.VMEM((rows, ffn), BF16),
            pltpu.VMEM((RING, group, kv_width), F32),
            pltpu.VMEM((3, group, kv_width), F32),
            pltpu.VMEM((2, group, kv_width), BF16),
            pltpu.VMEM((ty_size, seq_block, q_width), BF16),
            pltpu.VMEM((ty_size, seq_block, q_width), BF16),
            pltpu.SemaphoreType.DMA((pieces,)),
            pltpu.SemaphoreType.DMA((pieces,)),
            pltpu.SemaphoreType.DMA((pieces,)),
            pltpu.SemaphoreType.DMA((3,)),
            pltpu.SemaphoreType.DMA((3,)),
            pltpu.SemaphoreType.DMA((steps + 1, 3, 2)),
            pltpu.SemaphoreType.DMA((steps + 1, 3, 2)),
            pltpu.SemaphoreType.DMA((3,)),
            pltpu.SemaphoreType.DMA((3,)),
            pltpu.SemaphoreType.DMA((2,)),
            pltpu.SemaphoreType.DMA((ty_size,)),
            pltpu.SemaphoreType.DMA((ty_size,)),
            pltpu.SemaphoreType.DMA((3,)),
        ],
        compiler_params=pltpu.CompilerParams(
            collective_id=0, has_side_effects=True, vmem_limit_bytes=56 * 1024 * 1024
        ),
        name="project",
    )(x_main, x_kv, wq, wkv, wg, wu, gamma, cos_q, sin_q, cos_kv, sin_kv)


def solution(mesh):
    ty_size = mesh.shape["ty"]
    tx_size = mesh.shape["tx"]
    cache_spec = P(("dp", "ty", "tx"), None, None)

    def layer_shard(x_blk, lens_part, k_blk, v_blk, gamma_blk, w_query, w_key, w_value, w_gate, w_up, w_out, w_down):
        rows = x_blk.shape[0]
        d_model = x_blk.shape[1] * tx_size
        seq_block, ctx_len, head_dim = k_blk.shape
        half_ty, group = ty_size // 2, 2 * seq_block
        local_heads = w_query.shape[1] // head_dim
        row_idx = lax.axis_index("ty")
        col_idx = lax.axis_index("tx")
        ring_pos, core = col_idx // 2, col_idx % 2
        tile = min(256, w_gate.shape[1])

        lens_q = lax.dynamic_slice(lens_part.reshape(2, half_ty, RING, group), (core, 0, ring_pos, 0), (1, half_ty, 1, group))
        cos_q, sin_q = rope_tables(lens_q.reshape(-1), head_dim)
        block_start = (row_idx * tx_size + col_idx) * seq_block
        lens_own = lax.dynamic_slice_in_dim(lens_part, block_start, seq_block)
        lens_kv = lax.dynamic_slice_in_dim(lens_part, (row_idx * RING + ring_pos) * group, group)
        cos_kv, sin_kv = rope_tables(jnp.where(core == 0, lens_kv, 0), head_dim)

        act_own, q_owned, kv_new = project(
            x_blk, gamma_blk, w_query, w_key, w_value, w_gate, w_up, cos_q, sin_q, cos_kv, sin_kv,
            ty_size, seq_block, d_model, tile,
        )
        kv_own = lax.dynamic_slice_in_dim(kv_new, core * seq_block, seq_block, axis=1)
        positions = jnp.arange(ctx_len)
        at_slot = positions[None, :, None] == lens_own[:, None, None]
        k_out = jnp.where(at_slot, kv_own[0][:, None, :], k_blk)
        v_out = jnp.where(at_slot, kv_own[1][:, None, :], v_blk)

        q_owned = q_owned.reshape(ty_size, seq_block, local_heads, head_dim)
        scores = jnp.einsum("gbhd,btd->gbht", q_owned, k_out, preferred_element_type=F32) * (head_dim ** -0.5)
        in_range = positions[None, None, None, :] <= lens_own[None, :, None, None]
        scores = jnp.where(in_range, scores, -1e30)
        att_probs = jax.nn.softmax(scores, axis=-1).astype(BF16)
        att_owned = jnp.einsum("gbht,btd->gbhd", att_probs, v_out, preferred_element_type=F32).astype(BF16)
        att_column = lax.all_to_all(att_owned, "ty", 0, 0, tiled=True)
        att_rows = lax.all_gather(att_column, "tx", axis=1, tiled=False).reshape(rows, local_heads * head_dim)

        mlp_all = lax.all_gather(act_own, "tx", axis=0, tiled=False)
        mlp_act = mlp_all.reshape(RING, 2, half_ty, group, -1).transpose(1, 2, 0, 3, 4).reshape(rows, -1)
        part_out = jnp.dot(att_rows, w_out, preferred_element_type=F32) + jnp.dot(mlp_act, w_down, preferred_element_type=F32)
        out_sum = lax.psum(part_out.astype(BF16), "ty")
        y_blk = (x_blk.astype(F32) + out_sum.astype(F32)).astype(BF16)
        return y_blk, k_out, v_out

    in_specs = (P("dp", "tx"), P("dp"), cache_spec, cache_spec, P("tx"), P("tx", "ty"), P("tx", None), P("tx", None), P("tx", "ty"), P("tx", "ty"), P("ty", "tx"), P("ty", "tx"))
    out_specs = (P("dp", "tx"), cache_spec, cache_spec)
    return jax.shard_map(layer_shard, mesh=mesh, in_specs=in_specs, out_specs=out_specs, check_vma=False)
```

```python
import functools

import jax
import jax.numpy as jnp
from jax import lax
from jax.experimental import pallas as pl
from jax.experimental.pallas import tpu as pltpu
from jax.sharding import PartitionSpec as P

EPSILON = 1e-6
ROPE_BASE = 10000.0
MESH = pl.DeviceIdType.MESH
RING = 4
CORES = 2
TWO = 2
LANES = 128
BOTH = (0, 1)
KINDS = (0, 1, 2)
MIB = 2**20
F32 = jnp.float32
BF16 = jnp.bfloat16


def rope_tables(positions, head_dim):
    half_dim = head_dim // 2
    inv_freqs = ROPE_BASE ** (-(jnp.arange(half_dim, dtype=F32) * 2.0) / head_dim)
    angles = positions.astype(F32)[:, None] * inv_freqs[None, :]
    cosines, sines = jnp.cos(angles), jnp.sin(angles)
    return jnp.concatenate([cosines, cosines], axis=-1), jnp.concatenate([-sines, sines], axis=-1)


def remote(src, dst, send_sem, recv_sem, ty, tx):
    return pltpu.make_async_remote_copy(
        src_ref=src, dst_ref=dst, send_sem=send_sem, recv_sem=recv_sem,
        device_id={"ty": ty, "tx": tx}, device_id_type=MESH,
    )


def project_kernel(
    ty_size, tile, d_model,
    x_main, x_kv, wq, wkv, wg, wu, gamma, cos_q, sin_q, cos_kv, sin_kv,
    act_out, q_out, kv_out,
    xs, ws, wkvs, gam, st, sr, p2, sd, sb, ra, rb, act, kvs, kvr, kvf, qs, qr,
    load_sem, pair_send, pair_recv, st_send, st_recv, ssem, rsem, kv_ssem, kv_rsem, kvf_sem, q_ssem, q_rsem, out_sem,
):
    row_idx = lax.axis_index("ty")
    col_idx = lax.axis_index("tx")
    ring_pos, core = col_idx // 2, col_idx % 2
    other = 1 - core
    half_ty = ty_size // 2
    group = xs.shape[1]
    seq_block = group // 2
    rows = half_ty * group
    hrows = rows // 2
    hg = half_ty // 2
    kdim = xs.shape[2]
    kblk = kdim // 2
    steps = wg.shape[1] // tile
    head_dim = cos_q.shape[1]
    q_width = wq.shape[1]
    pos_p, pos_m, pos_o = (ring_pos + 1) % RING, (ring_pos + RING - 1) % RING, (ring_pos + 2) % RING
    tx_p, tx_m, tx_o = pos_p * 2 + core, pos_m * 2 + core, pos_o * 2 + core
    tx_pair = ring_pos * 2 + other
    lanes = pl.ds(pl.multiple_of(core * kblk, LANES), kblk)
    krows = pl.ds(pl.multiple_of(core * kblk, LANES), kblk)

    pieces = []
    for d in range(RING):
        pieces.append((lambda c, d=d: x_main.at[c, :, d], xs.at[pl.ds(d * half_ty, half_ty), :, lanes]))
    pieces.append((lambda c: x_kv.at[row_idx], xs.at[pl.ds(RING * half_ty, RING), :, lanes]))
    pieces.append((lambda c: gamma, gam.at[:, lanes]))
    pieces.append((lambda c: wq, ws.at[0, krows, pl.ds(0, q_width)]))
    pieces.append((lambda c: wkv.at[c], wkvs.at[krows]))
    for t in range(steps):
        pieces.append((lambda c, t=t: wg.at[:, pl.ds(t * tile, tile)], ws.at[t + 1, krows, pl.ds(0, tile)]))
        pieces.append((lambda c, t=t: wu.at[:, pl.ds(t * tile, tile)], ws.at[t + 1, krows, pl.ds(tile, tile)]))
    loads = [pltpu.make_async_copy(src(core), dst, load_sem.at[n]) for n, (src, dst) in enumerate(pieces)]
    swaps = [remote(src(other), dst, pair_send.at[n], pair_recv.at[n], row_idx, tx_pair) for n, (src, dst) in enumerate(pieces)]
    for load in loads:
        load.start()
    st[...] = jnp.zeros_like(st)

    barrier = pltpu.get_barrier_semaphore()
    pl.semaphore_signal(barrier, device_id={"ty": row_idx, "tx": tx_pair}, device_id_type=MESH)
    for tx in (tx_p, tx_m, tx_o):
        pl.semaphore_signal(barrier, device_id={"ty": row_idx, "tx": tx}, device_id_type=MESH)
    for off in range(1, ty_size):
        for cc in BOTH:
            pl.semaphore_signal(
                barrier, device_id={"ty": (row_idx + off) % ty_size, "tx": ring_pos * 2 + cc}, device_id_type=MESH
            )
    pl.semaphore_wait(barrier, 4 + 2 * (ty_size - 1))
    for swap in swaps:
        swap.start()
    for n in range(6):
        loads[n].wait()
        swaps[n].wait_recv()

    blk = 2 * group
    blocks = (RING * half_ty + RING) // 2
    lane_tiles = kdim // 128

    def stat_block(b, _):
        def lane_tile(j, sums):
            part = xs[pl.ds(2 * b, 2), :, pl.ds(pl.multiple_of(j * 128, LANES), LANES)].reshape(blk, LANES).astype(F32)
            return sums[0] + part, sums[1] + part * part
        zero = jnp.zeros((blk, LANES), F32)
        s1, s2 = lax.fori_loop(0, lane_tiles, lane_tile, (zero, zero))
        st[pl.ds(b, 1), pl.ds(0, blk)] = jnp.sum(s1.T, axis=0, keepdims=True)
        st[pl.ds(b + st.shape[0] // 2, 1), pl.ds(0, blk)] = jnp.sum(s2.T, axis=0, keepdims=True)
        return 0

    lax.fori_loop(0, blocks, stat_block, 0)
    stat_copies = [
        remote(st, sr.at[n], st_send.at[n], st_recv.at[n], row_idx, tx) for n, tx in enumerate((tx_p, tx_m, tx_o))
    ]
    for copy in stat_copies:
        copy.start()
    for copy in stat_copies:
        copy.wait()
    total = ((st[...] + sr[0]) + (sr[1] + sr[2]))
    mean = total[: st.shape[0] // 2] / d_model
    var = total[st.shape[0] // 2 :] / d_model - mean * mean
    sr[0, : st.shape[0] // 2, :] = mean
    sr[1, : st.shape[0] // 2, :] = lax.rsqrt(var + EPSILON)

    def norm_block(b, _):
        mean_b = jnp.broadcast_to(sr[0, pl.ds(b, 1), :], (128, LANES)).T[:blk]
        rstd_b = jnp.broadcast_to(sr[1, pl.ds(b, 1), :], (128, LANES)).T[:blk]
        for j in range(lane_tiles):
            cols = slice(j * 128, (j + 1) * LANES)
            part = xs[pl.ds(2 * b, 2), :, cols].reshape(blk, LANES).astype(F32)
            normed = ((part - mean_b) * rstd_b * gam[0:1, cols]).astype(BF16)
            xs[pl.ds(2 * b, 2), :, cols] = normed.reshape(2, group, LANES)
        return 0

    lax.fori_loop(0, blocks, norm_block, 0)

    def left(start, count):
        return xs[pl.ds(start, count)].reshape(count * group, kdim)

    def mm(start, count, w):
        return jnp.dot(left(start, count), w, preferred_element_type=F32)

    def hop(s, n, kind, side):
        cols = pl.ds(0, n)
        src, dst = (
            (p2.at[s, pl.ds(side * hrows, hrows), cols], ra.at[s, side, :, cols]),
            (sd.at[s, side, :, cols], rb.at[s, side, 0, :, cols]),
            (sb.at[s, side, :, cols], rb.at[s, side, 1, :, cols]),
        )[kind]
        return remote(src, dst, ssem.at[s, kind, side], rsem.at[s, kind, side], row_idx, (tx_p, tx_m)[side])

    def stage_a(s, n):
        w = ws[s, :, 0:n]
        p2[s, :, 0:n] = mm(pos_o * half_ty, half_ty, w).astype(BF16)
        hop(s, n, 0, 0).start()
        hop(s, n, 0, 1).start()
        sd[s, 0, :, 0:n] = mm(pos_p * half_ty + hg, hg, w).astype(BF16)
        hop(s, n, 1, 0).start()
        sd[s, 1, :, 0:n] = mm(pos_m * half_ty, hg, w).astype(BF16)
        hop(s, n, 1, 1).start()

    def stage_b(s, n):
        w = ws[s, :, 0:n]
        for side, start in ((0, pos_p * half_ty), (1, pos_m * half_ty + hg)):
            own = mm(start, hg, w)
            hop(s, n, 0, side).wait_recv()
            sb[s, side, :, 0:n] = (own + ra[s, side, :, 0:n].astype(F32)).astype(BF16)
            hop(s, n, 2, side).start()

    def stage_c(s, n, finish):
        w = ws[s, :, 0:n]
        for half in BOTH:
            own = mm(ring_pos * half_ty + half * hg, hg, w)
            hop(s, n, 2, half).wait_recv()
            hop(s, n, 1, 1 - half).wait_recv()
            finish(half, own + rb[s, half, 1, :, 0:n].astype(F32) + rb[s, 1 - half, 0, :, 0:n].astype(F32))

    def turn(vals, cos2, sin2):
        return vals * cos2 + pltpu.roll(vals, head_dim // 2, 1) * sin2

    def finish_q(half, vals):
        tab = pl.ds(half * hrows, hrows)
        for h in range(q_width // head_dim):
            cols = slice(h * head_dim, (h + 1) * head_dim)
            turned = turn(vals[:, cols], cos_q[tab, :], sin_q[tab, :])
            for k in range(2 * hg):
                qs[half * 2 * hg + k, :, cols] = turned[k * seq_block : (k + 1) * seq_block].astype(BF16)

    def finish_mlp(s):
        def finish(half, vals):
            gate = vals[:, :tile].astype(BF16).astype(F32)
            up = vals[:, tile:].astype(BF16).astype(F32)
            act[pl.ds(half * hrows, hrows), pl.ds(pl.multiple_of((s - 1) * tile, tile), tile)] = (
                gate * jax.nn.sigmoid(gate) * up
            ).astype(BF16)
        return finish

    def q_copy(k):
        return remote(
            qs.at[k], qr.at[row_idx], q_ssem.at[k], q_rsem.at[row_idx],
            core * half_ty + k // 2, ring_pos * 2 + k % 2,
        )

    def q_is_self(k):
        return jnp.logical_and(core * half_ty + k // 2 == row_idx, core == k % 2)

    def kv_copy(n, pos):
        return remote(kvs.at[pos], kvr.at[n], kv_ssem.at[n], kv_rsem.at[n], row_idx, pos * 2 + core)

    wide = 2 * tile
    loads[6].wait()
    swaps[6].wait_recv()
    stage_a(0, q_width)
    loads[7].wait()
    swaps[7].wait_recv()
    kvs[...] = mm(RING * half_ty, RING, wkvs[...]).reshape(kvs.shape)
    for n, pos in enumerate((pos_p, pos_m, pos_o)):
        kv_copy(n, pos).start()
    for n in range(8, len(loads)):
        loads[n].wait()
        swaps[n].wait_recv()
    stage_a(1, wide)
    stage_b(0, q_width)
    for n, pos in enumerate((pos_p, pos_m, pos_o)):
        kv_copy(n, pos).wait_recv()
    new_row = (kvs[ring_pos] + kvr[0]) + (kvr[1] + kvr[2])
    kvf[core] = turn(new_row, cos_kv[...], sin_kv[...]).astype(BF16)
    kv_pair = remote(kvf.at[core], kvf.at[core], kvf_sem.at[0], kvf_sem.at[1], row_idx, tx_pair)
    kv_pair.start()
    stage_a(2, wide)
    stage_b(1, wide)
    stage_c(0, q_width, finish_q)
    for k in range(ty_size):
        @pl.when(q_is_self(k))
        def _():
            pltpu.make_async_copy(qs.at[k], qr.at[row_idx], q_rsem.at[row_idx]).start()

        @pl.when(jnp.logical_not(q_is_self(k)))
        def _():
            q_copy(k).start()

    def middle(s, _):
        stage_a(s, wide)
        stage_b(s - 1, wide)
        stage_c(s - 2, wide, finish_mlp(s - 2))
        return 0

    lax.fori_loop(3, steps + 1, middle, 0)
    stage_b(steps, wide)
    stage_c(steps - 1, wide, finish_mlp(steps - 1))
    stage_c(steps, wide, finish_mlp(steps))

    outs = [
        pltpu.make_async_copy(act, act_out, out_sem.at[0]),
        pltpu.make_async_copy(qr, q_out, out_sem.at[1]),
        pltpu.make_async_copy(kvf, kv_out, out_sem.at[2]),
    ]
    outs[0].start()
    for k in range(ty_size):
        remote(qs.at[0], qr.at[k], q_ssem.at[0], q_rsem.at[k], row_idx, tx_pair).wait_recv()
    outs[1].start()
    kv_pair.wait_send()
    remote(kvf.at[other], kvf.at[other], kvf_sem.at[0], kvf_sem.at[1], row_idx, tx_pair).wait_recv()
    outs[2].start()
    for k in range(ty_size):
        @pl.when(jnp.logical_not(q_is_self(k)))
        def _():
            q_copy(k).wait_send()
    for n, pos in enumerate((pos_p, pos_m, pos_o)):
        kv_copy(n, pos).wait_send()
    for swap in swaps:
        swap.wait_send()
    for kind in KINDS:
        for side in BOTH:
            hop(0, q_width, kind, side).wait_send()

    def drain(s, _):
        for kind in KINDS:
            for side in BOTH:
                hop(s, wide, kind, side).wait_send()
        return 0

    lax.fori_loop(1, steps + 1, drain, 0)
    for out in outs:
        out.wait()


def project(x_blk, gamma_blk, wq, wk, wv, wg, wu, cos_q, sin_q, cos_kv, sin_kv, ty_size, seq_block, d_model, tile):
    rows_all, kblk = x_blk.shape
    half_ty, group = ty_size // TWO, TWO * seq_block
    rows = half_ty * group
    q_width, ffn = wq.shape[1], wg.shape[1]
    kv_width = wk.shape[1]
    steps = ffn // tile
    wide = 2 * tile
    kdim = 2 * kblk
    x_main = x_blk.reshape(TWO, half_ty, RING, group, kblk)
    x_kv = x_blk.reshape(ty_size, RING, group, kblk)
    wkv = jnp.stack([wk, wv])
    gamma = jnp.broadcast_to(gamma_blk[None, :], (8, kblk))
    pieces = RING + 4 + 2 * steps
    stat_lines = 2 * (-(-((RING * half_ty + RING) // TWO) // 8) * 8)
    any_spec = pl.BlockSpec(memory_space=pl.ANY)
    vmem_spec = pl.BlockSpec(memory_space=pltpu.VMEM)
    return pl.pallas_call(
        functools.partial(project_kernel, ty_size, tile, d_model),
        out_shape=(
            jax.ShapeDtypeStruct((rows, ffn), BF16),
            jax.ShapeDtypeStruct((ty_size, seq_block, q_width), BF16),
            jax.ShapeDtypeStruct((TWO, group, kv_width), BF16),
        ),
        in_specs=[any_spec] * 7 + [vmem_spec] * 4,
        out_specs=(any_spec,) * 3,
        scratch_shapes=[
            pltpu.VMEM((RING * half_ty + RING, group, kdim), BF16),
            pltpu.VMEM((steps + 1, kdim, wide), BF16),
            pltpu.VMEM((kdim, kv_width), BF16),
            pltpu.VMEM((8, kdim), F32),
            pltpu.VMEM((stat_lines, LANES), F32),
            pltpu.VMEM((3, stat_lines, LANES), F32),
            pltpu.VMEM((steps + 1, rows, wide), BF16),
            pltpu.VMEM((steps + 1, TWO, rows // TWO, wide), BF16),
            pltpu.VMEM((steps + 1, TWO, rows // TWO, wide), BF16),
            pltpu.VMEM((steps + 1, TWO, rows // TWO, wide), BF16),
            pltpu.VMEM((steps + 1, TWO, TWO, rows // TWO, wide), BF16),
            pltpu.VMEM((rows, ffn), BF16),
            pltpu.VMEM((RING, group, kv_width), F32),
            pltpu.VMEM((3, group, kv_width), F32),
            pltpu.VMEM((TWO, group, kv_width), BF16),
            pltpu.VMEM((ty_size, seq_block, q_width), BF16),
            pltpu.VMEM((ty_size, seq_block, q_width), BF16),
            pltpu.SemaphoreType.DMA((pieces,)),
            pltpu.SemaphoreType.DMA((pieces,)),
            pltpu.SemaphoreType.DMA((pieces,)),
            pltpu.SemaphoreType.DMA((len(KINDS),)),
            pltpu.SemaphoreType.DMA((len(KINDS),)),
            pltpu.SemaphoreType.DMA((steps + 1, len(KINDS), TWO)),
            pltpu.SemaphoreType.DMA((steps + 1, len(KINDS), TWO)),
            pltpu.SemaphoreType.DMA((len(KINDS),)),
            pltpu.SemaphoreType.DMA((len(KINDS),)),
            pltpu.SemaphoreType.DMA((TWO,)),
            pltpu.SemaphoreType.DMA((ty_size,)),
            pltpu.SemaphoreType.DMA((ty_size,)),
            pltpu.SemaphoreType.DMA((len(KINDS),)),
        ],
        compiler_params=pltpu.CompilerParams(
            collective_id=0, has_side_effects=True, vmem_limit_bytes=56 * MIB
        ),
        name="project",
    )(x_main, x_kv, wq, wkv, wg, wu, gamma, cos_q, sin_q, cos_kv, sin_kv)


def combine_kernel(
    ty_size, chunks,
    att_in, act_in, x_in, wo, wd,
    y_out,
    att, mlp, wos, wds, yp, t1, xr, yf, p2_1, sd_1, sb_1, ra_1, rb_1, p2_2, sd_2, sb_2, ra_2, rb_2,
    w_sem, wp_send, wp_recv, a2a_send, a2a_recv, mlp_sem, gx_send, gx_recv, x_sem, xp_send, xp_recv,
    rs_send, rs_recv, ag_send, ag_recv, out_sem, outp_send, outp_recv,
):
    row_idx = lax.axis_index("ty")
    col_idx = lax.axis_index("tx")
    ring_pos, core = col_idx // 2, col_idx % 2
    other = 1 - core
    half_ty = ty_size // 2
    seq_block = att_in.shape[1]
    cols = wo.shape[1]
    hcols = cols // 2
    pos_p, pos_m = (ring_pos + 1) % RING, (ring_pos + RING - 1) % RING
    tx_side = (pos_p * 2 + core, pos_m * 2 + core)
    from_side = (pos_m, pos_p)
    tx_pair = ring_pos * 2 + other
    z_pos, y_pos = row_idx // RING, row_idx % RING
    up = lambda v: (v + 1) % RING
    down = lambda v: (v + RING - 1) % RING
    y_side = (z_pos * RING + up(y_pos), z_pos * RING + down(y_pos))
    z_side = (up(z_pos) * RING + y_pos, down(z_pos) * RING + y_pos)
    places = ((y_pos, z_pos), (z_pos, y_pos))
    sides = ((y_side, z_side), (z_side, y_side))
    blk = yp.shape[1] // RING
    sub = blk // RING
    mine = pl.ds(pl.multiple_of(core * cols, LANES), cols)

    def x_tile(c, r):
        b1, b2 = jnp.where(core == 0, y_pos, z_pos), jnp.where(core == 0, z_pos, y_pos)
        return x_in.at[c, 2 * r + b2 // 2, b1, b2 % 2]

    w_loads = [pltpu.make_async_copy(wd, wds.at[:, mine], w_sem.at[0]), pltpu.make_async_copy(wo, wos.at[:, mine], w_sem.at[1])]
    w_swaps = [
        remote(wd, wds.at[:, mine], wp_send.at[0], wp_recv.at[0], row_idx, tx_pair),
        remote(wo, wos.at[:, mine], wp_send.at[1], wp_recv.at[1], row_idx, tx_pair),
    ]
    mlp_loads = [pltpu.make_async_copy(act_in.at[r], mlp.at[r, ring_pos], mlp_sem.at[r]) for r in range(chunks)]
    x_loads = [pltpu.make_async_copy(x_tile(core, r), xr.at[core, r], x_sem.at[r]) for r in range(chunks)]
    x_swaps = [remote(x_tile(other, r), xr.at[core, r], xp_send.at[r], xp_recv.at[r], row_idx, tx_pair) for r in range(chunks)]
    for load in w_loads + mlp_loads + x_loads:
        load.start()

    barrier = pltpu.get_barrier_semaphore()
    pl.semaphore_signal(barrier, device_id={"ty": row_idx, "tx": tx_pair}, device_id_type=MESH)
    for tx in tx_side:
        pl.semaphore_signal(barrier, device_id={"ty": row_idx, "tx": tx}, device_id_type=MESH)
    for off in range(1, ty_size):
        for cc in BOTH:
            pl.semaphore_signal(
                barrier, device_id={"ty": (row_idx + off) % ty_size, "tx": ring_pos * 2 + cc}, device_id_type=MESH
            )
    pl.semaphore_wait(barrier, 3 + 2 * (ty_size - 1))

    def gather(r, part, stage, side):
        sems = gx_send.at[r, part, stage, side], gx_recv.at[r, part, stage, side]
        buf = (mlp, att)[part]
        if stage == 0:
            src = act_in.at[r] if part == 0 else att.at[r, ring_pos]
            return remote(src, buf.at[r, ring_pos], *sems, row_idx, tx_side[side])
        block = buf.at[r, from_side[side], side]
        return remote(block, block, *sems, row_idx, tx_side[side])

    home, home_core = row_idx % half_ty, row_idx // half_ty

    def a2a(k):
        return remote(
            att_in.at[k], att.at[home // 2, ring_pos, home % 2, core], a2a_send.at[k], a2a_recv.at[home, core],
            k, ring_pos * 2 + home_core,
        )

    def a2a_self(k):
        return jnp.logical_and(k == row_idx, core == home_core)

    for side in BOTH:
        gather(0, 0, 0, side).start()
    for k in range(ty_size):
        @pl.when(a2a_self(k))
        def _():
            pltpu.make_async_copy(
                att_in.at[k], att.at[home // 2, ring_pos, home % 2, core], a2a_recv.at[home, core]
            ).start()

        @pl.when(jnp.logical_not(a2a_self(k)))
        def _():
            a2a(k).start()
    for swap in w_swaps + x_swaps:
        swap.start()

    def att_ready(r):
        for g in (2 * r, 2 * r + 1):
            for cc in BOTH:
                remote(
                    att_in.at[0], att.at[r, ring_pos, g % 2, cc], a2a_send.at[0], a2a_recv.at[g, cc], row_idx, tx_pair
                ).wait_recv()

    def own_att(r):
        att_ready(r)
        for side in BOTH:
            gather(r, 1, 0, side).start()

    def own_mlp(r):
        for side in BOTH:
            gather(r, 0, 0, side).start()

    def forward(r):
        for part in BOTH:
            for side in BOTH:
                gather(r, part, 0, side).wait_recv()
                gather(r, part, 1, side).start()

    def multiply(r):
        mlp_loads[r].wait()
        for part in BOTH:
            for side in BOTH:
                gather(r, part, 1, side).wait_recv()
        rows = yp.shape[1]

        def tile(n, _):
            lanes = pl.ds(pl.multiple_of(n * 512, 512), 512)
            left_mlp = mlp[r].reshape(rows, mlp.shape[-1])
            left_att = att[r].reshape(rows, att.shape[-1])
            yp[r, :, lanes] = jnp.dot(left_mlp, wds[:, lanes], preferred_element_type=F32) + jnp.dot(
                left_att, wos[:, lanes], preferred_element_type=F32
            )
            return 0

        lax.fori_loop(0, yp.shape[2] // 512, tile, 0)

    bufs = ((p2_1, sd_1, sb_1, ra_1, rb_1), (p2_2, sd_2, sb_2, ra_2, rb_2))

    def hop(level, r, c, kind, side):
        p2, sd, sb, ra, rb = bufs[level]
        src, dst = (
            (p2.at[r, c, :, pl.ds(side * hcols, hcols)], ra.at[r, c, side]),
            (sd.at[r, c, side], rb.at[r, c, side, 0]),
            (sb.at[r, c, side], rb.at[r, c, side, 1]),
        )[kind]
        return remote(
            src, dst, rs_send.at[level, r, c, kind, side], rs_recv.at[level, r, c, kind, side],
            sides[c][level][side], col_idx,
        )

    def part_of(level, r, c, b, half):
        size = (blk, sub)[level]
        rows = pl.ds(pl.multiple_of(b * size, 8), size)
        if level == 0:
            return yp[r, rows, c * cols + half * hcols : c * cols + (half + 1) * hcols]
        return t1[r, c, rows, half * hcols : (half + 1) * hcols]

    def reduce_a(level, r):
        p2, sd = bufs[level][:2]
        for c in BOTH:
            pos = places[c][level]
            for half in BOTH:
                p2[r, c, :, half * hcols : (half + 1) * hcols] = part_of(level, r, c, (pos + 2) % RING, half).astype(BF16)
                hop(level, r, c, 0, half).start()
        for c in BOTH:
            pos = places[c][level]
            sd[r, c, 0] = part_of(level, r, c, up(pos), 1).astype(BF16)
            hop(level, r, c, 1, 0).start()
            sd[r, c, 1] = part_of(level, r, c, down(pos), 0).astype(BF16)
            hop(level, r, c, 1, 1).start()

    def reduce_b(level, r):
        sb, ra = bufs[level][2:4]
        for c in BOTH:
            pos = places[c][level]
            for side, b in ((0, up(pos)), (1, down(pos))):
                hop(level, r, c, 0, side).wait_recv()
                sb[r, c, side] = (part_of(level, r, c, b, side) + ra[r, c, side].astype(F32)).astype(BF16)
                hop(level, r, c, 2, side).start()

    def reduce_c(level, r, finish):
        rb = bufs[level][4]
        for c in BOTH:
            pos = places[c][level]
            for half in BOTH:
                hop(level, r, c, 1, 1 - half).wait_recv()
                hop(level, r, c, 2, half).wait_recv()
                finish(
                    c, half,
                    part_of(level, r, c, pos, half) + rb[r, c, half, 1].astype(F32) + rb[r, c, 1 - half, 0].astype(F32),
                )

    def spread(level, r, c, stage, side):
        ring, (p1, p2) = sides[c][level], places[c]
        sems = ag_send.at[level, r, c, stage, side], ag_recv.at[level, r, c, stage, side]
        near = (down, up)[side]
        if level == 1:
            if stage == 0:
                block = yf.at[r, c, p1, p2 // 2, p2 % 2]
            else:
                block = yf.at[r, c, p1, near(p2) // 2, near(p2) % 2, :, pl.ds(side * hcols, hcols)]
        elif stage == 0:
            block = yf.at[r, c, p1]
        else:
            block = yf.at[r, c, near(p1), side]
        return remote(block, block, *sems, ring[side], col_idx)

    def spread_own(level, r):
        for c in BOTH:
            for side in BOTH:
                spread(level, r, c, 0, side).start()

    def spread_on(level, r):
        for c in BOTH:
            for side in BOTH:
                spread(level, r, c, 0, side).wait_recv()
                spread(level, r, c, 1, side).start()

    def spread_end(level, r):
        for c in BOTH:
            for side in BOTH:
                spread(level, r, c, 1, side).wait_recv()

    def s3(r):
        reduce_b(0, r)

    def s4(r):
        def finish(c, half, vals):
            t1[r, c, :, half * hcols : (half + 1) * hcols] = vals
        reduce_c(0, r, finish)
        reduce_a(1, r)

    def s5(r):
        reduce_b(1, r)

    def s6(r):
        x_loads[r].wait()
        remote(x_tile(other, r), xr.at[other, r], xp_send.at[r], xp_recv.at[r], row_idx, tx_pair).wait_recv()

        def finish(c, half, vals):
            lanes = slice(half * hcols, (half + 1) * hcols)
            p1, p2 = places[c]
            yf[r, c, p1, p2 // 2, p2 % 2, :, lanes] = (xr[c, r, :, lanes].astype(F32) + vals).astype(BF16)
        reduce_c(1, r, finish)
        spread_own(1, r)

    def s7(r):
        spread_on(1, r)

    def s8(r):
        spread_end(1, r)
        spread_own(0, r)

    def s9(r):
        spread_on(0, r)

    def out_copy(r, p):
        return pltpu.make_async_copy(
            yf.at[r, core, p], y_out.at[core, pl.ds(2 * r, 2), p], out_sem.at[r, p]
        )

    def out_swap(r, p):
        return remote(
            yf.at[r, other, p], y_out.at[core, pl.ds(2 * r, 2), p],
            outp_send.at[r, p], outp_recv.at[r, p], row_idx, tx_pair,
        )

    def s10(r):
        spread_end(0, r)
        for p in range(RING):
            out_swap(r, p).start()
            out_copy(r, p).start()

    def s2(r):
        multiply(r)
        reduce_a(0, r)

    own_mlp(1)
    own_att(0)
    own_att(1)
    forward(0)
    own_mlp(2)
    own_att(2)
    forward(1)
    own_mlp(3)
    own_att(3)
    for n in BOTH:
        w_loads[n].wait()
        w_swaps[n].wait_recv()
    stages = (s2, s3, s4, s5, s6, s7, s8, s9, s10)
    first = (0, 4, 8, 9)
    for tick in range(first[-1] + len(stages)):
        for r in range(chunks):
            n = tick - first[r]
            if 0 <= n < len(stages):
                stages[n](r)
        if tick == first[1] - 1:
            forward(2)
        if tick == first[2] - 1:
            forward(3)

    for swap in w_swaps + x_swaps:
        swap.wait_send()
    for k in range(ty_size):
        @pl.when(jnp.logical_not(a2a_self(k)))
        def _():
            a2a(k).wait_send()
    for r in range(chunks):
        for a in BOTH:
            for b in BOTH:
                for side in BOTH:
                    gather(r, a, b, side).wait_send()
                    for level in BOTH:
                        spread(level, r, a, b, side).wait_send()
        for level in BOTH:
            for c in BOTH:
                for kind in KINDS:
                    for side in BOTH:
                        hop(level, r, c, kind, side).wait_send()
        for p in range(RING):
            out_copy(r, p).wait()
            out_swap(r, p).wait()


def combine(att_owned, act_own, x_blk, w_out, w_down, ty_size):
    seq_block = att_owned.shape[1]
    chunks = ty_size // 4
    group, half_ty = 2 * seq_block, ty_size // 2
    cols = w_out.shape[1]
    per = half_ty // chunks
    ffn, q_width = w_down.shape[0], w_out.shape[0]
    crows = RING * per * group
    blk, sub, hcols = crows // RING, crows // RING // RING, cols // 2
    any_spec = pl.BlockSpec(memory_space=pl.ANY)
    ring_bufs = []
    for m in (blk, sub):
        ring_bufs += [
            pltpu.VMEM((chunks, TWO, m, cols), BF16),
            pltpu.VMEM((chunks, TWO, TWO, m, hcols), BF16),
            pltpu.VMEM((chunks, TWO, TWO, m, hcols), BF16),
            pltpu.VMEM((chunks, TWO, TWO, m, hcols), BF16),
            pltpu.VMEM((chunks, TWO, TWO, TWO, m, hcols), BF16),
        ]
    dma = pltpu.SemaphoreType.DMA
    y = pl.pallas_call(
        functools.partial(combine_kernel, ty_size, chunks),
        out_shape=jax.ShapeDtypeStruct((TWO, half_ty, RING, TWO, seq_block, cols), BF16),
        in_specs=[any_spec] * 5,
        out_specs=any_spec,
        scratch_shapes=[
            pltpu.VMEM((chunks, RING, per, TWO, seq_block, q_width), BF16),
            pltpu.VMEM((chunks, RING, per, group, ffn), BF16),
            pltpu.VMEM((q_width, TWO * cols), BF16),
            pltpu.VMEM((ffn, TWO * cols), BF16),
            pltpu.VMEM((chunks, crows, TWO * cols), F32),
            pltpu.VMEM((chunks, TWO, blk, cols), F32),
            pltpu.VMEM((TWO, chunks, seq_block, cols), BF16),
            pltpu.VMEM((chunks, TWO, RING, TWO, TWO, seq_block, cols), BF16),
            *ring_bufs,
            dma((CORES,)), dma((CORES,)), dma((CORES,)),
            dma((ty_size,)), dma((half_ty, TWO)),
            dma((chunks,)),
            dma((chunks, TWO, TWO, TWO)), dma((chunks, TWO, TWO, TWO)),
            dma((chunks,)), dma((chunks,)), dma((chunks,)),
            dma((TWO, chunks, TWO, len(KINDS), TWO)), dma((TWO, chunks, TWO, len(KINDS), TWO)),
            dma((TWO, chunks, TWO, TWO, TWO)), dma((TWO, chunks, TWO, TWO, TWO)),
            dma((chunks, RING)), dma((chunks, RING)), dma((chunks, RING)),
        ],
        compiler_params=pltpu.CompilerParams(
            collective_id=1, has_side_effects=True, vmem_limit_bytes=60 * MIB
        ),
        name="combine",
    )(
        att_owned,
        act_own.reshape(chunks, per, group, ffn),
        x_blk.reshape(TWO, half_ty, RING, TWO, seq_block, cols),
        w_out,
        w_down,
    )
    return y.reshape(x_blk.shape)


def solution(mesh):
    ty_size = mesh.shape["ty"]
    tx_size = mesh.shape["tx"]
    cache_spec = P(("dp", "ty", "tx"), None, None)

    def layer_shard(x_blk, lens_part, k_blk, v_blk, gamma_blk, w_query, w_key, w_value, w_gate, w_up, w_out, w_down):
        rows = x_blk.shape[0]
        d_model = x_blk.shape[1] * tx_size
        seq_block, ctx_len, head_dim = k_blk.shape
        half_ty, group = ty_size // 2, 2 * seq_block
        local_heads = w_query.shape[1] // head_dim
        row_idx = lax.axis_index("ty")
        col_idx = lax.axis_index("tx")
        ring_pos, core = col_idx // 2, col_idx % 2
        tile = min(256, w_gate.shape[1])

        lens_q = lax.dynamic_slice(lens_part.reshape(2, half_ty, RING, group), (core, 0, ring_pos, 0), (1, half_ty, 1, group))
        cos_q, sin_q = rope_tables(lens_q.reshape(-1), head_dim)
        block_start = (row_idx * tx_size + col_idx) * seq_block
        lens_own = lax.dynamic_slice_in_dim(lens_part, block_start, seq_block)
        lens_kv = lax.dynamic_slice_in_dim(lens_part, (row_idx * RING + ring_pos) * group, group)
        cos_kv, sin_kv = rope_tables(jnp.where(core == 0, lens_kv, 0), head_dim)

        act_own, q_owned, kv_new = project(
            x_blk, gamma_blk, w_query, w_key, w_value, w_gate, w_up, cos_q, sin_q, cos_kv, sin_kv,
            ty_size, seq_block, d_model, tile,
        )
        kv_own = lax.dynamic_slice_in_dim(kv_new, core * seq_block, seq_block, axis=1)
        positions = jnp.arange(ctx_len)
        at_slot = positions[None, :, None] == lens_own[:, None, None]
        k_out = jnp.where(at_slot, kv_own[0][:, None, :], k_blk)
        v_out = jnp.where(at_slot, kv_own[1][:, None, :], v_blk)

        q_owned = q_owned.reshape(ty_size, seq_block, local_heads, head_dim)
        scores = jnp.einsum("gbhd,btd->gbht", q_owned, k_out, preferred_element_type=F32) * (head_dim ** -0.5)
        in_range = positions[None, None, None, :] <= lens_own[None, :, None, None]
        scores = jnp.where(in_range, scores, -1e30)
        att_probs = jax.nn.softmax(scores, axis=-1).astype(BF16)
        att_owned = jnp.einsum("gbht,btd->gbhd", att_probs, v_out, preferred_element_type=F32).astype(BF16)
        att_owned = att_owned.reshape(ty_size, seq_block, local_heads * head_dim)
        y_blk = combine(att_owned, act_own, x_blk, w_out, w_down, ty_size)
        return y_blk, k_out, v_out

    in_specs = (P("dp", "tx"), P("dp"), cache_spec, cache_spec, P("tx"), P("tx", "ty"), P("tx", None), P("tx", None), P("tx", "ty"), P("tx", "ty"), P("ty", "tx"), P("ty", "tx"))
    out_specs = (P("dp", "tx"), cache_spec, cache_spec)
    return jax.shard_map(layer_shard, mesh=mesh, in_specs=in_specs, out_specs=out_specs, check_vma=False)
```

```python
import functools

import jax
import jax.numpy as jnp
from jax import lax
from jax.experimental import pallas as pl
from jax.experimental.pallas import tpu as pltpu
from jax.sharding import PartitionSpec as P

EPSILON = 1e-6
ROPE_BASE = 10000.0
MESH = pl.DeviceIdType.MESH
RING = 4
CORES = 2
TWO = 2
LANES = 128
BOTH = (0, 1)
KINDS = (0, 1, 2)
MIB = 2**20
ORDER = "2030400250216003317041802251902332611033427143" + "528153629163721173828392931213"
F32 = jnp.float32
BF16 = jnp.bfloat16


def inverse_freqs(head_dim):
    half_dim = head_dim // 2
    freqs = ROPE_BASE ** (-(jnp.arange(half_dim, dtype=F32) * 2.0) / head_dim)
    return jnp.concatenate([freqs, freqs])[None, :]


def remote(src, dst, send_sem, recv_sem, ty, tx):
    return pltpu.make_async_remote_copy(
        src_ref=src, dst_ref=dst, send_sem=send_sem, recv_sem=recv_sem,
        device_id={"ty": ty, "tx": tx}, device_id_type=MESH,
    )


def project_kernel(
    ty_size, tile, d_model,
    x_main, x_kv, wq, wk, wv, wg, wu, gamma, lens, freqs,
    act_out, q_out, kv_out,
    xs, ws, wkvs, gam, st, sr, p2, sd, sb, ra, rb, act, kvs, kvr, kvf, qs, qr,
    load_sem, pair_send, pair_recv, st_send, st_recv, ssem, rsem, kv_ssem, kv_rsem, kvf_sem, q_ssem, q_rsem, out_sem,
):
    row_idx = lax.axis_index("ty")
    col_idx = lax.axis_index("tx")
    ring_pos, core = col_idx // 2, col_idx % 2
    other = 1 - core
    half_ty = ty_size // 2
    group = xs.shape[1]
    seq_block = group // 2
    rows = half_ty * group
    hrows = rows // 2
    hg = half_ty // 2
    kdim = xs.shape[2]
    kblk = kdim // 2
    steps = wg.shape[1] // tile
    head_dim = freqs.shape[1]
    q_width = wq.shape[1]
    pos_p, pos_m, pos_o = (ring_pos + 1) % RING, (ring_pos + RING - 1) % RING, (ring_pos + 2) % RING
    tx_p, tx_m, tx_o = pos_p * 2 + core, pos_m * 2 + core, pos_o * 2 + core
    tx_pair = ring_pos * 2 + other
    lanes = pl.ds(pl.multiple_of(core * kblk, LANES), kblk)
    krows = pl.ds(pl.multiple_of(core * kblk, LANES), kblk)

    pieces = []
    for d in range(RING):
        pieces.append((lambda c, d=d: x_main.at[c, :, d], xs.at[pl.ds(d * half_ty, half_ty), :, lanes]))
    pieces.append((lambda c: x_kv.at[row_idx], xs.at[pl.ds(RING * half_ty, RING), :, lanes]))
    pieces.append((lambda c: gamma, gam.at[:, lanes]))
    pieces.append((lambda c: wq, ws.at[0, krows, pl.ds(0, q_width)]))
    kv_piece = len(pieces)
    pieces.append((lambda c: wk, wkvs.at[krows]))
    for t in range(steps):
        pieces.append((lambda c, t=t: wg.at[:, pl.ds(t * tile, tile)], ws.at[t + 1, krows, pl.ds(0, tile)]))
        pieces.append((lambda c, t=t: wu.at[:, pl.ds(t * tile, tile)], ws.at[t + 1, krows, pl.ds(tile, tile)]))
    loads = [pltpu.make_async_copy(src(core), dst, load_sem.at[n]) for n, (src, dst) in enumerate(pieces)]
    swaps = [remote(src(other), dst, pair_send.at[n], pair_recv.at[n], row_idx, tx_pair) for n, (src, dst) in enumerate(pieces)]
    def start(copies, kv_copies, wants):
        for n, copy in enumerate(copies):
            if n != kv_piece:
                copy.start()
            else:
                for which in BOTH:
                    pl.when(wants == which)(kv_copies[which].start)

    start(loads, [pltpu.make_async_copy(w, wkvs.at[krows], load_sem.at[kv_piece]) for w in (wk, wv)], core)
    st[...] = jnp.zeros_like(st)

    barrier = pltpu.get_barrier_semaphore()
    pl.semaphore_signal(barrier, device_id={"ty": row_idx, "tx": tx_pair}, device_id_type=MESH)
    for tx in (tx_p, tx_m, tx_o):
        pl.semaphore_signal(barrier, device_id={"ty": row_idx, "tx": tx}, device_id_type=MESH)
    for off in range(1, ty_size):
        for cc in BOTH:
            pl.semaphore_signal(
                barrier, device_id={"ty": (row_idx + off) % ty_size, "tx": ring_pos * 2 + cc}, device_id_type=MESH
            )
    pl.semaphore_wait(barrier, 4 + 2 * (ty_size - 1))
    kv_swaps = [
        remote(w, wkvs.at[krows], pair_send.at[kv_piece], pair_recv.at[kv_piece], row_idx, tx_pair) for w in (wk, wv)
    ]
    start(swaps, kv_swaps, other)

    blk = 2 * group
    blocks = (RING * half_ty + RING) // 2
    lane_tiles = kdim // 128

    def add_stats(slab):
        def stat_block(b, _):
            def lane_tile(j, sums):
                tile_lanes = pl.ds(pl.multiple_of(slab * kblk + j * LANES, LANES), LANES)
                part = xs[pl.ds(2 * b, 2), :, tile_lanes].reshape(blk, LANES).astype(F32)
                return sums[0] + part, sums[1] + part * part
            zero = jnp.zeros((blk, LANES), F32)
            sums = lax.fori_loop(0, kblk // LANES, lane_tile, (zero, zero))
            for which in BOTH:
                line = pl.ds(b + which * (st.shape[0] // 2), 1)
                st[line, pl.ds(0, blk)] += jnp.sum(sums[which].T, axis=0, keepdims=True)
            return 0

        lax.fori_loop(0, blocks, stat_block, 0)

    for n in range(kv_piece - 1):
        loads[n].wait()
    add_stats(core)
    for n in range(kv_piece - 1):
        swaps[n].wait_recv()
    add_stats(other)
    stat_copies = [
        remote(st, sr.at[n], st_send.at[n], st_recv.at[n], row_idx, tx) for n, tx in enumerate((tx_p, tx_m, tx_o))
    ]
    for copy in stat_copies:
        copy.start()
    for copy in stat_copies:
        copy.wait()
    total = ((st[...] + sr[0]) + (sr[1] + sr[2]))
    mean = total[: st.shape[0] // 2] / d_model
    var = total[st.shape[0] // 2 :] / d_model - mean * mean
    sr[0, : st.shape[0] // 2, :] = mean
    sr[1, : st.shape[0] // 2, :] = lax.rsqrt(var + EPSILON)

    def norm_block(b, _):
        mean_b = jnp.broadcast_to(sr[0, pl.ds(b, 1), :], (128, LANES)).T[:blk]
        rstd_b = jnp.broadcast_to(sr[1, pl.ds(b, 1), :], (128, LANES)).T[:blk]
        for j in range(lane_tiles):
            cols = slice(j * 128, (j + 1) * LANES)
            part = xs[pl.ds(2 * b, 2), :, cols].reshape(blk, LANES).astype(F32)
            normed = ((part - mean_b) * rstd_b * gam[0:1, cols]).astype(BF16)
            xs[pl.ds(2 * b, 2), :, cols] = normed.reshape(2, group, LANES)
        return 0

    per_dest = half_ty // 2

    def norm_dest(d, count):
        lax.fori_loop(d * per_dest, d * per_dest + count, norm_block, 0)


    def left(start, count):
        return xs[pl.ds(start, count)].reshape(count * group, kdim)

    def mm(start, count, w):
        return jnp.dot(left(start, count), w, preferred_element_type=F32)

    def hop(s, n, kind, side):
        cols = pl.ds(0, n)
        src, dst = (
            (p2.at[s, pl.ds(side * hrows, hrows), cols], ra.at[s, side, :, cols]),
            (sd.at[s, side, :, cols], rb.at[s, side, 0, :, cols]),
            (sb.at[s, side, :, cols], rb.at[s, side, 1, :, cols]),
        )[kind]
        return remote(src, dst, ssem.at[s, kind, side], rsem.at[s, kind, side], row_idx, (tx_p, tx_m)[side])

    def stage_far(s, n):
        w = ws[s, :, 0:n]
        p2[s, :, 0:n] = mm(pos_o * half_ty, half_ty, w).astype(BF16)
        hop(s, n, 0, 0).start()
        hop(s, n, 0, 1).start()

    def stage_near(s, n):
        w = ws[s, :, 0:n]
        sd[s, 0, :, 0:n] = mm(pos_p * half_ty + hg, hg, w).astype(BF16)
        hop(s, n, 1, 0).start()
        sd[s, 1, :, 0:n] = mm(pos_m * half_ty, hg, w).astype(BF16)
        hop(s, n, 1, 1).start()

    def stage_a(s, n):
        stage_far(s, n)
        stage_near(s, n)

    def stage_b(s, n):
        w = ws[s, :, 0:n]
        for side, start in ((0, pos_p * half_ty), (1, pos_m * half_ty + hg)):
            own = mm(start, hg, w)
            hop(s, n, 0, side).wait_recv()
            sb[s, side, :, 0:n] = (own + ra[s, side, :, 0:n].astype(F32)).astype(BF16)
            hop(s, n, 2, side).start()

    def stage_c(s, n, finish):
        w = ws[s, :, 0:n]
        for half in BOTH:
            own = mm(ring_pos * half_ty + half * hg, hg, w)
            hop(s, n, 2, half).wait_recv()
            hop(s, n, 1, 1 - half).wait_recv()
            finish(half, own + rb[s, half, 1, :, 0:n].astype(F32) + rb[s, 1 - half, 0, :, 0:n].astype(F32))

    low = lax.broadcasted_iota(jnp.int32, (group, head_dim), 1) < head_dim // 2

    def tables(positions):
        angles = jnp.broadcast_to(positions.astype(F32), (head_dim, group)).T * freqs[...]
        sines = jnp.sin(angles)
        return jnp.cos(angles), jnp.where(low, -sines, sines)

    def turn(vals, cos2, sin2):
        return vals * cos2 + pltpu.roll(vals, head_dim // 2, 1) * sin2

    def finish_q(half, vals):
        for g in range(hg):
            cos2, sin2 = tables(lens[pl.ds((core * half_ty + half * hg + g) * RING + ring_pos, 1), :])
            for h in range(q_width // head_dim):
                cols = slice(h * head_dim, (h + 1) * head_dim)
                turned = turn(vals[g * group : (g + 1) * group, cols], cos2, sin2).astype(BF16)
                for k in BOTH:
                    qs[2 * (half * hg + g) + k, :, cols] = turned[k * seq_block : (k + 1) * seq_block]

    def finish_mlp(s):
        def finish(half, vals):
            gate = vals[:, :tile].astype(BF16).astype(F32)
            up = vals[:, tile:].astype(BF16).astype(F32)
            act[pl.ds(half * hrows, hrows), pl.ds(pl.multiple_of((s - 1) * tile, tile), tile)] = (
                gate * jax.nn.sigmoid(gate) * up
            ).astype(BF16)
        return finish

    def q_copy(k):
        return remote(
            qs.at[k], qr.at[row_idx], q_ssem.at[k], q_rsem.at[row_idx],
            core * half_ty + k // 2, ring_pos * 2 + k % 2,
        )

    def q_is_self(k):
        return jnp.logical_and(core * half_ty + k // 2 == row_idx, core == k % 2)

    def kv_copy(n, pos):
        return remote(kvs.at[pos], kvr.at[n], kv_ssem.at[n], kv_rsem.at[n], row_idx, pos * 2 + core)

    wide = 2 * tile
    norm_dest(pos_o, per_dest)
    for n in (kv_piece - 1, kv_piece):
        loads[n].wait()
        swaps[n].wait_recv()
    stage_far(0, q_width)
    norm_dest(pos_p, per_dest)
    norm_dest(pos_m, per_dest)
    stage_near(0, q_width)
    norm_dest(RING, 2)
    kvs[...] = mm(RING * half_ty, RING, wkvs[...]).reshape(kvs.shape)
    for n, pos in enumerate((pos_p, pos_m, pos_o)):
        kv_copy(n, pos).start()
    norm_dest(ring_pos, per_dest)
    for n in range(kv_piece + 1, len(loads)):
        loads[n].wait()
        swaps[n].wait_recv()
    stage_a(1, wide)
    stage_b(0, q_width)
    for n, pos in enumerate((pos_p, pos_m, pos_o)):
        kv_copy(n, pos).wait_recv()
    new_row = (kvs[ring_pos] + kvr[0]) + (kvr[1] + kvr[2])
    kvf[core] = turn(new_row, *tables(lens[pl.ds(row_idx * RING + ring_pos, 1), :] * other)).astype(BF16)
    kv_pair = remote(kvf.at[core], kvf.at[core], kvf_sem.at[0], kvf_sem.at[1], row_idx, tx_pair)
    kv_pair.start()
    stage_a(2, wide)
    stage_b(1, wide)
    stage_c(0, q_width, finish_q)
    for k in range(ty_size):
        @pl.when(q_is_self(k))
        def _():
            pltpu.make_async_copy(qs.at[k], qr.at[row_idx], q_rsem.at[row_idx]).start()

        @pl.when(jnp.logical_not(q_is_self(k)))
        def _():
            q_copy(k).start()

    def middle(s, _):
        stage_a(s, wide)
        stage_b(s - 1, wide)
        stage_c(s - 2, wide, finish_mlp(s - 2))
        return 0

    lax.fori_loop(3, steps + 1, middle, 0)
    stage_b(steps, wide)
    stage_c(steps - 1, wide, finish_mlp(steps - 1))
    stage_c(steps, wide, finish_mlp(steps))

    outs = [
        pltpu.make_async_copy(act, act_out, out_sem.at[0]),
        pltpu.make_async_copy(qr, q_out, out_sem.at[1]),
        pltpu.make_async_copy(kvf, kv_out, out_sem.at[2]),
    ]
    outs[0].start()
    for k in range(ty_size):
        remote(qs.at[0], qr.at[k], q_ssem.at[0], q_rsem.at[k], row_idx, tx_pair).wait_recv()
    outs[1].start()
    kv_pair.wait_send()
    remote(kvf.at[other], kvf.at[other], kvf_sem.at[0], kvf_sem.at[1], row_idx, tx_pair).wait_recv()
    outs[2].start()
    for k in range(ty_size):
        @pl.when(jnp.logical_not(q_is_self(k)))
        def _():
            q_copy(k).wait_send()
    for n, pos in enumerate((pos_p, pos_m, pos_o)):
        kv_copy(n, pos).wait_send()
    for swap in swaps:
        swap.wait_send()
    for kind in KINDS:
        for side in BOTH:
            hop(0, q_width, kind, side).wait_send()

    def drain(s, _):
        for kind in KINDS:
            for side in BOTH:
                hop(s, wide, kind, side).wait_send()
        return 0

    lax.fori_loop(1, steps + 1, drain, 0)
    for out in outs:
        out.wait()


def project(x_blk, gamma_blk, wq, wk, wv, wg, wu, lens, head_dim, ty_size, seq_block, d_model, tile):
    rows_all, kblk = x_blk.shape
    half_ty, group = ty_size // TWO, TWO * seq_block
    rows = half_ty * group
    q_width, ffn = wq.shape[1], wg.shape[1]
    kv_width = wk.shape[1]
    steps = ffn // tile
    wide = 2 * tile
    kdim = 2 * kblk
    x_main = x_blk.reshape(TWO, half_ty, RING, group, kblk)
    x_kv = x_blk.reshape(ty_size, RING, group, kblk)
    pieces = RING + 4 + 2 * steps
    stat_lines = 2 * (-(-((RING * half_ty + RING) // TWO) // 8) * 8)
    any_spec = pl.BlockSpec(memory_space=pl.ANY)
    vmem_spec = pl.BlockSpec(memory_space=pltpu.VMEM)
    return pl.pallas_call(
        functools.partial(project_kernel, ty_size, tile, d_model),
        out_shape=(
            jax.ShapeDtypeStruct((rows, ffn), BF16),
            jax.ShapeDtypeStruct((ty_size, seq_block, q_width), BF16),
            jax.ShapeDtypeStruct((TWO, group, kv_width), BF16),
        ),
        in_specs=[any_spec] * 8 + [vmem_spec] * 2,
        out_specs=(any_spec,) * 3,
        scratch_shapes=[
            pltpu.VMEM((RING * half_ty + RING, group, kdim), BF16),
            pltpu.VMEM((steps + 1, kdim, wide), BF16),
            pltpu.VMEM((kdim, kv_width), BF16),
            pltpu.VMEM((1, kdim), F32),
            pltpu.VMEM((stat_lines, LANES), F32),
            pltpu.VMEM((3, stat_lines, LANES), F32),
            pltpu.VMEM((steps + 1, rows, wide), BF16),
            pltpu.VMEM((steps + 1, TWO, rows // TWO, wide), BF16),
            pltpu.VMEM((steps + 1, TWO, rows // TWO, wide), BF16),
            pltpu.VMEM((steps + 1, TWO, rows // TWO, wide), BF16),
            pltpu.VMEM((steps + 1, TWO, TWO, rows // TWO, wide), BF16),
            pltpu.VMEM((rows, ffn), BF16),
            pltpu.VMEM((RING, group, kv_width), F32),
            pltpu.VMEM((3, group, kv_width), F32),
            pltpu.VMEM((TWO, group, kv_width), BF16),
            pltpu.VMEM((ty_size, seq_block, q_width), BF16),
            pltpu.VMEM((ty_size, seq_block, q_width), BF16),
            pltpu.SemaphoreType.DMA((pieces,)),
            pltpu.SemaphoreType.DMA((pieces,)),
            pltpu.SemaphoreType.DMA((pieces,)),
            pltpu.SemaphoreType.DMA((len(KINDS),)),
            pltpu.SemaphoreType.DMA((len(KINDS),)),
            pltpu.SemaphoreType.DMA((steps + 1, len(KINDS), TWO)),
            pltpu.SemaphoreType.DMA((steps + 1, len(KINDS), TWO)),
            pltpu.SemaphoreType.DMA((len(KINDS),)),
            pltpu.SemaphoreType.DMA((len(KINDS),)),
            pltpu.SemaphoreType.DMA((TWO,)),
            pltpu.SemaphoreType.DMA((ty_size,)),
            pltpu.SemaphoreType.DMA((ty_size,)),
            pltpu.SemaphoreType.DMA((len(KINDS),)),
        ],
        compiler_params=pltpu.CompilerParams(
            collective_id=0, has_side_effects=True, vmem_limit_bytes=56 * MIB
        ),
        name="project",
    )(
        x_main, x_kv, wq, wk, wv, wg, wu, gamma_blk[None, :], lens.reshape(-1, group), inverse_freqs(head_dim)
    )


def combine_kernel(
    ty_size, chunks,
    att_in, act_in, x_in, wo, wd,
    y_out,
    att, mlp, wos, wds, yp, t1, xr, yf, p2_1, sd_1, sb_1, ra_1, rb_1, p2_2, sd_2, sb_2, ra_2, rb_2,
    w_sem, wp_send, wp_recv, a2a_send, a2a_recv, mlp_sem, gx_send, gx_recv, x_sem, xp_send, xp_recv,
    rs_send, rs_recv, ag_send, ag_recv, out_sem, outp_send, outp_recv,
):
    row_idx = lax.axis_index("ty")
    col_idx = lax.axis_index("tx")
    ring_pos, core = col_idx // 2, col_idx % 2
    other = 1 - core
    half_ty = ty_size // 2
    seq_block = att_in.shape[1]
    cols = wo.shape[1]
    hcols = cols // 2
    pos_p, pos_m = (ring_pos + 1) % RING, (ring_pos + RING - 1) % RING
    tx_side = (pos_p * 2 + core, pos_m * 2 + core)
    from_side = (pos_m, pos_p)
    tx_pair = ring_pos * 2 + other
    z_pos, y_pos = row_idx // RING, row_idx % RING
    up = lambda v: (v + 1) % RING
    down = lambda v: (v + RING - 1) % RING
    y_side = (z_pos * RING + up(y_pos), z_pos * RING + down(y_pos))
    z_side = (up(z_pos) * RING + y_pos, down(z_pos) * RING + y_pos)
    places = ((y_pos, z_pos), (z_pos, y_pos))
    sides = ((y_side, z_side), (z_side, y_side))
    blk = yp.shape[1] // RING
    sub = blk // RING
    mine = pl.ds(pl.multiple_of(core * cols, LANES), cols)

    def x_tile(c, r):
        b1, b2 = jnp.where(core == 0, y_pos, z_pos), jnp.where(core == 0, z_pos, y_pos)
        return x_in.at[c, 2 * r + b2 // 2, b1, b2 % 2]

    w_loads = [pltpu.make_async_copy(wd, wds.at[:, mine], w_sem.at[0]), pltpu.make_async_copy(wo, wos.at[:, mine], w_sem.at[1])]
    w_swaps = [
        remote(wd, wds.at[:, mine], wp_send.at[0], wp_recv.at[0], row_idx, tx_pair),
        remote(wo, wos.at[:, mine], wp_send.at[1], wp_recv.at[1], row_idx, tx_pair),
    ]
    mlp_loads = [pltpu.make_async_copy(act_in.at[r], mlp.at[r, ring_pos], mlp_sem.at[r]) for r in range(chunks)]
    x_loads = [pltpu.make_async_copy(x_tile(core, r), xr.at[core, r], x_sem.at[r]) for r in range(chunks)]
    x_swaps = [remote(x_tile(other, r), xr.at[core, r], xp_send.at[r], xp_recv.at[r], row_idx, tx_pair) for r in range(chunks)]
    for load in w_loads + mlp_loads + x_loads:
        load.start()

    barrier = pltpu.get_barrier_semaphore()
    pl.semaphore_signal(barrier, device_id={"ty": row_idx, "tx": tx_pair}, device_id_type=MESH)
    for tx in tx_side:
        pl.semaphore_signal(barrier, device_id={"ty": row_idx, "tx": tx}, device_id_type=MESH)
    for off in range(1, ty_size):
        for cc in BOTH:
            pl.semaphore_signal(
                barrier, device_id={"ty": (row_idx + off) % ty_size, "tx": ring_pos * 2 + cc}, device_id_type=MESH
            )
    pl.semaphore_wait(barrier, 3 + 2 * (ty_size - 1))

    def gather(r, part, stage, side):
        sems = gx_send.at[r, part, stage, side], gx_recv.at[r, part, stage, side]
        buf = (mlp, att)[part]
        if stage == 0:
            src = act_in.at[r] if part == 0 else att.at[r, ring_pos]
            return remote(src, buf.at[r, ring_pos], *sems, row_idx, tx_side[side])
        block = buf.at[r, from_side[side], side]
        return remote(block, block, *sems, row_idx, tx_side[side])

    home, home_core = row_idx % half_ty, row_idx // half_ty

    def a2a(k):
        return remote(
            att_in.at[k], att.at[home // 2, ring_pos, home % 2, core], a2a_send.at[k], a2a_recv.at[home, core],
            k, ring_pos * 2 + home_core,
        )

    def a2a_self(k):
        return jnp.logical_and(k == row_idx, core == home_core)

    for side in BOTH:
        gather(0, 0, 0, side).start()
    for k in range(ty_size):
        @pl.when(a2a_self(k))
        def _():
            pltpu.make_async_copy(
                att_in.at[k], att.at[home // 2, ring_pos, home % 2, core], a2a_recv.at[home, core]
            ).start()

        @pl.when(jnp.logical_not(a2a_self(k)))
        def _():
            a2a(k).start()
    for swap in w_swaps + x_swaps:
        swap.start()

    def att_ready(r):
        for g in (2 * r, 2 * r + 1):
            for cc in BOTH:
                remote(
                    att_in.at[0], att.at[r, ring_pos, g % 2, cc], a2a_send.at[0], a2a_recv.at[g, cc], row_idx, tx_pair
                ).wait_recv()

    def own_att(r):
        att_ready(r)
        for side in BOTH:
            gather(r, 1, 0, side).start()

    def own_mlp(r):
        for side in BOTH:
            gather(r, 0, 0, side).start()

    def forward(r):
        for part in BOTH:
            for side in BOTH:
                gather(r, part, 0, side).wait_recv()
                gather(r, part, 1, side).start()

    def multiply(r):
        mlp_loads[r].wait()
        for part in BOTH:
            for side in BOTH:
                gather(r, part, 1, side).wait_recv()
        rows = yp.shape[1]

        def tile(n, _):
            lanes = pl.ds(pl.multiple_of(n * 512, 512), 512)
            left_mlp = mlp[r].reshape(rows, mlp.shape[-1])
            left_att = att[r].reshape(rows, att.shape[-1])
            yp[r, :, lanes] = jnp.dot(left_mlp, wds[:, lanes], preferred_element_type=F32) + jnp.dot(
                left_att, wos[:, lanes], preferred_element_type=F32
            )
            return 0

        lax.fori_loop(0, yp.shape[2] // 512, tile, 0)

    bufs = ((p2_1, sd_1, sb_1, ra_1, rb_1), (p2_2, sd_2, sb_2, ra_2, rb_2))

    def hop(level, r, c, kind, side):
        p2, sd, sb, ra, rb = bufs[level]
        src, dst = (
            (p2.at[r, c, :, pl.ds(side * hcols, hcols)], ra.at[r, c, side]),
            (sd.at[r, c, side], rb.at[r, c, side, 0]),
            (sb.at[r, c, side], rb.at[r, c, side, 1]),
        )[kind]
        return remote(
            src, dst, rs_send.at[level, r, c, kind, side], rs_recv.at[level, r, c, kind, side],
            sides[c][level][side], col_idx,
        )

    def part_of(level, r, c, b, half):
        size = (blk, sub)[level]
        rows = pl.ds(pl.multiple_of(b * size, 8), size)
        if level == 0:
            return yp[r, rows, c * cols + half * hcols : c * cols + (half + 1) * hcols]
        return t1[r, c, rows, half * hcols : (half + 1) * hcols]

    def reduce_a(level, r):
        p2, sd = bufs[level][:2]
        for c in BOTH:
            pos = places[c][level]
            for half in BOTH:
                p2[r, c, :, half * hcols : (half + 1) * hcols] = part_of(level, r, c, (pos + 2) % RING, half).astype(BF16)
                hop(level, r, c, 0, half).start()
        for c in BOTH:
            pos = places[c][level]
            sd[r, c, 0] = part_of(level, r, c, up(pos), 1).astype(BF16)
            hop(level, r, c, 1, 0).start()
            sd[r, c, 1] = part_of(level, r, c, down(pos), 0).astype(BF16)
            hop(level, r, c, 1, 1).start()

    def reduce_b(level, r):
        sb, ra = bufs[level][2:4]
        for c in BOTH:
            pos = places[c][level]
            for side, b in ((0, up(pos)), (1, down(pos))):
                hop(level, r, c, 0, side).wait_recv()
                sb[r, c, side] = (part_of(level, r, c, b, side) + ra[r, c, side].astype(F32)).astype(BF16)
                hop(level, r, c, 2, side).start()

    def reduce_c(level, r, finish):
        rb = bufs[level][4]
        for c in BOTH:
            pos = places[c][level]
            for half in BOTH:
                hop(level, r, c, 1, 1 - half).wait_recv()
                hop(level, r, c, 2, half).wait_recv()
                finish(
                    c, half,
                    part_of(level, r, c, pos, half) + rb[r, c, half, 1].astype(F32) + rb[r, c, 1 - half, 0].astype(F32),
                )

    def spread(level, r, c, stage, side):
        ring, (p1, p2) = sides[c][level], places[c]
        sems = ag_send.at[level, r, c, stage, side], ag_recv.at[level, r, c, stage, side]
        near = (down, up)[side]
        if level == 1:
            if stage == 0:
                block = yf.at[r, c, p1, p2 // 2, p2 % 2]
            else:
                block = yf.at[r, c, p1, near(p2) // 2, near(p2) % 2, :, pl.ds(side * hcols, hcols)]
        elif stage == 0:
            block = yf.at[r, c, p1]
        else:
            block = yf.at[r, c, near(p1), side]
        return remote(block, block, *sems, ring[side], col_idx)

    def spread_own(level, r):
        for c in BOTH:
            for side in BOTH:
                spread(level, r, c, 0, side).start()

    def spread_on(level, r):
        for c in BOTH:
            for side in BOTH:
                spread(level, r, c, 0, side).wait_recv()
                spread(level, r, c, 1, side).start()

    def spread_end(level, r):
        for c in BOTH:
            for side in BOTH:
                spread(level, r, c, 1, side).wait_recv()

    def s3(r):
        reduce_b(0, r)

    def s4(r):
        def finish(c, half, vals):
            t1[r, c, :, half * hcols : (half + 1) * hcols] = vals
        reduce_c(0, r, finish)
        reduce_a(1, r)

    def s5(r):
        reduce_b(1, r)

    def s6(r):
        x_loads[r].wait()
        remote(x_tile(other, r), xr.at[other, r], xp_send.at[r], xp_recv.at[r], row_idx, tx_pair).wait_recv()

        def finish(c, half, vals):
            lanes = slice(half * hcols, (half + 1) * hcols)
            p1, p2 = places[c]
            yf[r, c, p1, p2 // 2, p2 % 2, :, lanes] = (xr[c, r, :, lanes].astype(F32) + vals).astype(BF16)
        reduce_c(1, r, finish)
        spread_own(1, r)

    def s7(r):
        spread_on(1, r)

    def s8(r):
        spread_end(1, r)
        spread_own(0, r)

    def s9(r):
        spread_on(0, r)

    def out_copy(r, p):
        return pltpu.make_async_copy(
            yf.at[r, core, p], y_out.at[core, pl.ds(2 * r, 2), p], out_sem.at[r, p]
        )

    def out_swap(r, p):
        return remote(
            yf.at[r, other, p], y_out.at[core, pl.ds(2 * r, 2), p],
            outp_send.at[r, p], outp_recv.at[r, p], row_idx, tx_pair,
        )

    def s10(r):
        spread_end(0, r)
        for p in range(RING):
            out_swap(r, p).start()
            out_copy(r, p).start()

    def s2(r):
        multiply(r)
        reduce_a(0, r)

    own_mlp(1)
    own_att(0)
    own_att(1)
    forward(0)
    own_mlp(2)
    own_att(2)
    forward(1)
    own_mlp(3)
    own_att(3)
    for n in BOTH:
        w_loads[n].wait()
        w_swaps[n].wait_recv()
    stages = (forward, s10, s2, s3, s4, s5, s6, s7, s8, s9)
    for stage, r in zip(ORDER[0::TWO], ORDER[1::TWO]):
        stages[int(stage)](int(r))

    for swap in w_swaps + x_swaps:
        swap.wait_send()
    for k in range(ty_size):
        @pl.when(jnp.logical_not(a2a_self(k)))
        def _():
            a2a(k).wait_send()
    for r in range(chunks):
        for a in BOTH:
            for b in BOTH:
                for side in BOTH:
                    gather(r, a, b, side).wait_send()
                    for level in BOTH:
                        spread(level, r, a, b, side).wait_send()
        for level in BOTH:
            for c in BOTH:
                for kind in KINDS:
                    for side in BOTH:
                        hop(level, r, c, kind, side).wait_send()
        for p in range(RING):
            out_copy(r, p).wait()
            out_swap(r, p).wait()


def combine(att_owned, act_own, x_blk, w_out, w_down, ty_size):
    seq_block = att_owned.shape[1]
    chunks = ty_size // 4
    group, half_ty = 2 * seq_block, ty_size // 2
    cols = w_out.shape[1]
    per = half_ty // chunks
    ffn, q_width = w_down.shape[0], w_out.shape[0]
    crows = RING * per * group
    blk, sub, hcols = crows // RING, crows // RING // RING, cols // 2
    any_spec = pl.BlockSpec(memory_space=pl.ANY)
    ring_bufs = []
    for m in (blk, sub):
        ring_bufs += [
            pltpu.VMEM((chunks, TWO, m, cols), BF16),
            pltpu.VMEM((chunks, TWO, TWO, m, hcols), BF16),
            pltpu.VMEM((chunks, TWO, TWO, m, hcols), BF16),
            pltpu.VMEM((chunks, TWO, TWO, m, hcols), BF16),
            pltpu.VMEM((chunks, TWO, TWO, TWO, m, hcols), BF16),
        ]
    dma = pltpu.SemaphoreType.DMA
    y = pl.pallas_call(
        functools.partial(combine_kernel, ty_size, chunks),
        out_shape=jax.ShapeDtypeStruct((TWO, half_ty, RING, TWO, seq_block, cols), BF16),
        in_specs=[any_spec] * 5,
        out_specs=any_spec,
        scratch_shapes=[
            pltpu.VMEM((chunks, RING, per, TWO, seq_block, q_width), BF16),
            pltpu.VMEM((chunks, RING, per, group, ffn), BF16),
            pltpu.VMEM((q_width, TWO * cols), BF16),
            pltpu.VMEM((ffn, TWO * cols), BF16),
            pltpu.VMEM((chunks, crows, TWO * cols), F32),
            pltpu.VMEM((chunks, TWO, blk, cols), F32),
            pltpu.VMEM((TWO, chunks, seq_block, cols), BF16),
            pltpu.VMEM((chunks, TWO, RING, TWO, TWO, seq_block, cols), BF16),
            *ring_bufs,
            dma((CORES,)), dma((CORES,)), dma((CORES,)),
            dma((ty_size,)), dma((half_ty, TWO)),
            dma((chunks,)),
            dma((chunks, TWO, TWO, TWO)), dma((chunks, TWO, TWO, TWO)),
            dma((chunks,)), dma((chunks,)), dma((chunks,)),
            dma((TWO, chunks, TWO, len(KINDS), TWO)), dma((TWO, chunks, TWO, len(KINDS), TWO)),
            dma((TWO, chunks, TWO, TWO, TWO)), dma((TWO, chunks, TWO, TWO, TWO)),
            dma((chunks, RING)), dma((chunks, RING)), dma((chunks, RING)),
        ],
        compiler_params=pltpu.CompilerParams(
            collective_id=1, has_side_effects=True, vmem_limit_bytes=60 * MIB
        ),
        name="combine",
    )(
        att_owned,
        act_own.reshape(chunks, per, group, ffn),
        x_blk.reshape(TWO, half_ty, RING, TWO, seq_block, cols),
        w_out,
        w_down,
    )
    return y.reshape(x_blk.shape)


def solution(mesh):
    ty_size = mesh.shape["ty"]
    tx_size = mesh.shape["tx"]
    cache_spec = P(("dp", "ty", "tx"), None, None)

    def layer_shard(x_blk, lens_part, k_blk, v_blk, gamma_blk, w_query, w_key, w_value, w_gate, w_up, w_out, w_down):
        rows = x_blk.shape[0]
        d_model = x_blk.shape[1] * tx_size
        seq_block, ctx_len, head_dim = k_blk.shape
        local_heads = w_query.shape[1] // head_dim
        row_idx = lax.axis_index("ty")
        col_idx = lax.axis_index("tx")
        ring_pos, core = col_idx // 2, col_idx % 2
        tile = min(256, w_gate.shape[1])

        block_start = (row_idx * tx_size + col_idx) * seq_block
        lens_own = lax.dynamic_slice_in_dim(lens_part, block_start, seq_block)
        act_own, q_owned, kv_new = project(
            x_blk, gamma_blk, w_query, w_key, w_value, w_gate, w_up, lens_part, head_dim,
            ty_size, seq_block, d_model, tile,
        )
        kv_own = lax.dynamic_slice_in_dim(kv_new, core * seq_block, seq_block, axis=1)
        positions = jnp.arange(ctx_len)
        at_slot = positions[None, :, None] == lens_own[:, None, None]
        k_out = jnp.where(at_slot, kv_own[0][:, None, :], k_blk)
        v_out = jnp.where(at_slot, kv_own[1][:, None, :], v_blk)

        q_owned = q_owned.reshape(ty_size, seq_block, local_heads, head_dim)
        scores = jnp.einsum("gbhd,btd->gbht", q_owned, k_out, preferred_element_type=F32) * (head_dim ** -0.5)
        in_range = positions[None, None, None, :] <= lens_own[None, :, None, None]
        scores = jnp.where(in_range, scores, -1e30)
        att_probs = jax.nn.softmax(scores, axis=-1).astype(BF16)
        att_owned = jnp.einsum("gbht,btd->gbhd", att_probs, v_out, preferred_element_type=F32).astype(BF16)
        att_owned = att_owned.reshape(ty_size, seq_block, local_heads * head_dim)
        y_blk = combine(att_owned, act_own, x_blk, w_out, w_down, ty_size)
        return y_blk, k_out, v_out

    in_specs = (P("dp", "tx"), P("dp"), cache_spec, cache_spec, P("tx"), P("tx", "ty"), P("tx", None), P("tx", None), P("tx", "ty"), P("tx", "ty"), P("ty", "tx"), P("ty", "tx"))
    out_specs = (P("dp", "tx"), cache_spec, cache_spec)
    return jax.shard_map(layer_shard, mesh=mesh, in_specs=in_specs, out_specs=out_specs, check_vma=False)
```

```python
import functools

import jax
import jax.numpy as jnp
from jax import lax
from jax.experimental import pallas as pl
from jax.experimental.pallas import tpu as pltpu
from jax.sharding import PartitionSpec as P

EPSILON = 1e-6
ROPE_BASE = 10000.0
MESH = pl.DeviceIdType.MESH
RING = 4
CORES = 2
TWO = 2
LANES = 128
TILE = 512
BOTH = (0, 1)
KINDS = (0, 1, 2)
MIB = 2**20
SIZES = (1, 2, 2, 2, 1)
ORDER = (
    "m1A0m0g1a0a1g0h0a2h1m2h2m3202130g2314041a3a451g35022h3616032"
    + "m42371g4h4423381522443903462539144637254738283649293t194t0t3"
    + "t2t4"
)
F32 = jnp.float32
BF16 = jnp.bfloat16


def inverse_freqs(head_dim):
    half_dim = head_dim // 2
    freqs = ROPE_BASE ** (-(jnp.arange(half_dim, dtype=F32) * 2.0) / head_dim)
    return jnp.concatenate([freqs, freqs])[None, :]


def remote(src, dst, send_sem, recv_sem, ty, tx):
    return pltpu.make_async_remote_copy(
        src_ref=src, dst_ref=dst, send_sem=send_sem, recv_sem=recv_sem,
        device_id={"ty": ty, "tx": tx}, device_id_type=MESH,
    )


def project_kernel(
    ty_size, tile, d_model,
    x_main, x_kv, wq, wk, wv, wg, wu, gamma, lens, freqs,
    act_out, q_out, kv_out,
    xs, ws, wkvs, gam, st, sr, p2, sd, sb, ra, rb, act, kvs, kvr, kvf, qs, qr,
    load_sem, pair_send, pair_recv, st_send, st_recv, ssem, rsem, kv_ssem, kv_rsem, kvf_sem, q_ssem, q_rsem, out_sem,
):
    row_idx = lax.axis_index("ty")
    col_idx = lax.axis_index("tx")
    ring_pos, core = col_idx // 2, col_idx % 2
    other = 1 - core
    half_ty = ty_size // 2
    group = xs.shape[1]
    seq_block = group // 2
    rows = half_ty * group
    hrows = rows // 2
    hg = half_ty // 2
    kdim = xs.shape[2]
    kblk = kdim // 2
    steps = wg.shape[1] // tile
    head_dim = freqs.shape[1]
    q_width = wq.shape[1]
    pos_p, pos_m, pos_o = (ring_pos + 1) % RING, (ring_pos + RING - 1) % RING, (ring_pos + 2) % RING
    tx_p, tx_m, tx_o = pos_p * 2 + core, pos_m * 2 + core, pos_o * 2 + core
    tx_pair = ring_pos * 2 + other
    lanes = pl.ds(pl.multiple_of(core * kblk, LANES), kblk)
    krows = pl.ds(pl.multiple_of(core * kblk, LANES), kblk)

    pieces = []
    for d in range(RING):
        pieces.append((lambda c, d=d: x_main.at[c, :, d], xs.at[pl.ds(d * half_ty, half_ty), :, lanes]))
    pieces.append((lambda c: x_kv.at[row_idx], xs.at[pl.ds(RING * half_ty, RING), :, lanes]))
    pieces.append((lambda c: gamma, gam.at[core]))
    pieces.append((lambda c: wq, ws.at[0, krows, pl.ds(0, q_width)]))
    kv_piece = len(pieces)
    pieces.append((lambda c: wk, wkvs.at[krows]))
    for t in range(steps):
        pieces.append((lambda c, t=t: wg.at[:, pl.ds(t * tile, tile)], ws.at[t + 1, krows, pl.ds(0, tile)]))
        pieces.append((lambda c, t=t: wu.at[:, pl.ds(t * tile, tile)], ws.at[t + 1, krows, pl.ds(tile, tile)]))
    loads = [pltpu.make_async_copy(src(core), dst, load_sem.at[n]) for n, (src, dst) in enumerate(pieces)]
    swaps = [remote(src(other), dst, pair_send.at[n], pair_recv.at[n], row_idx, tx_pair) for n, (src, dst) in enumerate(pieces)]
    def start(copies, kv_copies, wants):
        for n, copy in enumerate(copies):
            if n != kv_piece:
                copy.start()
            else:
                for which in BOTH:
                    pl.when(wants == which)(kv_copies[which].start)

    start(loads, [pltpu.make_async_copy(w, wkvs.at[krows], load_sem.at[kv_piece]) for w in (wk, wv)], core)
    st[...] = jnp.zeros_like(st)

    barrier = pltpu.get_barrier_semaphore()
    pl.semaphore_signal(barrier, device_id={"ty": row_idx, "tx": tx_pair}, device_id_type=MESH)
    for tx in (tx_p, tx_m, tx_o):
        pl.semaphore_signal(barrier, device_id={"ty": row_idx, "tx": tx}, device_id_type=MESH)
    for off in range(1, ty_size):
        for cc in BOTH:
            pl.semaphore_signal(
                barrier, device_id={"ty": (row_idx + off) % ty_size, "tx": ring_pos * 2 + cc}, device_id_type=MESH
            )
    pl.semaphore_wait(barrier, 4 + 2 * (ty_size - 1))
    kv_swaps = [
        remote(w, wkvs.at[krows], pair_send.at[kv_piece], pair_recv.at[kv_piece], row_idx, tx_pair) for w in (wk, wv)
    ]
    start(swaps, kv_swaps, other)

    blk = 2 * group
    blocks = (RING * half_ty + RING) // 2
    lane_tiles, slab_tiles = kdim // LANES, kblk // LANES

    def add_stats(slab):
        def stat_block(b, _):
            def lane_tile(j, sums):
                tile_lanes = pl.ds(pl.multiple_of(slab * kblk + j * LANES, LANES), LANES)
                part = xs[pl.ds(2 * b, 2), :, tile_lanes].reshape(blk, LANES).astype(F32)
                return sums[0] + part, sums[1] + part * part
            zero = jnp.zeros((blk, LANES), F32)
            sums = lax.fori_loop(0, kblk // LANES, lane_tile, (zero, zero))
            for which in BOTH:
                line = pl.ds(b + which * (st.shape[0] // 2), 1)
                st[line, pl.ds(0, blk)] += jnp.sum(sums[which].T, axis=0, keepdims=True)
            return 0

        lax.fori_loop(0, blocks, stat_block, 0)

    for n in range(kv_piece - 1):
        loads[n].wait()
    add_stats(core)
    for n in range(kv_piece - 1):
        swaps[n].wait_recv()
    add_stats(other)
    stat_copies = [
        remote(st, sr.at[n], st_send.at[n], st_recv.at[n], row_idx, tx) for n, tx in enumerate((tx_p, tx_m, tx_o))
    ]
    for copy in stat_copies:
        copy.start()
    for copy in stat_copies:
        copy.wait()
    total = ((st[...] + sr[0]) + (sr[1] + sr[2]))
    mean = total[: st.shape[0] // 2] / d_model
    var = total[st.shape[0] // 2 :] / d_model - mean * mean
    sr[0, : st.shape[0] // 2, :] = mean
    sr[1, : st.shape[0] // 2, :] = lax.rsqrt(var + EPSILON)

    def norm_block(b, _):
        mean_b = jnp.broadcast_to(sr[0, pl.ds(b, 1), :], (128, LANES)).T[:blk]
        rstd_b = jnp.broadcast_to(sr[1, pl.ds(b, 1), :], (128, LANES)).T[:blk]
        for j in range(lane_tiles):
            cols = slice(j * 128, (j + 1) * LANES)
            part = xs[pl.ds(2 * b, 2), :, cols].reshape(blk, LANES).astype(F32)
            normed = ((part - mean_b) * rstd_b * gam[j // slab_tiles, pl.ds(j % slab_tiles, 1), :]).astype(BF16)
            xs[pl.ds(2 * b, 2), :, cols] = normed.reshape(2, group, LANES)
        return 0

    per_dest = half_ty // 2

    def norm_dest(d, count):
        lax.fori_loop(d * per_dest, d * per_dest + count, norm_block, 0)


    def left(start, count):
        return xs[pl.ds(start, count)].reshape(count * group, kdim)

    def mm(start, count, w):
        return jnp.dot(left(start, count), w, preferred_element_type=F32)

    def hop(s, n, kind, side):
        cols = pl.ds(0, n)
        src, dst = (
            (p2.at[s, pl.ds(side * hrows, hrows), cols], ra.at[s, side, :, cols]),
            (sd.at[s, side, :, cols], rb.at[s, side, 0, :, cols]),
            (sb.at[s, side, :, cols], rb.at[s, side, 1, :, cols]),
        )[kind]
        return remote(src, dst, ssem.at[s, kind, side], rsem.at[s, kind, side], row_idx, (tx_p, tx_m)[side])

    def stage_far(s, n):
        w = ws[s, :, 0:n]
        p2[s, :, 0:n] = mm(pos_o * half_ty, half_ty, w).astype(BF16)
        hop(s, n, 0, 0).start()
        hop(s, n, 0, 1).start()

    def stage_near(s, n):
        w = ws[s, :, 0:n]
        sd[s, 0, :, 0:n] = mm(pos_p * half_ty + hg, hg, w).astype(BF16)
        hop(s, n, 1, 0).start()
        sd[s, 1, :, 0:n] = mm(pos_m * half_ty, hg, w).astype(BF16)
        hop(s, n, 1, 1).start()

    def stage_a(s, n):
        stage_far(s, n)
        stage_near(s, n)

    def stage_b(s, n):
        w = ws[s, :, 0:n]
        for side, start in ((0, pos_p * half_ty), (1, pos_m * half_ty + hg)):
            own = mm(start, hg, w)
            hop(s, n, 0, side).wait_recv()
            sb[s, side, :, 0:n] = (own + ra[s, side, :, 0:n].astype(F32)).astype(BF16)
            hop(s, n, 2, side).start()

    def stage_c(s, n, finish):
        w = ws[s, :, 0:n]
        for half in BOTH:
            own = mm(ring_pos * half_ty + half * hg, hg, w)
            hop(s, n, 2, half).wait_recv()
            hop(s, n, 1, 1 - half).wait_recv()
            finish(half, own + rb[s, half, 1, :, 0:n].astype(F32) + rb[s, 1 - half, 0, :, 0:n].astype(F32))

    low = lax.broadcasted_iota(jnp.int32, (group, head_dim), 1) < head_dim // 2

    def tables(positions):
        angles = jnp.broadcast_to(positions.astype(F32), (head_dim, group)).T * freqs[...]
        sines = jnp.sin(angles)
        return jnp.cos(angles), jnp.where(low, -sines, sines)

    def turn(vals, cos2, sin2):
        return vals * cos2 + pltpu.roll(vals, head_dim // 2, 1) * sin2

    def finish_q(half, vals):
        for g in range(hg):
            cos2, sin2 = tables(lens[pl.ds((core * half_ty + half * hg + g) * RING + ring_pos, 1), :])
            for h in range(q_width // head_dim):
                cols = slice(h * head_dim, (h + 1) * head_dim)
                turned = turn(vals[g * group : (g + 1) * group, cols], cos2, sin2).astype(BF16)
                for k in BOTH:
                    qs[2 * (half * hg + g) + k, :, cols] = turned[k * seq_block : (k + 1) * seq_block]

    def finish_mlp(s):
        def finish(half, vals):
            gate = vals[:, :tile].astype(BF16).astype(F32)
            up = vals[:, tile:].astype(BF16).astype(F32)
            act[pl.ds(half * hrows, hrows), pl.ds(pl.multiple_of((s - 1) * tile, tile), tile)] = (
                gate * jax.nn.sigmoid(gate) * up
            ).astype(BF16)
        return finish

    def q_copy(k):
        return remote(
            qs.at[k], qr.at[row_idx], q_ssem.at[k], q_rsem.at[row_idx],
            core * half_ty + k // 2, ring_pos * 2 + k % 2,
        )

    def q_is_self(k):
        return jnp.logical_and(core * half_ty + k // 2 == row_idx, core == k % 2)

    def kv_copy(n, pos):
        return remote(kvs.at[pos], kvr.at[n], kv_ssem.at[n], kv_rsem.at[n], row_idx, pos * 2 + core)

    wide = 2 * tile
    norm_dest(pos_o, per_dest)
    for n in (kv_piece - 1, kv_piece):
        loads[n].wait()
        swaps[n].wait_recv()
    stage_far(0, q_width)
    norm_dest(pos_p, per_dest)
    norm_dest(pos_m, per_dest)
    stage_near(0, q_width)
    norm_dest(RING, 2)
    kvs[...] = mm(RING * half_ty, RING, wkvs[...]).reshape(kvs.shape)
    for n, pos in enumerate((pos_p, pos_m, pos_o)):
        kv_copy(n, pos).start()
    norm_dest(ring_pos, per_dest)
    for n in range(kv_piece + 1, len(loads)):
        loads[n].wait()
        swaps[n].wait_recv()
    stage_a(1, wide)
    stage_b(0, q_width)
    for n, pos in enumerate((pos_p, pos_m, pos_o)):
        kv_copy(n, pos).wait_recv()
    new_row = (kvs[ring_pos] + kvr[0]) + (kvr[1] + kvr[2])
    kvf[core] = turn(new_row, *tables(lens[pl.ds(row_idx * RING + ring_pos, 1), :] * other)).astype(BF16)
    kv_pair = remote(kvf.at[core], kvf.at[core], kvf_sem.at[0], kvf_sem.at[1], row_idx, tx_pair)
    kv_pair.start()
    stage_a(2, wide)
    stage_b(1, wide)
    stage_c(0, q_width, finish_q)
    for k in range(ty_size):
        @pl.when(q_is_self(k))
        def _():
            pltpu.make_async_copy(qs.at[k], qr.at[row_idx], q_rsem.at[row_idx]).start()

        @pl.when(jnp.logical_not(q_is_self(k)))
        def _():
            q_copy(k).start()

    def middle(s, _):
        stage_a(s, wide)
        stage_b(s - 1, wide)
        stage_c(s - 2, wide, finish_mlp(s - 2))
        return 0

    lax.fori_loop(3, steps + 1, middle, 0)
    stage_b(steps, wide)
    stage_c(steps - 1, wide, finish_mlp(steps - 1))
    stage_c(steps, wide, finish_mlp(steps))

    outs = [
        pltpu.make_async_copy(act, act_out, out_sem.at[0]),
        pltpu.make_async_copy(qr, q_out, out_sem.at[1]),
        pltpu.make_async_copy(kvf, kv_out, out_sem.at[2]),
    ]
    outs[0].start()
    for k in range(ty_size):
        remote(qs.at[0], qr.at[k], q_ssem.at[0], q_rsem.at[k], row_idx, tx_pair).wait_recv()
    outs[1].start()
    kv_pair.wait_send()
    remote(kvf.at[other], kvf.at[other], kvf_sem.at[0], kvf_sem.at[1], row_idx, tx_pair).wait_recv()
    outs[2].start()
    for k in range(ty_size):
        @pl.when(jnp.logical_not(q_is_self(k)))
        def _():
            q_copy(k).wait_send()
    for n, pos in enumerate((pos_p, pos_m, pos_o)):
        kv_copy(n, pos).wait_send()
    for swap in swaps:
        swap.wait_send()
    for kind in KINDS:
        for side in BOTH:
            hop(0, q_width, kind, side).wait_send()

    def drain(s, _):
        for kind in KINDS:
            for side in BOTH:
                hop(s, wide, kind, side).wait_send()
        return 0

    lax.fori_loop(1, steps + 1, drain, 0)
    for out in outs:
        out.wait()


def project(x_blk, gamma_blk, wq, wk, wv, wg, wu, lens, head_dim, ty_size, seq_block, d_model, tile):
    rows_all, kblk = x_blk.shape
    half_ty, group = ty_size // TWO, TWO * seq_block
    rows = half_ty * group
    q_width, ffn = wq.shape[1], wg.shape[1]
    kv_width = wk.shape[1]
    steps = ffn // tile
    wide = 2 * tile
    kdim = 2 * kblk
    x_main = x_blk.reshape(TWO, half_ty, RING, group, kblk)
    x_kv = x_blk.reshape(ty_size, RING, group, kblk)
    pieces = RING + 4 + 2 * steps
    stat_lines = 2 * (-(-((RING * half_ty + RING) // TWO) // 8) * 8)
    any_spec = pl.BlockSpec(memory_space=pl.ANY)
    vmem_spec = pl.BlockSpec(memory_space=pltpu.VMEM)
    return pl.pallas_call(
        functools.partial(project_kernel, ty_size, tile, d_model),
        out_shape=(
            jax.ShapeDtypeStruct((rows, ffn), BF16),
            jax.ShapeDtypeStruct((ty_size, seq_block, q_width), BF16),
            jax.ShapeDtypeStruct((TWO, group, kv_width), BF16),
        ),
        in_specs=[any_spec] * 8 + [vmem_spec] * 2,
        out_specs=(any_spec,) * 3,
        scratch_shapes=[
            pltpu.VMEM((RING * half_ty + RING, group, kdim), BF16),
            pltpu.VMEM((steps + 1, kdim, wide), BF16),
            pltpu.VMEM((kdim, kv_width), BF16),
            pltpu.VMEM((CORES, kblk // LANES, LANES), F32),
            pltpu.VMEM((stat_lines, LANES), F32),
            pltpu.VMEM((3, stat_lines, LANES), F32),
            pltpu.VMEM((steps + 1, rows, wide), BF16),
            pltpu.VMEM((steps + 1, TWO, rows // TWO, wide), BF16),
            pltpu.VMEM((steps + 1, TWO, rows // TWO, wide), BF16),
            pltpu.VMEM((steps + 1, TWO, rows // TWO, wide), BF16),
            pltpu.VMEM((steps + 1, TWO, TWO, rows // TWO, wide), BF16),
            pltpu.VMEM((rows, ffn), BF16),
            pltpu.VMEM((RING, group, kv_width), F32),
            pltpu.VMEM((3, group, kv_width), F32),
            pltpu.VMEM((TWO, group, kv_width), BF16),
            pltpu.VMEM((ty_size, seq_block, q_width), BF16),
            pltpu.VMEM((ty_size, seq_block, q_width), BF16),
            pltpu.SemaphoreType.DMA((pieces,)),
            pltpu.SemaphoreType.DMA((pieces,)),
            pltpu.SemaphoreType.DMA((pieces,)),
            pltpu.SemaphoreType.DMA((len(KINDS),)),
            pltpu.SemaphoreType.DMA((len(KINDS),)),
            pltpu.SemaphoreType.DMA((steps + 1, len(KINDS), TWO)),
            pltpu.SemaphoreType.DMA((steps + 1, len(KINDS), TWO)),
            pltpu.SemaphoreType.DMA((len(KINDS),)),
            pltpu.SemaphoreType.DMA((len(KINDS),)),
            pltpu.SemaphoreType.DMA((TWO,)),
            pltpu.SemaphoreType.DMA((ty_size,)),
            pltpu.SemaphoreType.DMA((ty_size,)),
            pltpu.SemaphoreType.DMA((len(KINDS),)),
        ],
        compiler_params=pltpu.CompilerParams(
            collective_id=0, has_side_effects=True, vmem_limit_bytes=56 * MIB
        ),
        name="project",
    )(
        x_main, x_kv, wq, wk, wv, wg, wu, gamma_blk.reshape(-1, LANES), lens.reshape(-1, group), inverse_freqs(head_dim)
    )


def combine_kernel(
    ty_size,
    q_in, k_in, v_in, act_in, x_in, wo, wd, lens,
    y_out,
    kc, vc, q_raw, q_f32, o_f32, att_out, att, mlp, wos, wds, yp, t1, xr, yf, p2_1, sd_1, sb_1, ra_1, rb_1, p2_2, sd_2, sb_2, ra_2, rb_2, ex,
    qkv_sem, w_sem, wp_send, wp_recv, a2a_send, a2a_recv, mlp_sem, gx_send, gx_recv, x_sem, xp_send, xp_recv,
    rs_send, rs_recv, ag_send, ag_recv, out_sem, outp_send, outp_recv,
):
    row_idx = lax.axis_index("ty")
    col_idx = lax.axis_index("tx")
    ring_pos, core = col_idx // 2, col_idx % 2
    other = 1 - core
    half_ty = ty_size // 2
    chunks = len(SIZES)
    begin = [sum(SIZES[:r]) for r in range(chunks)]
    seq_block = q_in.shape[1]
    group = 2 * seq_block
    cols = wo.shape[1]
    hcols = cols // 2
    pos_p, pos_m = (ring_pos + 1) % RING, (ring_pos + RING - 1) % RING
    tx_side = (pos_p * 2 + core, pos_m * 2 + core)
    from_side = (pos_m, pos_p)
    tx_pair = ring_pos * 2 + other
    z_pos, y_pos = row_idx // RING, row_idx % RING
    up = lambda v: (v + 1) % RING
    down = lambda v: (v + RING - 1) % RING
    y_side = (z_pos * RING + up(y_pos), z_pos * RING + down(y_pos))
    z_side = (up(z_pos) * RING + y_pos, down(z_pos) * RING + y_pos)
    places = ((y_pos, z_pos), (z_pos, y_pos))
    sides = ((y_side, z_side), (z_side, y_side))
    exchange = [size == 1 for size in SIZES]
    mine = pl.ds(pl.multiple_of(core * cols, LANES), cols)

    def units(r):
        return pl.ds(begin[r] * 2 * RING, SIZES[r] * 2 * RING)

    def block_units(r, b):
        return pl.ds(begin[r] * 2 * RING + b * 2 * SIZES[r], 2 * SIZES[r])

    def unit(r, b1, b2):
        return begin[r] * 2 * RING + b1 * 2 * SIZES[r] + b2

    def x_tile(c, r):
        b1, b2 = jnp.where(core == 0, y_pos, z_pos), jnp.where(core == 0, z_pos, y_pos)
        return x_in.at[c, block_units(r, b1) if exchange[r] else pl.ds(unit(r, b1, b2), 1)]

    def x_slot(c, r):
        return xr.at[c, r, pl.ds(0, 2 * SIZES[r] if exchange[r] else 1)]

    def own(r):
        return pl.ds(begin[r], SIZES[r])

    w_loads = [pltpu.make_async_copy(wd, wds.at[:, mine], w_sem.at[0]), pltpu.make_async_copy(wo, wos.at[:, mine], w_sem.at[1])]
    w_swaps = [
        remote(wd, wds.at[:, mine], wp_send.at[0], wp_recv.at[0], row_idx, tx_pair),
        remote(wo, wos.at[:, mine], wp_send.at[1], wp_recv.at[1], row_idx, tx_pair),
    ]
    mlp_loads = [pltpu.make_async_copy(act_in.at[own(r)], mlp.at[own(r), ring_pos], mlp_sem.at[r]) for r in range(chunks)]
    x_loads = [pltpu.make_async_copy(x_tile(core, r), x_slot(core, r), x_sem.at[r]) for r in range(chunks)]
    x_swaps = [remote(x_tile(other, r), x_slot(core, r), xp_send.at[r], xp_recv.at[r], row_idx, tx_pair) for r in range(chunks)]
    qkv_loads = [
        pltpu.make_async_copy(src, dst, qkv_sem.at[n])
        for n, (src, dst) in enumerate(((q_in, q_raw), (k_in, kc), (v_in, vc)))
    ]
    for load in qkv_loads + w_loads + mlp_loads + x_loads:
        load.start()

    barrier = pltpu.get_barrier_semaphore()
    pl.semaphore_signal(barrier, device_id={"ty": row_idx, "tx": tx_pair}, device_id_type=MESH)
    for tx in tx_side:
        pl.semaphore_signal(barrier, device_id={"ty": row_idx, "tx": tx}, device_id_type=MESH)
    for off in range(1, ty_size):
        for cc in BOTH:
            pl.semaphore_signal(
                barrier, device_id={"ty": (row_idx + off) % ty_size, "tx": ring_pos * 2 + cc}, device_id_type=MESH
            )
    pl.semaphore_wait(barrier, 3 + 2 * (ty_size - 1))

    def gather(r, part, stage, side):
        sems = gx_send.at[r, part, stage, side], gx_recv.at[r, part, stage, side]
        buf = (mlp, att)[part]
        if stage == 0:
            src = act_in.at[own(r)] if part == 0 else att.at[own(r), ring_pos]
            return remote(src, buf.at[own(r), ring_pos], *sems, row_idx, tx_side[side])
        if part == 0:
            lanes = mlp.shape[-1] // 2
            block = mlp.at[own(r), from_side[side], :, pl.ds(side * lanes, lanes)]
        else:
            block = att.at[own(r), from_side[side], side]
        return remote(block, block, *sems, row_idx, tx_side[side])

    home, home_core = row_idx % half_ty, row_idx // half_ty

    def a2a(k):
        return remote(
            att_out.at[k], att.at[home, ring_pos, core], a2a_send.at[k], a2a_recv.at[home, core],
            k, ring_pos * 2 + home_core,
        )

    def a2a_self(k):
        return jnp.logical_and(k == row_idx, core == home_core)

    def attend(_):
        heads, lines, head_dim = q_f32.shape
        for load in qkv_loads:
            load.wait()
        for k in range(ty_size):
            for h in range(heads):
                lanes = slice(h * head_dim, (h + 1) * head_dim)
                q_f32[h, k * seq_block : (k + 1) * seq_block, :] = q_raw[k, :, lanes].astype(F32)
        slots = lax.broadcasted_iota(jnp.int32, (heads * ty_size, kc.shape[1]), 1)

        def sequence(b, _):
            picked = pl.ds(b, ty_size, stride=seq_block)
            queries = jnp.concatenate([q_f32[h, picked, :] for h in range(heads)]).astype(BF16)
            scores = lax.dot_general(
                queries, kc[b], (((1,), (1,)), ((), ())), preferred_element_type=F32
            ) * (head_dim**-0.5)
            scores = jnp.where(slots <= lens[b], scores, -1e30)
            weights = jnp.exp(scores - jnp.max(scores, axis=1, keepdims=True))
            probs = (weights / jnp.sum(weights, axis=1, keepdims=True)).astype(BF16)
            mixed = jnp.dot(probs, vc[b], preferred_element_type=F32)
            for h in range(heads):
                o_f32[h, picked, :] = mixed[h * ty_size : (h + 1) * ty_size]
            return 0

        lax.fori_loop(0, seq_block, sequence, 0, unroll=8)
        for k in range(ty_size):
            for h in range(heads):
                lanes = slice(h * head_dim, (h + 1) * head_dim)
                att_out[k, :, lanes] = o_f32[h, k * seq_block : (k + 1) * seq_block, :].astype(BF16)
        for k in range(ty_size):
            @pl.when(a2a_self(k))
            def _():
                pltpu.make_async_copy(
                    att_out.at[k], att.at[home, ring_pos, core], a2a_recv.at[home, core]
                ).start()

            @pl.when(jnp.logical_not(a2a_self(k)))
            def _():
                a2a(k).start()

    for swap in w_swaps + x_swaps:
        swap.start()

    def att_ready(r):
        for g in range(begin[r], begin[r] + SIZES[r]):
            for cc in BOTH:
                remote(
                    att_out.at[0], att.at[g, ring_pos, cc], a2a_send.at[0], a2a_recv.at[g, cc], row_idx, tx_pair
                ).wait_recv()

    def own_att(r):
        att_ready(r)
        for side in BOTH:
            gather(r, 1, 0, side).start()

    def own_mlp(r):
        for side in BOTH:
            gather(r, 0, 0, side).start()

    def forward(part, r):
        for side in BOTH:
            gather(r, part, 0, side).wait_recv()
            gather(r, part, 1, side).start()

    def multiply(r):
        mlp_loads[r].wait()
        for part in BOTH:
            for side in BOTH:
                gather(r, part, 1, side).wait_recv()
        rows = SIZES[r] * RING * group

        def tile(n, _):
            lanes = pl.ds(pl.multiple_of(n * TILE, TILE), TILE)
            left_mlp = mlp[own(r)].reshape(rows, mlp.shape[-1])
            left_att = att[own(r)].reshape(rows, att.shape[-1])
            yp[pl.ds(begin[r] * RING * group, rows), lanes] = jnp.dot(
                left_mlp, wds[:, lanes], preferred_element_type=F32
            ) + jnp.dot(left_att, wos[:, lanes], preferred_element_type=F32)
            return 0

        lax.fori_loop(0, yp.shape[1] // TILE, tile, 0)

    bufs = ((p2_1, sd_1, sb_1, ra_1, rb_1), (p2_2, sd_2, sb_2, ra_2, rb_2))

    def block_rows(level, r):
        return (SIZES[r] * group, seq_block)[level]

    def hop(level, r, c, kind, side):
        p2, sd, sb, ra, rb = bufs[level]
        m = pl.ds(0, block_rows(level, r))
        src, dst = (
            (p2.at[r, c, m, pl.ds(side * hcols, hcols)], ra.at[r, c, side, m]),
            (sd.at[r, c, side, m], rb.at[r, c, side, 0, m]),
            (sb.at[r, c, side, m], rb.at[r, c, side, 1, m]),
        )[kind]
        return remote(
            src, dst, rs_send.at[level, r, c, kind, side], rs_recv.at[level, r, c, kind, side],
            sides[c][level][side], col_idx,
        )

    def part_of(level, r, c, b, half):
        size = block_rows(level, r)
        if level == 0:
            rows = pl.ds(pl.multiple_of(begin[r] * RING * group + b * size, 8), size)
            return yp[rows, c * cols + half * hcols : c * cols + (half + 1) * hcols]
        return t1[r, c, pl.ds(pl.multiple_of(b * size, 8), size), half * hcols : (half + 1) * hcols]

    def reduce_a(level, r):
        p2, sd = bufs[level][:2]
        m = block_rows(level, r)
        for c in BOTH:
            pos = places[c][level]
            for half in BOTH:
                p2[r, c, :m, half * hcols : (half + 1) * hcols] = part_of(level, r, c, (pos + 2) % RING, half).astype(BF16)
                hop(level, r, c, 0, half).start()
        for c in BOTH:
            pos = places[c][level]
            for side, b in enumerate((up(pos), down(pos))):
                sd[r, c, side, :m] = part_of(level, r, c, b, 1 - side).astype(BF16)
                hop(level, r, c, 1, side).start()

    def reduce_b(level, r):
        sb, ra = bufs[level][2:4]
        m = block_rows(level, r)
        for c in BOTH:
            pos = places[c][level]
            for side, b in enumerate((up(pos), down(pos))):
                hop(level, r, c, 0, side).wait_recv()
                sb[r, c, side, :m] = (part_of(level, r, c, b, side) + ra[r, c, side, :m].astype(F32)).astype(BF16)
                hop(level, r, c, 2, side).start()

    def reduce_c(level, r, finish):
        rb = bufs[level][4]
        m = block_rows(level, r)
        for c in BOTH:
            pos = places[c][level]
            for half in BOTH:
                hop(level, r, c, 1, 1 - half).wait_recv()
                hop(level, r, c, 2, half).wait_recv()
                finish(
                    c, half,
                    part_of(level, r, c, pos, half)
                    + rb[r, c, half, 1, :m].astype(F32) + rb[r, c, 1 - half, 0, :m].astype(F32),
                )

    def spread(level, r, c, stage, side):
        ring, (p1, p2) = sides[c][level], places[c]
        sems = ag_send.at[level, r, c, stage, side], ag_recv.at[level, r, c, stage, side]
        near = (down, up)[side]
        half = pl.ds(side * hcols, hcols)
        if level == 1 and exchange[r]:
            m = pl.ds(0, block_rows(0, r))
            block = ex.at[r, c, p2, m] if stage == 0 else ex.at[r, c, near(p2), m, half]
        elif level == 1:
            block = yf.at[c, unit(r, p1, p2)] if stage == 0 else yf.at[c, unit(r, p1, near(p2)), :, half]
        elif stage == 0:
            block = yf.at[c, block_units(r, p1)]
        else:
            block = yf.at[c, pl.ds(unit(r, near(p1), side * SIZES[r]), SIZES[r])]
        return remote(block, block, *sems, ring[side], col_idx)

    def spread_own(level, r):
        for c in BOTH:
            for side in BOTH:
                spread(level, r, c, 0, side).start()

    def spread_on(level, r):
        for c in BOTH:
            for side in BOTH:
                spread(level, r, c, 0, side).wait_recv()
                spread(level, r, c, 1, side).start()

    def spread_end(level, r):
        for c in BOTH:
            for side in BOTH:
                spread(level, r, c, 1, side).wait_recv()

    def s3(r):
        reduce_b(0, r)

    def s4(r):
        m = block_rows(0, r)

        def finish(c, half, vals):
            lanes = slice(half * hcols, (half + 1) * hcols)
            if exchange[r]:
                ex[r, c, places[c][1], :m, lanes] = vals.astype(BF16)
            else:
                t1[r, c, :m, lanes] = vals
        reduce_c(0, r, finish)
        if exchange[r]:
            spread_own(1, r)
        else:
            reduce_a(1, r)

    def s5(r):
        if exchange[r]:
            spread_on(1, r)
        else:
            reduce_b(1, r)

    def s6(r):
        x_loads[r].wait()
        remote(x_tile(other, r), x_slot(other, r), xp_send.at[r], xp_recv.at[r], row_idx, tx_pair).wait_recv()
        if exchange[r]:
            m = block_rows(0, r)
            spread_end(1, r)
            for c in BOTH:
                for n in range(2 * SIZES[r]):
                    rows = slice(n * seq_block, (n + 1) * seq_block)
                    first, second, third, fourth = (ex[r, c, p, rows].astype(F32) for p in range(RING))
                    total = (first + second) + (third + fourth)
                    yf[c, unit(r, places[c][0], n)] = (xr[c, r, n].astype(F32) + total).astype(BF16)
            spread_own(0, r)
        else:
            def finish(c, half, vals):
                lanes = slice(half * hcols, (half + 1) * hcols)
                yf[c, unit(r, *places[c]), :, lanes] = (xr[c, r, 0, :, lanes].astype(F32) + vals).astype(BF16)
            reduce_c(1, r, finish)
            spread_own(1, r)

    def s7(r):
        spread_on(1, r)

    def s8(r):
        spread_end(1, r)
        spread_own(0, r)

    def s9(r):
        spread_on(0, r)

    def out_copy(r):
        return pltpu.make_async_copy(yf.at[core, units(r)], y_out.at[core, units(r)], out_sem.at[r])

    def out_swap(r):
        return remote(
            yf.at[other, units(r)], y_out.at[core, units(r)], outp_send.at[r], outp_recv.at[r], row_idx, tx_pair
        )

    def s10(r):
        spread_end(0, r)
        out_swap(r).start()
        out_copy(r).start()

    def s2(r):
        multiply(r)
        reduce_a(0, r)

    stages = dict(zip("mAagh23456789t", (
        own_mlp, attend, own_att, functools.partial(forward, 0), functools.partial(forward, 1),
        s2, s3, s4, s5, s6, s7, s8, s9, s10,
    )))
    products = ORDER[::TWO].index("2") * TWO
    for n in range(0, len(ORDER), TWO):
        if n == products:
            for load, swap in zip(w_loads, w_swaps):
                load.wait()
                swap.wait_recv()
        stages[ORDER[n]](int(ORDER[n + 1]))

    for swap in w_swaps + x_swaps:
        swap.wait_send()
    for k in range(ty_size):
        @pl.when(jnp.logical_not(a2a_self(k)))
        def _():
            a2a(k).wait_send()
    for r in range(chunks):
        for a in BOTH:
            for b in BOTH:
                for side in BOTH:
                    gather(r, a, b, side).wait_send()
                    for level in BOTH:
                        spread(level, r, a, b, side).wait_send()
        for level in BOTH[: 2 - exchange[r]]:
            for c in BOTH:
                for kind in KINDS:
                    for side in BOTH:
                        hop(level, r, c, kind, side).wait_send()
        out_copy(r).wait()
        out_swap(r).wait()


def combine(q_owned, k_out, v_out, lens_own, act_own, x_blk, w_out, w_down, ty_size):
    seq_block = q_owned.shape[1]
    head_dim = k_out.shape[TWO]
    chunks, most = len(SIZES), max(SIZES)
    group, half_ty = TWO * seq_block, ty_size // TWO
    cols = w_out.shape[1]
    hcols = cols // TWO
    ffn, q_width = w_down.shape[0], w_out.shape[0]
    any_spec = pl.BlockSpec(memory_space=pl.ANY)
    ring_bufs = []
    for m in (most * group, seq_block):
        half = (chunks, TWO, TWO, m, hcols)
        both = (chunks, TWO, TWO, TWO, m, hcols)
        ring_bufs += [pltpu.VMEM(shape, BF16) for shape in ((chunks, TWO, m, cols), half, half, half, both)]
    dma = pltpu.SemaphoreType.DMA
    y_units = (TWO, half_ty * RING * TWO, seq_block, cols)
    y = pl.pallas_call(
        functools.partial(combine_kernel, ty_size),
        out_shape=jax.ShapeDtypeStruct(y_units, BF16),
        in_specs=[any_spec] * 7 + [pl.BlockSpec(memory_space=pltpu.SMEM)],
        out_specs=any_spec,
        scratch_shapes=[
            pltpu.VMEM(k_out.shape, BF16),
            pltpu.VMEM(v_out.shape, BF16),
            pltpu.VMEM(q_owned.shape, BF16),
            pltpu.VMEM((q_width // head_dim, ty_size * seq_block, head_dim), F32),
            pltpu.VMEM((q_width // head_dim, ty_size * seq_block, head_dim), F32),
            pltpu.VMEM(q_owned.shape, BF16),
            pltpu.VMEM((half_ty, RING, TWO, seq_block, q_width), BF16),
            pltpu.VMEM((half_ty, RING, group, ffn), BF16),
            pltpu.VMEM((q_width, TWO * cols), BF16),
            pltpu.VMEM((ffn, TWO * cols), BF16),
            pltpu.VMEM((half_ty * RING * group, TWO * cols), F32),
            pltpu.VMEM((chunks, TWO, most * group, cols), F32),
            pltpu.VMEM((TWO, chunks, TWO * most, seq_block, cols), BF16),
            pltpu.VMEM(y_units, BF16),
            *ring_bufs,
            pltpu.VMEM((chunks, TWO, RING, most * group, cols), BF16),
            dma((len(KINDS),)), dma((CORES,)), dma((CORES,)), dma((CORES,)),
            dma((ty_size,)), dma((half_ty, TWO)),
            dma((chunks,)),
            dma((chunks, TWO, TWO, TWO)), dma((chunks, TWO, TWO, TWO)),
            dma((chunks,)), dma((chunks,)), dma((chunks,)),
            dma((TWO, chunks, TWO, len(KINDS), TWO)), dma((TWO, chunks, TWO, len(KINDS), TWO)),
            dma((TWO, chunks, TWO, TWO, TWO)), dma((TWO, chunks, TWO, TWO, TWO)),
            dma((chunks,)), dma((chunks,)), dma((chunks,)),
        ],
        compiler_params=pltpu.CompilerParams(
            collective_id=1, has_side_effects=True, vmem_limit_bytes=60 * MIB
        ),
        name="combine",
    )(q_owned, k_out, v_out, act_own.reshape(half_ty, group, ffn), x_blk.reshape(y_units), w_out, w_down, lens_own)
    return y.reshape(x_blk.shape)


def solution(mesh):
    ty_size = mesh.shape["ty"]
    tx_size = mesh.shape["tx"]
    cache_spec = P(("dp", "ty", "tx"), None, None)

    def layer_shard(x_blk, lens_part, k_blk, v_blk, gamma_blk, w_query, w_key, w_value, w_gate, w_up, w_out, w_down):
        rows = x_blk.shape[0]
        d_model = x_blk.shape[1] * tx_size
        seq_block, ctx_len, head_dim = k_blk.shape
        row_idx = lax.axis_index("ty")
        col_idx = lax.axis_index("tx")
        ring_pos, core = col_idx // 2, col_idx % 2
        tile = min(256, w_gate.shape[1])

        block_start = (row_idx * tx_size + col_idx) * seq_block
        lens_own = lax.dynamic_slice_in_dim(lens_part, block_start, seq_block)
        act_own, q_owned, kv_new = project(
            x_blk, gamma_blk, w_query, w_key, w_value, w_gate, w_up, lens_part, head_dim,
            ty_size, seq_block, d_model, tile,
        )
        kv_own = lax.dynamic_slice_in_dim(kv_new, core * seq_block, seq_block, axis=1)
        positions = jnp.arange(ctx_len)
        at_slot = positions[None, :, None] == lens_own[:, None, None]
        k_out = jnp.where(at_slot, kv_own[0][:, None, :], k_blk)
        v_out = jnp.where(at_slot, kv_own[1][:, None, :], v_blk)

        y_blk = combine(q_owned, k_out, v_out, lens_own, act_own, x_blk, w_out, w_down, ty_size)
        return y_blk, k_out, v_out

    in_specs = (P("dp", "tx"), P("dp"), cache_spec, cache_spec, P("tx"), P("tx", "ty"), P("tx", None), P("tx", None), P("tx", "ty"), P("tx", "ty"), P("ty", "tx"), P("ty", "tx"))
    out_specs = (P("dp", "tx"), cache_spec, cache_spec)
    return jax.shard_map(layer_shard, mesh=mesh, in_specs=in_specs, out_specs=out_specs, check_vma=False)
```

```python
import functools

import jax
import jax.numpy as jnp
import numpy as np
from jax import lax
from jax.experimental import pallas as pl
from jax.experimental.pallas import tpu as pltpu
from jax.sharding import PartitionSpec as P

EPSILON = 1e-6
ROPE_BASE = 10000.0
MESH = pl.DeviceIdType.MESH
RING = 4
CORES = 2
TWO = 2
LANES = 128
TILE = 512
BOTH = (0, 1)
KINDS = (0, 1, 2)
MIB = 2**20
SIZES = (1, 2, 2, 2, 1)
ORDER = (
    "m1A0m0g1a0a1g0h0a2h1m2h2m3202130g2314041a3a451g35022h3616032"
    + "m42371g4h4423381522443903462539144637254738283649293t194t0t3"
    + "t2t4"
)
F32 = jnp.float32
BF16 = jnp.bfloat16


def inverse_freqs(head_dim):
    powers = np.arange(head_dim // 2, dtype=np.float32) * np.float32(2.0) / np.float32(head_dim)
    freqs = np.float32(ROPE_BASE) ** -powers
    return jnp.asarray(np.concatenate([freqs, freqs])[None, :])


def updated(cache, row, length):
    slots = lax.broadcasted_iota(jnp.int32, cache.shape, 0)
    return jnp.where(slots == length, row, cache.astype(F32)).astype(BF16)


def remote(src, dst, send_sem, recv_sem, ty, tx):
    return pltpu.make_async_remote_copy(
        src_ref=src, dst_ref=dst, send_sem=send_sem, recv_sem=recv_sem,
        device_id={"ty": ty, "tx": tx}, device_id_type=MESH,
    )


def project_kernel(
    ty_size, tile, d_model,
    x_main, x_kv, wq, wk, wv, wg, wu, gamma, lens, freqs,
    act_out, q_out, kv_out,
    xs, ws, wkvs, gam, st, sr, p2, sd, sb, ra, rb, act, kvs, kvr, kvf, qs, qr,
    load_sem, pair_send, pair_recv, st_send, st_recv, ssem, rsem, kv_ssem, kv_rsem, kvf_sem, q_ssem, q_rsem, act_sem, out_sem,
):
    row_idx = lax.axis_index("ty")
    col_idx = lax.axis_index("tx")
    ring_pos, core = col_idx // 2, col_idx % 2
    other = 1 - core
    half_ty = ty_size // 2
    group = xs.shape[1]
    seq_block = group // 2
    rows = half_ty * group
    hrows = rows // 2
    hg = half_ty // 2
    kdim = xs.shape[2]
    kblk = kdim // 2
    steps = wg.shape[1] // tile
    head_dim = freqs.shape[1]
    q_width = wq.shape[1]
    pos_p, pos_m, pos_o = (ring_pos + 1) % RING, (ring_pos + RING - 1) % RING, (ring_pos + 2) % RING
    tx_p, tx_m, tx_o = pos_p * 2 + core, pos_m * 2 + core, pos_o * 2 + core
    tx_pair = ring_pos * 2 + other
    lanes = pl.ds(pl.multiple_of(core * kblk, LANES), kblk)
    krows = pl.ds(pl.multiple_of(core * kblk, LANES), kblk)

    pieces = []
    for d in range(RING):
        pieces.append((lambda c, d=d: x_main.at[c, :, d], xs.at[pl.ds(d * half_ty, half_ty), :, lanes]))
    pieces.append((lambda c: x_kv.at[row_idx], xs.at[pl.ds(RING * half_ty, RING), :, lanes]))
    pieces.append((lambda c: gamma, gam.at[core]))
    pieces.append((lambda c: wq, ws.at[0, krows, pl.ds(0, q_width)]))
    kv_piece = len(pieces)
    pieces.append((lambda c: wk, wkvs.at[krows]))
    for t in range(steps):
        pieces.append((lambda c, t=t: wg.at[:, pl.ds(t * tile, tile)], ws.at[t + 1, krows, pl.ds(0, tile)]))
        pieces.append((lambda c, t=t: wu.at[:, pl.ds(t * tile, tile)], ws.at[t + 1, krows, pl.ds(tile, tile)]))
    loads = [pltpu.make_async_copy(src(core), dst, load_sem.at[n]) for n, (src, dst) in enumerate(pieces)]
    swaps = [remote(src(other), dst, pair_send.at[n], pair_recv.at[n], row_idx, tx_pair) for n, (src, dst) in enumerate(pieces)]
    def start(copies, kv_copies, wants, first):
        for n, copy in enumerate(copies):
            if n < first:
                continue
            if n != kv_piece:
                copy.start()
            else:
                for which in BOTH:
                    pl.when(wants == which)(kv_copies[which].start)

    start(loads, [pltpu.make_async_copy(w, wkvs.at[krows], load_sem.at[kv_piece]) for w in (wk, wv)], core, 0)
    st[...] = jnp.zeros_like(st)

    barrier = pltpu.get_barrier_semaphore()
    pl.semaphore_signal(barrier, device_id={"ty": row_idx, "tx": tx_pair}, device_id_type=MESH)
    for tx in (tx_p, tx_m, tx_o):
        pl.semaphore_signal(barrier, device_id={"ty": row_idx, "tx": tx}, device_id_type=MESH)
    for off in range(1, ty_size):
        for cc in BOTH:
            pl.semaphore_signal(
                barrier, device_id={"ty": (row_idx + off) % ty_size, "tx": ring_pos * 2 + cc}, device_id_type=MESH
            )
    pl.semaphore_wait(barrier, 4 + 2 * (ty_size - 1))
    kv_swaps = [
        remote(w, wkvs.at[krows], pair_send.at[kv_piece], pair_recv.at[kv_piece], row_idx, tx_pair) for w in (wk, wv)
    ]
    for swap in swaps[: kv_piece - 1]:
        swap.start()

    blk = 2 * group
    blocks = (RING * half_ty + RING) // 2
    per_dest = half_ty // 2
    lane_tiles, slab_tiles = kdim // LANES, kblk // LANES

    def add_stats(slab, first, count):
        def stat_block(b, _):
            def lane_tile(j, sums):
                tile_lanes = pl.ds(pl.multiple_of(slab * kblk + j * LANES, LANES), LANES)
                part = xs[pl.ds(2 * b, 2), :, tile_lanes].reshape(blk, LANES).astype(F32)
                return sums[0] + part, sums[1] + part * part
            zero = jnp.zeros((blk, LANES), F32)
            sums = lax.fori_loop(0, kblk // LANES, lane_tile, (zero, zero))
            for which in BOTH:
                line = pl.ds(b + which * (st.shape[0] // 2), 1)
                st[line, pl.ds(0, blk)] += jnp.sum(sums[which].T, axis=0, keepdims=True)
            return 0

        lax.fori_loop(first, first + count, stat_block, 0)

    for n in range(kv_piece - 1):
        loads[n].wait()
    add_stats(core, 0, blocks)
    for n in range(kv_piece - 1):
        swaps[n].wait_recv()
        if n <= RING:
            add_stats(other, n * per_dest, per_dest if n < RING else RING // 2)
    start(swaps, kv_swaps, other, kv_piece - 1)
    stat_copies = [
        remote(st, sr.at[n], st_send.at[n], st_recv.at[n], row_idx, tx) for n, tx in enumerate((tx_p, tx_m, tx_o))
    ]
    for copy in stat_copies:
        copy.start()
    for copy in stat_copies:
        copy.wait()
    total = ((st[...] + sr[0]) + (sr[1] + sr[2]))
    mean = total[: st.shape[0] // 2] / d_model
    var = total[st.shape[0] // 2 :] / d_model - mean * mean
    sr[0, : st.shape[0] // 2, :] = mean
    sr[1, : st.shape[0] // 2, :] = lax.rsqrt(var + EPSILON)

    def norm_block(b, _):
        mean_b = jnp.broadcast_to(sr[0, pl.ds(b, 1), :], (128, LANES)).T[:blk]
        rstd_b = jnp.broadcast_to(sr[1, pl.ds(b, 1), :], (128, LANES)).T[:blk]
        for j in range(lane_tiles):
            cols = slice(j * 128, (j + 1) * LANES)
            part = xs[pl.ds(2 * b, 2), :, cols].reshape(blk, LANES).astype(F32)
            normed = ((part - mean_b) * rstd_b * gam[j // slab_tiles, pl.ds(j % slab_tiles, 1), :]).astype(BF16)
            xs[pl.ds(2 * b, 2), :, cols] = normed.reshape(2, group, LANES)
        return 0


    def norm_dest(d, count):
        lax.fori_loop(d * per_dest, d * per_dest + count, norm_block, 0)


    def left(start, count):
        return xs[pl.ds(start, count)].reshape(count * group, kdim)

    def mm(start, count, w):
        return jnp.dot(left(start, count), w, preferred_element_type=F32)

    def hop(s, n, kind, side):
        cols = pl.ds(0, n)
        src, dst = (
            (p2.at[s, pl.ds(side * hrows, hrows), cols], ra.at[s, side, :, cols]),
            (sd.at[s, side, :, cols], rb.at[s, side, 0, :, cols]),
            (sb.at[s, side, :, cols], rb.at[s, side, 1, :, cols]),
        )[kind]
        return remote(src, dst, ssem.at[s, kind, side], rsem.at[s, kind, side], row_idx, (tx_p, tx_m)[side])

    def stage_far(s, n):
        w = ws[s, :, 0:n]
        p2[s, :, 0:n] = mm(pos_o * half_ty, half_ty, w).astype(BF16)
        hop(s, n, 0, 0).start()
        hop(s, n, 0, 1).start()

    def stage_near(s, n):
        w = ws[s, :, 0:n]
        sd[s, 0, :, 0:n] = mm(pos_p * half_ty + hg, hg, w).astype(BF16)
        hop(s, n, 1, 0).start()
        sd[s, 1, :, 0:n] = mm(pos_m * half_ty, hg, w).astype(BF16)
        hop(s, n, 1, 1).start()

    def stage_a(s, n):
        stage_far(s, n)
        stage_near(s, n)

    def stage_b(s, n):
        w = ws[s, :, 0:n]
        for side, start in ((0, pos_p * half_ty), (1, pos_m * half_ty + hg)):
            own = mm(start, hg, w)
            hop(s, n, 0, side).wait_recv()
            sb[s, side, :, 0:n] = (own + ra[s, side, :, 0:n].astype(F32)).astype(BF16)
            hop(s, n, 2, side).start()

    def stage_c(s, n, finish):
        w = ws[s, :, 0:n]
        for half in BOTH:
            own = mm(ring_pos * half_ty + half * hg, hg, w)
            hop(s, n, 2, half).wait_recv()
            hop(s, n, 1, 1 - half).wait_recv()
            finish(half, own + rb[s, half, 1, :, 0:n].astype(F32) + rb[s, 1 - half, 0, :, 0:n].astype(F32))

    low = lax.broadcasted_iota(jnp.int32, (group, head_dim), 1) < head_dim // 2

    def tables(positions):
        angles = jnp.broadcast_to(positions.astype(F32), (head_dim, group)).T * freqs[...]
        sines = jnp.sin(angles)
        return jnp.cos(angles), jnp.where(low, -sines, sines)

    def turn(vals, cos2, sin2):
        return vals * cos2 + pltpu.roll(vals, head_dim // 2, 1) * sin2

    def finish_q(half, vals):
        for g in range(hg):
            cos2, sin2 = tables(lens[pl.ds((core * half_ty + half * hg + g) * RING + ring_pos, 1), :])
            for h in range(q_width // head_dim):
                cols = slice(h * head_dim, (h + 1) * head_dim)
                turned = turn(vals[g * group : (g + 1) * group, cols], cos2, sin2).astype(BF16)
                for k in BOTH:
                    qs[2 * (half * hg + g) + k, :, cols] = turned[k * seq_block : (k + 1) * seq_block]

    def act_copy(s):
        tile_lanes = pl.ds(pl.multiple_of((s - 1) * tile, tile), tile)
        return pltpu.make_async_copy(act.at[:, tile_lanes], act_out.at[:, tile_lanes], act_sem.at[s])

    def finish_mlp(s):
        def finish(half, vals):
            gate = vals[:, :tile].astype(BF16).astype(F32)
            up = vals[:, tile:].astype(BF16).astype(F32)
            act[pl.ds(half * hrows, hrows), pl.ds(pl.multiple_of((s - 1) * tile, tile), tile)] = (
                gate * jax.nn.sigmoid(gate) * up
            ).astype(BF16)
            if half:
                act_copy(s).start()
        return finish

    def q_copy(k):
        return remote(
            qs.at[k], qr.at[row_idx], q_ssem.at[k], q_rsem.at[row_idx],
            core * half_ty + k // 2, ring_pos * 2 + k % 2,
        )

    def q_is_self(k):
        return jnp.logical_and(core * half_ty + k // 2 == row_idx, core == k % 2)

    def kv_copy(n, pos):
        return remote(kvs.at[pos], kvr.at[n], kv_ssem.at[n], kv_rsem.at[n], row_idx, pos * 2 + core)

    wide = 2 * tile
    norm_dest(pos_o, per_dest)
    for n in (kv_piece - 1, kv_piece):
        loads[n].wait()
        swaps[n].wait_recv()
    stage_far(0, q_width)
    norm_dest(pos_p, per_dest)
    norm_dest(pos_m, per_dest)
    stage_near(0, q_width)
    norm_dest(RING, 2)
    kvs[...] = mm(RING * half_ty, RING, wkvs[...]).reshape(kvs.shape)
    for n, pos in enumerate((pos_p, pos_m, pos_o)):
        kv_copy(n, pos).start()
    norm_dest(ring_pos, per_dest)

    def weights_here(first, last):
        for n in range(kv_piece + 2 * first - 1, kv_piece + 2 * last + 1):
            loads[n].wait()
            swaps[n].wait_recv()

    weights_here(1, 1)
    stage_a(1, wide)
    stage_b(0, q_width)
    for n, pos in enumerate((pos_p, pos_m, pos_o)):
        kv_copy(n, pos).wait_recv()
    new_row = (kvs[ring_pos] + kvr[0]) + (kvr[1] + kvr[2])
    kvf[core] = turn(new_row, *tables(lens[pl.ds(row_idx * RING + ring_pos, 1), :] * other)).astype(BF16)
    kv_pair = remote(kvf.at[core], kvf.at[core], kvf_sem.at[0], kvf_sem.at[1], row_idx, tx_pair)
    kv_pair.start()
    weights_here(2, 2)
    stage_a(2, wide)
    stage_b(1, wide)
    stage_c(0, q_width, finish_q)
    for k in range(ty_size):
        @pl.when(q_is_self(k))
        def _():
            pltpu.make_async_copy(qs.at[k], qr.at[row_idx], q_rsem.at[row_idx]).start()

        @pl.when(jnp.logical_not(q_is_self(k)))
        def _():
            q_copy(k).start()

    def middle(s, _):
        stage_a(s, wide)
        stage_b(s - 1, wide)
        stage_c(s - 2, wide, finish_mlp(s - 2))
        return 0

    weights_here(3, steps)
    lax.fori_loop(3, steps + 1, middle, 0)
    stage_b(steps, wide)
    stage_c(steps - 1, wide, finish_mlp(steps - 1))
    stage_c(steps, wide, finish_mlp(steps))

    outs = [
        pltpu.make_async_copy(qr, q_out, out_sem.at[0]),
        pltpu.make_async_copy(kvf, kv_out, out_sem.at[1]),
    ]
    for k in range(ty_size):
        remote(qs.at[0], qr.at[k], q_ssem.at[0], q_rsem.at[k], row_idx, tx_pair).wait_recv()
    outs[0].start()
    kv_pair.wait_send()
    remote(kvf.at[other], kvf.at[other], kvf_sem.at[0], kvf_sem.at[1], row_idx, tx_pair).wait_recv()
    outs[1].start()
    for k in range(ty_size):
        @pl.when(jnp.logical_not(q_is_self(k)))
        def _():
            q_copy(k).wait_send()
    for n, pos in enumerate((pos_p, pos_m, pos_o)):
        kv_copy(n, pos).wait_send()
    for swap in swaps:
        swap.wait_send()
    for kind in KINDS:
        for side in BOTH:
            hop(0, q_width, kind, side).wait_send()

    def drain(s, _):
        act_copy(s).wait()
        for kind in KINDS:
            for side in BOTH:
                hop(s, wide, kind, side).wait_send()
        return 0

    lax.fori_loop(1, steps + 1, drain, 0)
    for out in outs:
        out.wait()


def project(x_blk, gamma_blk, wq, wk, wv, wg, wu, lens, head_dim, ty_size, seq_block, d_model, tile):
    rows_all, kblk = x_blk.shape
    half_ty, group = ty_size // TWO, TWO * seq_block
    rows = half_ty * group
    q_width, ffn = wq.shape[1], wg.shape[1]
    kv_width = wk.shape[1]
    steps = ffn // tile
    wide = 2 * tile
    kdim = 2 * kblk
    x_main = x_blk.reshape(TWO, half_ty, RING, group, kblk)
    x_kv = x_blk.reshape(ty_size, RING, group, kblk)
    pieces = RING + 4 + 2 * steps
    stat_lines = 2 * (-(-((RING * half_ty + RING) // TWO) // 8) * 8)
    any_spec = pl.BlockSpec(memory_space=pl.ANY)
    vmem_spec = pl.BlockSpec(memory_space=pltpu.VMEM)
    return pl.pallas_call(
        functools.partial(project_kernel, ty_size, tile, d_model),
        out_shape=(
            jax.ShapeDtypeStruct((rows, ffn), BF16),
            jax.ShapeDtypeStruct((ty_size, seq_block, q_width), BF16),
            jax.ShapeDtypeStruct((TWO, group, kv_width), BF16),
        ),
        in_specs=[any_spec] * 8 + [vmem_spec] * 2,
        out_specs=(any_spec,) * 3,
        scratch_shapes=[
            pltpu.VMEM((RING * half_ty + RING, group, kdim), BF16),
            pltpu.VMEM((steps + 1, kdim, wide), BF16),
            pltpu.VMEM((kdim, kv_width), BF16),
            pltpu.VMEM((CORES, kblk // LANES, LANES), F32),
            pltpu.VMEM((stat_lines, LANES), F32),
            pltpu.VMEM((3, stat_lines, LANES), F32),
            pltpu.VMEM((steps + 1, rows, wide), BF16),
            pltpu.VMEM((steps + 1, TWO, rows // TWO, wide), BF16),
            pltpu.VMEM((steps + 1, TWO, rows // TWO, wide), BF16),
            pltpu.VMEM((steps + 1, TWO, rows // TWO, wide), BF16),
            pltpu.VMEM((steps + 1, TWO, TWO, rows // TWO, wide), BF16),
            pltpu.VMEM((rows, ffn), BF16),
            pltpu.VMEM((RING, group, kv_width), F32),
            pltpu.VMEM((3, group, kv_width), F32),
            pltpu.VMEM((TWO, group, kv_width), BF16),
            pltpu.VMEM((ty_size, seq_block, q_width), BF16),
            pltpu.VMEM((ty_size, seq_block, q_width), BF16),
            pltpu.SemaphoreType.DMA((pieces,)),
            pltpu.SemaphoreType.DMA((pieces,)),
            pltpu.SemaphoreType.DMA((pieces,)),
            pltpu.SemaphoreType.DMA((len(KINDS),)),
            pltpu.SemaphoreType.DMA((len(KINDS),)),
            pltpu.SemaphoreType.DMA((steps + 1, len(KINDS), TWO)),
            pltpu.SemaphoreType.DMA((steps + 1, len(KINDS), TWO)),
            pltpu.SemaphoreType.DMA((len(KINDS),)),
            pltpu.SemaphoreType.DMA((len(KINDS),)),
            pltpu.SemaphoreType.DMA((TWO,)),
            pltpu.SemaphoreType.DMA((ty_size,)),
            pltpu.SemaphoreType.DMA((ty_size,)),
            pltpu.SemaphoreType.DMA((steps + 1,)),
            pltpu.SemaphoreType.DMA((TWO,)),
        ],
        compiler_params=pltpu.CompilerParams(
            collective_id=0, has_side_effects=True, vmem_limit_bytes=56 * MIB
        ),
        name="project",
    )(
        x_main, x_kv, wq, wk, wv, wg, wu, gamma_blk.reshape(-1, LANES), lens.reshape(-1, group), inverse_freqs(head_dim)
    )


def combine_kernel(
    ty_size,
    q_in, kv_in, k_in, v_in, act_in, x_in, wo, wd, lens,
    y_out,
    kvn, kv_f32, kc, vc, q_raw, q_f32, o_f32, att_out, att, mlp, wos, wds, yp, t1, xr, yf, p2_1, sd_1, sb_1, ra_1, rb_1, p2_2, sd_2, sb_2, ra_2, rb_2, ex,
    qkv_sem, w_sem, wp_send, wp_recv, a2a_send, a2a_recv, mlp_sem, gx_send, gx_recv, x_sem, xp_send, xp_recv,
    rs_send, rs_recv, ag_send, ag_recv, out_sem, outp_send, outp_recv,
):
    row_idx = lax.axis_index("ty")
    col_idx = lax.axis_index("tx")
    ring_pos, core = col_idx // 2, col_idx % 2
    other = 1 - core
    half_ty = ty_size // 2
    chunks = len(SIZES)
    begin = [sum(SIZES[:r]) for r in range(chunks)]
    seq_block = q_in.shape[1]
    group = 2 * seq_block
    cols = wo.shape[1]
    hcols = cols // 2
    pos_p, pos_m = (ring_pos + 1) % RING, (ring_pos + RING - 1) % RING
    tx_side = (pos_p * 2 + core, pos_m * 2 + core)
    from_side = (pos_m, pos_p)
    tx_pair = ring_pos * 2 + other
    z_pos, y_pos = row_idx // RING, row_idx % RING
    up = lambda v: (v + 1) % RING
    down = lambda v: (v + RING - 1) % RING
    y_side = (z_pos * RING + up(y_pos), z_pos * RING + down(y_pos))
    z_side = (up(z_pos) * RING + y_pos, down(z_pos) * RING + y_pos)
    places = ((y_pos, z_pos), (z_pos, y_pos))
    sides = ((y_side, z_side), (z_side, y_side))
    exchange = [size == 1 for size in SIZES]
    mine = pl.ds(pl.multiple_of(core * cols, LANES), cols)

    def units(r):
        return pl.ds(begin[r] * 2 * RING, SIZES[r] * 2 * RING)

    def block_units(r, b):
        return pl.ds(begin[r] * 2 * RING + b * 2 * SIZES[r], 2 * SIZES[r])

    def unit(r, b1, b2):
        return begin[r] * 2 * RING + b1 * 2 * SIZES[r] + b2

    def x_tile(c, r):
        b1, b2 = jnp.where(core == 0, y_pos, z_pos), jnp.where(core == 0, z_pos, y_pos)
        return x_in.at[c, block_units(r, b1) if exchange[r] else pl.ds(unit(r, b1, b2), 1)]

    def x_slot(c, r):
        return xr.at[c, r, pl.ds(0, 2 * SIZES[r] if exchange[r] else 1)]

    def own(r):
        return pl.ds(begin[r], SIZES[r])

    w_loads = [pltpu.make_async_copy(wd, wds.at[:, mine], w_sem.at[0]), pltpu.make_async_copy(wo, wos.at[:, mine], w_sem.at[1])]
    w_swaps = [
        remote(wd, wds.at[:, mine], wp_send.at[0], wp_recv.at[0], row_idx, tx_pair),
        remote(wo, wos.at[:, mine], wp_send.at[1], wp_recv.at[1], row_idx, tx_pair),
    ]
    mlp_loads = [pltpu.make_async_copy(act_in.at[own(r)], mlp.at[own(r), ring_pos], mlp_sem.at[r]) for r in range(chunks)]
    x_loads = [pltpu.make_async_copy(x_tile(core, r), x_slot(core, r), x_sem.at[r]) for r in range(chunks)]
    x_swaps = [remote(x_tile(other, r), x_slot(core, r), xp_send.at[r], xp_recv.at[r], row_idx, tx_pair) for r in range(chunks)]
    qkv_loads = [
        pltpu.make_async_copy(src, dst, qkv_sem.at[n])
        for n, (src, dst) in enumerate(((q_in, q_raw), (kv_in, kvn), (k_in, kc), (v_in, vc)))
    ]
    for load in qkv_loads + w_loads + mlp_loads + x_loads:
        load.start()

    barrier = pltpu.get_barrier_semaphore()
    pl.semaphore_signal(barrier, device_id={"ty": row_idx, "tx": tx_pair}, device_id_type=MESH)
    for tx in tx_side:
        pl.semaphore_signal(barrier, device_id={"ty": row_idx, "tx": tx}, device_id_type=MESH)
    for off in range(1, ty_size):
        for cc in BOTH:
            pl.semaphore_signal(
                barrier, device_id={"ty": (row_idx + off) % ty_size, "tx": ring_pos * 2 + cc}, device_id_type=MESH
            )
    pl.semaphore_wait(barrier, 3 + 2 * (ty_size - 1))

    def gather(r, part, stage, side):
        sems = gx_send.at[r, part, stage, side], gx_recv.at[r, part, stage, side]
        buf = (mlp, att)[part]
        if stage == 0:
            src = act_in.at[own(r)] if part == 0 else att.at[own(r), ring_pos]
            return remote(src, buf.at[own(r), ring_pos], *sems, row_idx, tx_side[side])
        if part == 0:
            lanes = mlp.shape[-1] // 2
            block = mlp.at[own(r), from_side[side], :, pl.ds(side * lanes, lanes)]
        else:
            block = att.at[own(r), from_side[side], side]
        return remote(block, block, *sems, row_idx, tx_side[side])

    home, home_core = row_idx % half_ty, row_idx // half_ty

    def a2a(k):
        return remote(
            att_out.at[k], att.at[home, ring_pos, core], a2a_send.at[k], a2a_recv.at[home, core],
            k, ring_pos * 2 + home_core,
        )

    def a2a_self(k):
        return jnp.logical_and(k == row_idx, core == home_core)

    def attend(_):
        heads, lines, head_dim = q_f32.shape
        for load in qkv_loads:
            load.wait()
        for k in range(ty_size):
            for h in range(heads):
                lanes = slice(h * head_dim, (h + 1) * head_dim)
                q_f32[h, k * seq_block : (k + 1) * seq_block, :] = q_raw[k, :, lanes].astype(F32)
        kv_f32[...] = kvn[...].astype(F32)
        slots = lax.broadcasted_iota(jnp.int32, (heads * ty_size, kc.shape[1]), 1)

        def sequence(b, _):
            picked = pl.ds(b, ty_size, stride=seq_block)
            fresh = pl.ds(core * seq_block + b, 1)
            keys = updated(kc[b], kv_f32[0, fresh, :], lens[b])
            vals = updated(vc[b], kv_f32[1, fresh, :], lens[b])
            queries = jnp.concatenate([q_f32[h, picked, :] for h in range(heads)]).astype(BF16)
            scores = lax.dot_general(
                queries, keys, (((1,), (1,)), ((), ())), preferred_element_type=F32
            ) * (head_dim**-0.5)
            scores = jnp.where(slots <= lens[b], scores, -1e30)
            weights = jnp.exp(scores - jnp.max(scores, axis=1, keepdims=True))
            probs = (weights / jnp.sum(weights, axis=1, keepdims=True)).astype(BF16)
            mixed = jnp.dot(probs, vals, preferred_element_type=F32)
            for h in range(heads):
                o_f32[h, picked, :] = mixed[h * ty_size : (h + 1) * ty_size]
            return 0

        lax.fori_loop(0, seq_block, sequence, 0, unroll=8)
        for k in range(ty_size):
            for h in range(heads):
                lanes = slice(h * head_dim, (h + 1) * head_dim)
                att_out[k, :, lanes] = o_f32[h, k * seq_block : (k + 1) * seq_block, :].astype(BF16)
        for k in range(ty_size):
            @pl.when(a2a_self(k))
            def _():
                pltpu.make_async_copy(
                    att_out.at[k], att.at[home, ring_pos, core], a2a_recv.at[home, core]
                ).start()

            @pl.when(jnp.logical_not(a2a_self(k)))
            def _():
                a2a(k).start()

    for swap in w_swaps + x_swaps:
        swap.start()

    def att_ready(r):
        for g in range(begin[r], begin[r] + SIZES[r]):
            for cc in BOTH:
                remote(
                    att_out.at[0], att.at[g, ring_pos, cc], a2a_send.at[0], a2a_recv.at[g, cc], row_idx, tx_pair
                ).wait_recv()

    def own_att(r):
        att_ready(r)
        for side in BOTH:
            gather(r, 1, 0, side).start()

    def own_mlp(r):
        for side in BOTH:
            gather(r, 0, 0, side).start()

    def forward(part, r):
        for side in BOTH:
            gather(r, part, 0, side).wait_recv()
            gather(r, part, 1, side).start()

    def multiply(r):
        mlp_loads[r].wait()
        for part in BOTH:
            for side in BOTH:
                gather(r, part, 1, side).wait_recv()
        rows = SIZES[r] * RING * group

        def tile(n, _):
            lanes = pl.ds(pl.multiple_of(n * TILE, TILE), TILE)
            left_mlp = mlp[own(r)].reshape(rows, mlp.shape[-1])
            left_att = att[own(r)].reshape(rows, att.shape[-1])
            yp[pl.ds(begin[r] * RING * group, rows), lanes] = jnp.dot(
                left_mlp, wds[:, lanes], preferred_element_type=F32
            ) + jnp.dot(left_att, wos[:, lanes], preferred_element_type=F32)
            return 0

        lax.fori_loop(0, yp.shape[1] // TILE, tile, 0)

    bufs = ((p2_1, sd_1, sb_1, ra_1, rb_1), (p2_2, sd_2, sb_2, ra_2, rb_2))

    def block_rows(level, r):
        return (SIZES[r] * group, seq_block)[level]

    def hop(level, r, c, kind, side):
        p2, sd, sb, ra, rb = bufs[level]
        m = pl.ds(0, block_rows(level, r))
        src, dst = (
            (p2.at[r, c, m, pl.ds(side * hcols, hcols)], ra.at[r, c, side, m]),
            (sd.at[r, c, side, m], rb.at[r, c, side, 0, m]),
            (sb.at[r, c, side, m], rb.at[r, c, side, 1, m]),
        )[kind]
        return remote(
            src, dst, rs_send.at[level, r, c, kind, side], rs_recv.at[level, r, c, kind, side],
            sides[c][level][side], col_idx,
        )

    def part_of(level, r, c, b, half):
        size = block_rows(level, r)
        if level == 0:
            rows = pl.ds(pl.multiple_of(begin[r] * RING * group + b * size, 8), size)
            return yp[rows, c * cols + half * hcols : c * cols + (half + 1) * hcols]
        return t1[r, c, pl.ds(pl.multiple_of(b * size, 8), size), half * hcols : (half + 1) * hcols]

    def reduce_a(level, r):
        p2, sd = bufs[level][:2]
        m = block_rows(level, r)
        for c in BOTH:
            pos = places[c][level]
            for half in BOTH:
                p2[r, c, :m, half * hcols : (half + 1) * hcols] = part_of(level, r, c, (pos + 2) % RING, half).astype(BF16)
                hop(level, r, c, 0, half).start()
        for c in BOTH:
            pos = places[c][level]
            for side, b in enumerate((up(pos), down(pos))):
                sd[r, c, side, :m] = part_of(level, r, c, b, 1 - side).astype(BF16)
                hop(level, r, c, 1, side).start()

    def reduce_b(level, r):
        sb, ra = bufs[level][2:4]
        m = block_rows(level, r)
        for c in BOTH:
            pos = places[c][level]
            for side, b in enumerate((up(pos), down(pos))):
                hop(level, r, c, 0, side).wait_recv()
                sb[r, c, side, :m] = (part_of(level, r, c, b, side) + ra[r, c, side, :m].astype(F32)).astype(BF16)
                hop(level, r, c, 2, side).start()

    def reduce_c(level, r, finish):
        rb = bufs[level][4]
        m = block_rows(level, r)
        for c in BOTH:
            pos = places[c][level]
            for half in BOTH:
                hop(level, r, c, 1, 1 - half).wait_recv()
                hop(level, r, c, 2, half).wait_recv()
                finish(
                    c, half,
                    part_of(level, r, c, pos, half)
                    + rb[r, c, half, 1, :m].astype(F32) + rb[r, c, 1 - half, 0, :m].astype(F32),
                )

    def spread(level, r, c, stage, side):
        ring, (p1, p2) = sides[c][level], places[c]
        sems = ag_send.at[level, r, c, stage, side], ag_recv.at[level, r, c, stage, side]
        near = (down, up)[side]
        half = pl.ds(side * hcols, hcols)
        if level == 1 and exchange[r]:
            m = pl.ds(0, block_rows(0, r))
            block = ex.at[r, c, p2, m] if stage == 0 else ex.at[r, c, near(p2), m, half]
        elif level == 1:
            block = yf.at[c, unit(r, p1, p2)] if stage == 0 else yf.at[c, unit(r, p1, near(p2)), :, half]
        elif stage == 0:
            block = yf.at[c, block_units(r, p1)]
        else:
            block = yf.at[c, pl.ds(unit(r, near(p1), side * SIZES[r]), SIZES[r])]
        return remote(block, block, *sems, ring[side], col_idx)

    def spread_own(level, r):
        for c in BOTH:
            for side in BOTH:
                spread(level, r, c, 0, side).start()

    def spread_on(level, r):
        for c in BOTH:
            for side in BOTH:
                spread(level, r, c, 0, side).wait_recv()
                spread(level, r, c, 1, side).start()

    def spread_end(level, r):
        for c in BOTH:
            for side in BOTH:
                spread(level, r, c, 1, side).wait_recv()

    def s3(r):
        reduce_b(0, r)

    def s4(r):
        m = block_rows(0, r)

        def finish(c, half, vals):
            lanes = slice(half * hcols, (half + 1) * hcols)
            if exchange[r]:
                ex[r, c, places[c][1], :m, lanes] = vals.astype(BF16)
            else:
                t1[r, c, :m, lanes] = vals
        reduce_c(0, r, finish)
        if exchange[r]:
            spread_own(1, r)
        else:
            reduce_a(1, r)

    def s5(r):
        if exchange[r]:
            spread_on(1, r)
        else:
            reduce_b(1, r)

    def s6(r):
        x_loads[r].wait()
        remote(x_tile(other, r), x_slot(other, r), xp_send.at[r], xp_recv.at[r], row_idx, tx_pair).wait_recv()
        if exchange[r]:
            m = block_rows(0, r)
            spread_end(1, r)
            for c in BOTH:
                for n in range(2 * SIZES[r]):
                    rows = slice(n * seq_block, (n + 1) * seq_block)
                    first, second, third, fourth = (ex[r, c, p, rows].astype(F32) for p in range(RING))
                    total = (first + second) + (third + fourth)
                    yf[c, unit(r, places[c][0], n)] = (xr[c, r, n].astype(F32) + total).astype(BF16)
            spread_own(0, r)
        else:
            def finish(c, half, vals):
                lanes = slice(half * hcols, (half + 1) * hcols)
                yf[c, unit(r, *places[c]), :, lanes] = (xr[c, r, 0, :, lanes].astype(F32) + vals).astype(BF16)
            reduce_c(1, r, finish)
            spread_own(1, r)

    def s7(r):
        spread_on(1, r)

    def s8(r):
        spread_end(1, r)
        spread_own(0, r)

    def s9(r):
        spread_on(0, r)

    def out_copy(r):
        return pltpu.make_async_copy(yf.at[core, units(r)], y_out.at[core, units(r)], out_sem.at[r])

    def out_swap(r):
        return remote(
            yf.at[other, units(r)], y_out.at[core, units(r)], outp_send.at[r], outp_recv.at[r], row_idx, tx_pair
        )

    def s10(r):
        spread_end(0, r)
        out_swap(r).start()
        out_copy(r).start()

    def s2(r):
        multiply(r)
        reduce_a(0, r)

    stages = dict(zip("mAagh23456789t", (
        own_mlp, attend, own_att, functools.partial(forward, 0), functools.partial(forward, 1),
        s2, s3, s4, s5, s6, s7, s8, s9, s10,
    )))
    products = ORDER[::TWO].index("2") * TWO
    for n in range(0, len(ORDER), TWO):
        if n == products:
            for load, swap in zip(w_loads, w_swaps):
                load.wait()
                swap.wait_recv()
        stages[ORDER[n]](int(ORDER[n + 1]))

    for swap in w_swaps + x_swaps:
        swap.wait_send()
    for k in range(ty_size):
        @pl.when(jnp.logical_not(a2a_self(k)))
        def _():
            a2a(k).wait_send()
    for r in range(chunks):
        for a in BOTH:
            for b in BOTH:
                for side in BOTH:
                    gather(r, a, b, side).wait_send()
                    for level in BOTH:
                        spread(level, r, a, b, side).wait_send()
        for level in BOTH[: 2 - exchange[r]]:
            for c in BOTH:
                for kind in KINDS:
                    for side in BOTH:
                        hop(level, r, c, kind, side).wait_send()
        out_copy(r).wait()
        out_swap(r).wait()


def combine(q_owned, kv_new, k_blk, v_blk, lens_own, act_own, x_blk, w_out, w_down, ty_size):
    seq_block = q_owned.shape[1]
    head_dim = k_blk.shape[TWO]
    chunks, most = len(SIZES), max(SIZES)
    group, half_ty = TWO * seq_block, ty_size // TWO
    cols = w_out.shape[1]
    hcols = cols // TWO
    ffn, q_width = w_down.shape[0], w_out.shape[0]
    any_spec = pl.BlockSpec(memory_space=pl.ANY)
    ring_bufs = []
    for m in (most * group, seq_block):
        half = (chunks, TWO, TWO, m, hcols)
        both = (chunks, TWO, TWO, TWO, m, hcols)
        ring_bufs += [pltpu.VMEM(shape, BF16) for shape in ((chunks, TWO, m, cols), half, half, half, both)]
    dma = pltpu.SemaphoreType.DMA
    y_units = (TWO, half_ty * RING * TWO, seq_block, cols)
    y = pl.pallas_call(
        functools.partial(combine_kernel, ty_size),
        out_shape=jax.ShapeDtypeStruct(y_units, BF16),
        in_specs=[any_spec] * 8 + [pl.BlockSpec(memory_space=pltpu.SMEM)],
        out_specs=any_spec,
        scratch_shapes=[
            pltpu.VMEM(kv_new.shape, BF16),
            pltpu.VMEM(kv_new.shape, F32),
            pltpu.VMEM(k_blk.shape, BF16),
            pltpu.VMEM(v_blk.shape, BF16),
            pltpu.VMEM(q_owned.shape, BF16),
            pltpu.VMEM((q_width // head_dim, ty_size * seq_block, head_dim), F32),
            pltpu.VMEM((q_width // head_dim, ty_size * seq_block, head_dim), F32),
            pltpu.VMEM(q_owned.shape, BF16),
            pltpu.VMEM((half_ty, RING, TWO, seq_block, q_width), BF16),
            pltpu.VMEM((half_ty, RING, group, ffn), BF16),
            pltpu.VMEM((q_width, TWO * cols), BF16),
            pltpu.VMEM((ffn, TWO * cols), BF16),
            pltpu.VMEM((half_ty * RING * group, TWO * cols), F32),
            pltpu.VMEM((chunks, TWO, most * group, cols), F32),
            pltpu.VMEM((TWO, chunks, TWO * most, seq_block, cols), BF16),
            pltpu.VMEM(y_units, BF16),
            *ring_bufs,
            pltpu.VMEM((chunks, TWO, RING, most * group, cols), BF16),
            dma((RING,)), dma((CORES,)), dma((CORES,)), dma((CORES,)),
            dma((ty_size,)), dma((half_ty, TWO)),
            dma((chunks,)),
            dma((chunks, TWO, TWO, TWO)), dma((chunks, TWO, TWO, TWO)),
            dma((chunks,)), dma((chunks,)), dma((chunks,)),
            dma((TWO, chunks, TWO, len(KINDS), TWO)), dma((TWO, chunks, TWO, len(KINDS), TWO)),
            dma((TWO, chunks, TWO, TWO, TWO)), dma((TWO, chunks, TWO, TWO, TWO)),
            dma((chunks,)), dma((chunks,)), dma((chunks,)),
        ],
        compiler_params=pltpu.CompilerParams(
            collective_id=1, has_side_effects=True, vmem_limit_bytes=60 * MIB
        ),
        name="combine",
    )(q_owned, kv_new, k_blk, v_blk, act_own.reshape(half_ty, group, ffn), x_blk.reshape(y_units), w_out, w_down, lens_own)
    return y.reshape(x_blk.shape)


def emit_kernel(pieces, y_in, kv_in, k_in, v_in, lens, y_out, k_out, v_out, ys, kvn, kv_f32, kc, vc, load_sem, y_sem, out_sem, y_out_sem):
    core = lax.axis_index("tx") % CORES
    seq_block = kc.shape[0]
    size = ys.shape[0] // pieces
    loads = [
        pltpu.make_async_copy(src, dst, load_sem.at[n]) for n, (src, dst) in enumerate(((kv_in, kvn), (k_in, kc), (v_in, vc)))
    ]
    part = [pl.ds(n * size, size) for n in range(pieces)]
    y_loads = [pltpu.make_async_copy(y_in.at[p], ys.at[p], y_sem.at[n]) for n, p in enumerate(part)]
    y_stores = [pltpu.make_async_copy(ys.at[p], y_out.at[p], y_out_sem.at[n]) for n, p in enumerate(part)]
    stores = [pltpu.make_async_copy(kc, k_out, out_sem.at[0]), pltpu.make_async_copy(vc, v_out, out_sem.at[1])]
    for load in loads + y_loads:
        load.start()
    for load in loads:
        load.wait()
    kv_f32[...] = kvn[...].astype(F32)

    def sequence(b, _):
        fresh = pl.ds(core * seq_block + b, 1)
        kc[b] = updated(kc[b], kv_f32[0, fresh, :], lens[b])
        vc[b] = updated(vc[b], kv_f32[1, fresh, :], lens[b])
        return 0

    lax.fori_loop(0, seq_block, sequence, 0, unroll=4)
    for store in stores:
        store.start()
    for load, store in zip(y_loads, y_stores):
        load.wait()
        store.start()
    for store in y_stores + stores:
        store.wait()


def emit(y, kv_new, k_blk, v_blk, lens_own):
    pieces = 8
    any_spec = pl.BlockSpec(memory_space=pl.ANY)
    dma = pltpu.SemaphoreType.DMA
    return pl.pallas_call(
        functools.partial(emit_kernel, pieces),
        out_shape=tuple(jax.ShapeDtypeStruct(a.shape, BF16) for a in (y, k_blk, v_blk)),
        in_specs=[any_spec] * RING + [pl.BlockSpec(memory_space=pltpu.SMEM)],
        out_specs=(any_spec,) * len(KINDS),
        scratch_shapes=[
            pltpu.VMEM(y.shape, BF16),
            pltpu.VMEM(kv_new.shape, BF16),
            pltpu.VMEM(kv_new.shape, F32),
            pltpu.VMEM(k_blk.shape, BF16),
            pltpu.VMEM(v_blk.shape, BF16),
            dma((len(KINDS),)), dma((pieces,)), dma((TWO,)), dma((pieces,)),
        ],
        compiler_params=pltpu.CompilerParams(vmem_limit_bytes=60 * MIB),
        name="emit",
    )(y, kv_new, k_blk, v_blk, lens_own)


def solution(mesh):
    ty_size = mesh.shape["ty"]
    tx_size = mesh.shape["tx"]
    cache_spec = P(("dp", "ty", "tx"), None, None)

    def layer_shard(x_blk, lens_part, k_blk, v_blk, gamma_blk, w_query, w_key, w_value, w_gate, w_up, w_out, w_down):
        rows = x_blk.shape[0]
        d_model = x_blk.shape[1] * tx_size
        seq_block, _, head_dim = k_blk.shape
        row_idx = lax.axis_index("ty")
        col_idx = lax.axis_index("tx")
        tile = min(256, w_gate.shape[1])

        block_start = (row_idx * tx_size + col_idx) * seq_block
        lens_own = lax.dynamic_slice_in_dim(lens_part, block_start, seq_block)
        act_own, q_owned, kv_new = project(
            x_blk, gamma_blk, w_query, w_key, w_value, w_gate, w_up, lens_part, head_dim,
            ty_size, seq_block, d_model, tile,
        )
        y_raw = combine(q_owned, kv_new, k_blk, v_blk, lens_own, act_own, x_blk, w_out, w_down, ty_size)
        y_blk, k_out, v_out = emit(y_raw, kv_new, k_blk, v_blk, lens_own)
        return y_blk, k_out, v_out

    in_specs = (P("dp", "tx"), P("dp"), cache_spec, cache_spec, P("tx"), P("tx", "ty"), P("tx", None), P("tx", None), P("tx", "ty"), P("tx", "ty"), P("ty", "tx"), P("ty", "tx"))
    out_specs = (P("dp", "tx"), cache_spec, cache_spec)
    return jax.shard_map(layer_shard, mesh=mesh, in_specs=in_specs, out_specs=out_specs, check_vma=False)
```

```python
import functools

import jax
import jax.numpy as jnp
import numpy as np
from jax import lax
from jax.experimental import pallas as pl
from jax.experimental.pallas import tpu as pltpu
from jax.sharding import PartitionSpec as P

EPSILON = 1e-6
ROPE_BASE = 10000.0
MESH = pl.DeviceIdType.MESH
RING = 4
CORES = 2
TWO = 2
LANES = 128
TILE = 512
BOTH = (0, 1)
KINDS = (0, 1, 2)
MIB = 2**20
SIZES = (1, 2, 2, 2, 1)
ORDER = (
    "m1A0m0g1a0a1g0h0a2h1m2h2m3202130g2314041a3a451g35022h3616032"
    + "m42371g4h4423381522443903462539144637254738283649293t194t0t3"
    + "t2t4"
)
F32 = jnp.float32
BF16 = jnp.bfloat16


def inverse_freqs(head_dim):
    powers = np.arange(head_dim // 2, dtype=np.float32) * np.float32(2.0) / np.float32(head_dim)
    freqs = np.float32(ROPE_BASE) ** -powers
    return jnp.asarray(np.concatenate([freqs, freqs])[None, :])


def updated(cache, row, length):
    slots = lax.broadcasted_iota(jnp.int32, cache.shape, 0)
    return jnp.where(slots == length, row, cache.astype(F32)).astype(BF16)


def remote(src, dst, send_sem, recv_sem, ty, tx):
    return pltpu.make_async_remote_copy(
        src_ref=src, dst_ref=dst, send_sem=send_sem, recv_sem=recv_sem,
        device_id={"ty": ty, "tx": tx}, device_id_type=MESH,
    )


def project_kernel(
    ty_size, tile, d_model,
    x_main, x_kv, wq, wk, wv, wg, wu, gamma, lens, freqs,
    act_out, q_out, kv_out,
    spots, xs, ws, wkvs, gam, st, sr, p2, sd, sb, ra, rb, act, kvs, kvr, kvf, qs, qr,
    load_sem, pair_send, pair_recv, st_send, st_recv, ssem, rsem, kv_ssem, kv_rsem, kvf_sem, q_ssem, q_rsem, act_sem, out_sem,
):
    row_idx = lax.axis_index("ty")
    col_idx = lax.axis_index("tx")
    ring_pos, core = col_idx // 2, col_idx % 2
    other = 1 - core
    half_ty = ty_size // 2
    group = xs.shape[1]
    seq_block = group // 2
    rows = half_ty * group
    hrows = rows // 2
    hg = half_ty // 2
    kdim = xs.shape[2]
    kblk = kdim // 2
    steps = wg.shape[1] // tile
    head_dim = freqs.shape[1]
    q_width = wq.shape[1]
    pos_p, pos_m, pos_o = (ring_pos + 1) % RING, (ring_pos + RING - 1) % RING, (ring_pos + 2) % RING
    tx_p, tx_m, tx_o = pos_p * 2 + core, pos_m * 2 + core, pos_o * 2 + core
    tx_pair = ring_pos * 2 + other
    lanes = pl.ds(pl.multiple_of(core * kblk, LANES), kblk)
    krows = pl.ds(pl.multiple_of(core * kblk, LANES), kblk)

    pieces = []
    for d in range(RING):
        pieces.append((lambda c, d=d: x_main.at[c, :, d], xs.at[pl.ds(d * half_ty, half_ty), :, lanes]))
    pieces.append((lambda c: x_kv.at[row_idx], xs.at[pl.ds(RING * half_ty, RING), :, lanes]))
    pieces.append((lambda c: gamma, gam.at[core]))
    pieces.append((lambda c: wq, ws.at[0, krows, pl.ds(0, q_width)]))
    kv_piece = len(pieces)
    pieces.append((lambda c: wk, wkvs.at[krows]))
    for t in range(steps):
        pieces.append((lambda c, t=t: wg.at[:, pl.ds(t * tile, tile)], ws.at[t + 1, krows, pl.ds(0, tile)]))
        pieces.append((lambda c, t=t: wu.at[:, pl.ds(t * tile, tile)], ws.at[t + 1, krows, pl.ds(tile, tile)]))
    loads = [pltpu.make_async_copy(src(core), dst, load_sem.at[n]) for n, (src, dst) in enumerate(pieces)]
    swaps = [remote(src(other), dst, pair_send.at[n], pair_recv.at[n], row_idx, tx_pair) for n, (src, dst) in enumerate(pieces)]
    def start(copies, kv_copies, wants, first):
        for n, copy in enumerate(copies):
            if n < first:
                continue
            if n != kv_piece:
                copy.start()
            else:
                for which in BOTH:
                    pl.when(wants == which)(kv_copies[which].start)

    start(loads, [pltpu.make_async_copy(w, wkvs.at[krows], load_sem.at[kv_piece]) for w in (wk, wv)], core, 0)
    st[...] = jnp.zeros_like(st)

    barrier = pltpu.get_barrier_semaphore()
    pl.semaphore_signal(barrier, device_id={"ty": row_idx, "tx": tx_pair}, device_id_type=MESH)
    for tx in (tx_p, tx_m, tx_o):
        pl.semaphore_signal(barrier, device_id={"ty": row_idx, "tx": tx}, device_id_type=MESH)
    for off in range(1, ty_size):
        for cc in BOTH:
            pl.semaphore_signal(
                barrier, device_id={"ty": (row_idx + off) % ty_size, "tx": ring_pos * 2 + cc}, device_id_type=MESH
            )
    pl.semaphore_wait(barrier, 4 + 2 * (ty_size - 1))
    kv_swaps = [
        remote(w, wkvs.at[krows], pair_send.at[kv_piece], pair_recv.at[kv_piece], row_idx, tx_pair) for w in (wk, wv)
    ]
    for swap in swaps[: kv_piece - 1]:
        swap.start()

    blk = 2 * group
    blocks = (RING * half_ty + RING) // 2
    per_dest = half_ty // 2
    lane_tiles, slab_tiles = kdim // LANES, kblk // LANES

    def add_stats(slab, first, count):
        def stat_block(b, _):
            def lane_tile(j, sums):
                tile_lanes = pl.ds(pl.multiple_of(slab * kblk + j * LANES, LANES), LANES)
                part = xs[pl.ds(2 * b, 2), :, tile_lanes].reshape(blk, LANES).astype(F32)
                return sums[0] + part, sums[1] + part * part
            zero = jnp.zeros((blk, LANES), F32)
            sums = lax.fori_loop(0, kblk // LANES, lane_tile, (zero, zero))
            for which in BOTH:
                line = pl.ds(b + which * (st.shape[0] // 2), 1)
                st[line, pl.ds(0, blk)] += jnp.sum(sums[which].T, axis=0, keepdims=True)
            return 0

        lax.fori_loop(first, first + count, stat_block, 0)

    for n in range(kv_piece - 1):
        loads[n].wait()
    add_stats(core, 0, blocks)
    for n in range(kv_piece - 1):
        swaps[n].wait_recv()
        if n <= RING:
            add_stats(other, n * per_dest, per_dest if n < RING else RING // 2)
    start(swaps, kv_swaps, other, kv_piece - 1)
    stat_copies = [
        remote(st, sr.at[n], st_send.at[n], st_recv.at[n], row_idx, tx) for n, tx in enumerate((tx_p, tx_m, tx_o))
    ]
    for copy in stat_copies:
        copy.start()
    for copy in stat_copies:
        copy.wait()
    total = ((st[...] + sr[0]) + (sr[1] + sr[2]))
    mean = total[: st.shape[0] // 2] / d_model
    var = total[st.shape[0] // 2 :] / d_model - mean * mean
    sr[0, : st.shape[0] // 2, :] = mean
    sr[1, : st.shape[0] // 2, :] = lax.rsqrt(var + EPSILON)

    def norm_block(b, _):
        mean_b = jnp.broadcast_to(sr[0, pl.ds(b, 1), :], (128, LANES)).T[:blk]
        rstd_b = jnp.broadcast_to(sr[1, pl.ds(b, 1), :], (128, LANES)).T[:blk]
        for j in range(lane_tiles):
            cols = slice(j * 128, (j + 1) * LANES)
            part = xs[pl.ds(2 * b, 2), :, cols].reshape(blk, LANES).astype(F32)
            normed = ((part - mean_b) * rstd_b * gam[j // slab_tiles, pl.ds(j % slab_tiles, 1), :]).astype(BF16)
            xs[pl.ds(2 * b, 2), :, cols] = normed.reshape(2, group, LANES)
        return 0


    def norm_dest(d, count):
        lax.fori_loop(d * per_dest, d * per_dest + count, norm_block, 0)


    def left(start, count):
        return xs[pl.ds(start, count)].reshape(count * group, kdim)

    def mm(start, count, w):
        return jnp.dot(left(start, count), w, preferred_element_type=F32)

    def hop(s, n, kind, side):
        cols = pl.ds(0, n)
        src, dst = (
            (p2.at[s, pl.ds(side * hrows, hrows), cols], ra.at[s, side, :, cols]),
            (sd.at[s, side, :, cols], rb.at[s, side, 0, :, cols]),
            (sb.at[s, side, :, cols], rb.at[s, side, 1, :, cols]),
        )[kind]
        return remote(src, dst, ssem.at[s, kind, side], rsem.at[s, kind, side], row_idx, (tx_p, tx_m)[side])

    def stage_far(s, n):
        w = ws[s, :, 0:n]
        p2[s, :, 0:n] = mm(pos_o * half_ty, half_ty, w).astype(BF16)
        hop(s, n, 0, 0).start()
        hop(s, n, 0, 1).start()

    def stage_near(s, n):
        w = ws[s, :, 0:n]
        sd[s, 0, :, 0:n] = mm(pos_p * half_ty + hg, hg, w).astype(BF16)
        hop(s, n, 1, 0).start()
        sd[s, 1, :, 0:n] = mm(pos_m * half_ty, hg, w).astype(BF16)
        hop(s, n, 1, 1).start()

    def stage_a(s, n):
        stage_far(s, n)
        stage_near(s, n)

    def stage_b(s, n):
        w = ws[s, :, 0:n]
        for side, start in ((0, pos_p * half_ty), (1, pos_m * half_ty + hg)):
            own = mm(start, hg, w)
            hop(s, n, 0, side).wait_recv()
            sb[s, side, :, 0:n] = (own + ra[s, side, :, 0:n].astype(F32)).astype(BF16)
            hop(s, n, 2, side).start()

    def stage_c(s, n, finish):
        w = ws[s, :, 0:n]
        for half in BOTH:
            own = mm(ring_pos * half_ty + half * hg, hg, w)
            hop(s, n, 2, half).wait_recv()
            hop(s, n, 1, 1 - half).wait_recv()
            finish(half, own + rb[s, half, 1, :, 0:n].astype(F32) + rb[s, 1 - half, 0, :, 0:n].astype(F32))

    low = lax.broadcasted_iota(jnp.int32, (group, head_dim), 1) < head_dim // 2

    def tables(index, turns):
        start = index * group
        line = start // LANES
        for n, at in enumerate((line, jnp.minimum(line + 1, lens.shape[0] - 1))):
            down_rows = jnp.broadcast_to(lens[pl.ds(at, 1), :].astype(F32), (LANES, LANES)).T
            spots[pl.ds(n * LANES, LANES), :] = down_rows
        angles = spots[pl.ds(pl.multiple_of(start % LANES, 8), group), :] * (freqs[...] * turns)
        sines = jnp.sin(angles)
        return jnp.cos(angles), jnp.where(low, -sines, sines)

    def turn(vals, cos2, sin2):
        return vals * cos2 + pltpu.roll(vals, head_dim // 2, 1) * sin2

    def finish_q(half, vals):
        for g in range(hg):
            cos2, sin2 = tables((core * half_ty + half * hg + g) * RING + ring_pos, 1.0)
            for h in range(q_width // head_dim):
                cols = slice(h * head_dim, (h + 1) * head_dim)
                turned = turn(vals[g * group : (g + 1) * group, cols], cos2, sin2).astype(BF16)
                for k in BOTH:
                    qs[2 * (half * hg + g) + k, :, cols] = turned[k * seq_block : (k + 1) * seq_block]

    def act_copy(s):
        tile_lanes = pl.ds(pl.multiple_of((s - 1) * tile, tile), tile)
        return pltpu.make_async_copy(act.at[:, tile_lanes], act_out.at[:, tile_lanes], act_sem.at[s])

    def finish_mlp(s):
        def finish(half, vals):
            gate = vals[:, :tile].astype(BF16).astype(F32)
            up = vals[:, tile:].astype(BF16).astype(F32)
            act[pl.ds(half * hrows, hrows), pl.ds(pl.multiple_of((s - 1) * tile, tile), tile)] = (
                gate * jax.nn.sigmoid(gate) * up
            ).astype(BF16)
            if half:
                act_copy(s).start()
        return finish

    def q_copy(k):
        return remote(
            qs.at[k], qr.at[row_idx], q_ssem.at[k], q_rsem.at[row_idx],
            core * half_ty + k // 2, ring_pos * 2 + k % 2,
        )

    def q_is_self(k):
        return jnp.logical_and(core * half_ty + k // 2 == row_idx, core == k % 2)

    def kv_copy(n, pos):
        return remote(kvs.at[pos], kvr.at[n], kv_ssem.at[n], kv_rsem.at[n], row_idx, pos * 2 + core)

    wide = 2 * tile
    norm_dest(pos_o, per_dest)
    for n in (kv_piece - 1, kv_piece):
        loads[n].wait()
        swaps[n].wait_recv()
    stage_far(0, q_width)
    norm_dest(pos_p, per_dest)
    norm_dest(pos_m, per_dest)
    stage_near(0, q_width)
    norm_dest(RING, 2)
    kvs[...] = mm(RING * half_ty, RING, wkvs[...]).reshape(kvs.shape)
    for n, pos in enumerate((pos_p, pos_m, pos_o)):
        kv_copy(n, pos).start()
    norm_dest(ring_pos, per_dest)

    def weights_here(first, last):
        for n in range(kv_piece + 2 * first - 1, kv_piece + 2 * last + 1):
            loads[n].wait()
            swaps[n].wait_recv()

    weights_here(1, 1)
    stage_a(1, wide)
    stage_b(0, q_width)
    for n, pos in enumerate((pos_p, pos_m, pos_o)):
        kv_copy(n, pos).wait_recv()
    new_row = (kvs[ring_pos] + kvr[0]) + (kvr[1] + kvr[2])
    kvf[core] = turn(new_row, *tables(row_idx * RING + ring_pos, other.astype(F32))).astype(BF16)
    kv_pair = remote(kvf.at[core], kvf.at[core], kvf_sem.at[0], kvf_sem.at[1], row_idx, tx_pair)
    kv_pair.start()
    weights_here(2, 2)
    stage_a(2, wide)
    stage_b(1, wide)
    stage_c(0, q_width, finish_q)
    for k in range(ty_size):
        @pl.when(q_is_self(k))
        def _():
            pltpu.make_async_copy(qs.at[k], qr.at[row_idx], q_rsem.at[row_idx]).start()

        @pl.when(jnp.logical_not(q_is_self(k)))
        def _():
            q_copy(k).start()

    def middle(s, _):
        stage_a(s, wide)
        stage_b(s - 1, wide)
        stage_c(s - 2, wide, finish_mlp(s - 2))
        return 0

    weights_here(3, steps)
    lax.fori_loop(3, steps + 1, middle, 0)
    stage_b(steps, wide)
    stage_c(steps - 1, wide, finish_mlp(steps - 1))
    stage_c(steps, wide, finish_mlp(steps))

    outs = [
        pltpu.make_async_copy(qr, q_out, out_sem.at[0]),
        pltpu.make_async_copy(kvf, kv_out, out_sem.at[1]),
    ]
    for k in range(ty_size):
        remote(qs.at[0], qr.at[k], q_ssem.at[0], q_rsem.at[k], row_idx, tx_pair).wait_recv()
    outs[0].start()
    kv_pair.wait_send()
    remote(kvf.at[other], kvf.at[other], kvf_sem.at[0], kvf_sem.at[1], row_idx, tx_pair).wait_recv()
    outs[1].start()
    for k in range(ty_size):
        @pl.when(jnp.logical_not(q_is_self(k)))
        def _():
            q_copy(k).wait_send()
    for n, pos in enumerate((pos_p, pos_m, pos_o)):
        kv_copy(n, pos).wait_send()
    for swap in swaps:
        swap.wait_send()
    for kind in KINDS:
        for side in BOTH:
            hop(0, q_width, kind, side).wait_send()

    def drain(s, _):
        act_copy(s).wait()
        for kind in KINDS:
            for side in BOTH:
                hop(s, wide, kind, side).wait_send()
        return 0

    lax.fori_loop(1, steps + 1, drain, 0)
    for out in outs:
        out.wait()


def project(x_blk, gamma_blk, wq, wk, wv, wg, wu, lens, head_dim, ty_size, seq_block, d_model, tile):
    rows_all, kblk = x_blk.shape
    half_ty, group = ty_size // TWO, TWO * seq_block
    rows = half_ty * group
    q_width, ffn = wq.shape[1], wg.shape[1]
    kv_width = wk.shape[1]
    steps = ffn // tile
    wide = 2 * tile
    kdim = 2 * kblk
    x_main = x_blk.reshape(TWO, half_ty, RING, group, kblk)
    x_kv = x_blk.reshape(ty_size, RING, group, kblk)
    pieces = RING + 4 + 2 * steps
    stat_lines = 2 * (-(-((RING * half_ty + RING) // TWO) // 8) * 8)
    any_spec = pl.BlockSpec(memory_space=pl.ANY)
    vmem_spec = pl.BlockSpec(memory_space=pltpu.VMEM)
    return pl.pallas_call(
        functools.partial(project_kernel, ty_size, tile, d_model),
        out_shape=(
            jax.ShapeDtypeStruct((rows, ffn), BF16),
            jax.ShapeDtypeStruct((ty_size, seq_block, q_width), BF16),
            jax.ShapeDtypeStruct((TWO, group, kv_width), BF16),
        ),
        in_specs=[any_spec] * 8 + [vmem_spec] * 2,
        out_specs=(any_spec,) * 3,
        scratch_shapes=[
            pltpu.VMEM((TWO * LANES, LANES), F32),
            pltpu.VMEM((RING * half_ty + RING, group, kdim), BF16),
            pltpu.VMEM((steps + 1, kdim, wide), BF16),
            pltpu.VMEM((kdim, kv_width), BF16),
            pltpu.VMEM((CORES, kblk // LANES, LANES), F32),
            pltpu.VMEM((stat_lines, LANES), F32),
            pltpu.VMEM((3, stat_lines, LANES), F32),
            pltpu.VMEM((steps + 1, rows, wide), BF16),
            pltpu.VMEM((steps + 1, TWO, rows // TWO, wide), BF16),
            pltpu.VMEM((steps + 1, TWO, rows // TWO, wide), BF16),
            pltpu.VMEM((steps + 1, TWO, rows // TWO, wide), BF16),
            pltpu.VMEM((steps + 1, TWO, TWO, rows // TWO, wide), BF16),
            pltpu.VMEM((rows, ffn), BF16),
            pltpu.VMEM((RING, group, kv_width), F32),
            pltpu.VMEM((3, group, kv_width), F32),
            pltpu.VMEM((TWO, group, kv_width), BF16),
            pltpu.VMEM((ty_size, seq_block, q_width), BF16),
            pltpu.VMEM((ty_size, seq_block, q_width), BF16),
            pltpu.SemaphoreType.DMA((pieces,)),
            pltpu.SemaphoreType.DMA((pieces,)),
            pltpu.SemaphoreType.DMA((pieces,)),
            pltpu.SemaphoreType.DMA((len(KINDS),)),
            pltpu.SemaphoreType.DMA((len(KINDS),)),
            pltpu.SemaphoreType.DMA((steps + 1, len(KINDS), TWO)),
            pltpu.SemaphoreType.DMA((steps + 1, len(KINDS), TWO)),
            pltpu.SemaphoreType.DMA((len(KINDS),)),
            pltpu.SemaphoreType.DMA((len(KINDS),)),
            pltpu.SemaphoreType.DMA((TWO,)),
            pltpu.SemaphoreType.DMA((ty_size,)),
            pltpu.SemaphoreType.DMA((ty_size,)),
            pltpu.SemaphoreType.DMA((steps + 1,)),
            pltpu.SemaphoreType.DMA((TWO,)),
        ],
        compiler_params=pltpu.CompilerParams(
            collective_id=0, has_side_effects=True, vmem_limit_bytes=56 * MIB
        ),
        name="project",
    )(
        x_main, x_kv, wq, wk, wv, wg, wu, gamma_blk.reshape(-1, LANES), lens.reshape(-1, LANES), inverse_freqs(head_dim)
    )


def combine_kernel(
    ty_size,
    q_in, kv_in, k_in, v_in, act_in, x_in, wo, wd, lens,
    y_out,
    kvn, kv_f32, kc, vc, q_raw, q_f32, o_f32, att_out, att, mlp, wos, wds, yp, t1, xr, yf, p2_1, sd_1, sb_1, ra_1, rb_1, p2_2, sd_2, sb_2, ra_2, rb_2, ex,
    qkv_sem, w_sem, wp_send, wp_recv, a2a_send, a2a_recv, mlp_sem, gx_send, gx_recv, x_sem, xp_send, xp_recv,
    rs_send, rs_recv, ag_send, ag_recv, out_sem, outp_send, outp_recv,
):
    row_idx = lax.axis_index("ty")
    col_idx = lax.axis_index("tx")
    ring_pos, core = col_idx // 2, col_idx % 2
    other = 1 - core
    half_ty = ty_size // 2
    chunks = len(SIZES)
    begin = [sum(SIZES[:r]) for r in range(chunks)]
    seq_block = q_in.shape[1]
    group = 2 * seq_block
    cols = wo.shape[1]
    hcols = cols // 2
    pos_p, pos_m = (ring_pos + 1) % RING, (ring_pos + RING - 1) % RING
    tx_side = (pos_p * 2 + core, pos_m * 2 + core)
    from_side = (pos_m, pos_p)
    tx_pair = ring_pos * 2 + other
    z_pos, y_pos = row_idx // RING, row_idx % RING
    up = lambda v: (v + 1) % RING
    down = lambda v: (v + RING - 1) % RING
    y_side = (z_pos * RING + up(y_pos), z_pos * RING + down(y_pos))
    z_side = (up(z_pos) * RING + y_pos, down(z_pos) * RING + y_pos)
    places = ((y_pos, z_pos), (z_pos, y_pos))
    sides = ((y_side, z_side), (z_side, y_side))
    exchange = [size == 1 for size in SIZES]
    mine = pl.ds(pl.multiple_of(core * cols, LANES), cols)

    def units(r):
        return pl.ds(begin[r] * 2 * RING, SIZES[r] * 2 * RING)

    def block_units(r, b):
        return pl.ds(begin[r] * 2 * RING + b * 2 * SIZES[r], 2 * SIZES[r])

    def unit(r, b1, b2):
        return begin[r] * 2 * RING + b1 * 2 * SIZES[r] + b2

    def x_tile(c, r):
        b1, b2 = jnp.where(core == 0, y_pos, z_pos), jnp.where(core == 0, z_pos, y_pos)
        return x_in.at[c, block_units(r, b1) if exchange[r] else pl.ds(unit(r, b1, b2), 1)]

    def x_slot(c, r):
        return xr.at[c, r, pl.ds(0, 2 * SIZES[r] if exchange[r] else 1)]

    def own(r):
        return pl.ds(begin[r], SIZES[r])

    w_loads = [pltpu.make_async_copy(wd, wds.at[:, mine], w_sem.at[0]), pltpu.make_async_copy(wo, wos.at[:, mine], w_sem.at[1])]
    w_swaps = [
        remote(wd, wds.at[:, mine], wp_send.at[0], wp_recv.at[0], row_idx, tx_pair),
        remote(wo, wos.at[:, mine], wp_send.at[1], wp_recv.at[1], row_idx, tx_pair),
    ]
    mlp_loads = [pltpu.make_async_copy(act_in.at[own(r)], mlp.at[own(r), ring_pos], mlp_sem.at[r]) for r in range(chunks)]
    x_loads = [pltpu.make_async_copy(x_tile(core, r), x_slot(core, r), x_sem.at[r]) for r in range(chunks)]
    x_swaps = [remote(x_tile(other, r), x_slot(core, r), xp_send.at[r], xp_recv.at[r], row_idx, tx_pair) for r in range(chunks)]
    qkv_loads = [
        pltpu.make_async_copy(src, dst, qkv_sem.at[n])
        for n, (src, dst) in enumerate(((q_in, q_raw), (kv_in, kvn), (k_in, kc), (v_in, vc)))
    ]
    for load in qkv_loads + w_loads + mlp_loads + x_loads:
        load.start()

    barrier = pltpu.get_barrier_semaphore()
    pl.semaphore_signal(barrier, device_id={"ty": row_idx, "tx": tx_pair}, device_id_type=MESH)
    for tx in tx_side:
        pl.semaphore_signal(barrier, device_id={"ty": row_idx, "tx": tx}, device_id_type=MESH)
    for off in range(1, ty_size):
        for cc in BOTH:
            pl.semaphore_signal(
                barrier, device_id={"ty": (row_idx + off) % ty_size, "tx": ring_pos * 2 + cc}, device_id_type=MESH
            )
    pl.semaphore_wait(barrier, 3 + 2 * (ty_size - 1))

    def gather(r, part, stage, side):
        sems = gx_send.at[r, part, stage, side], gx_recv.at[r, part, stage, side]
        buf = (mlp, att)[part]
        if stage == 0:
            src = act_in.at[own(r)] if part == 0 else att.at[own(r), ring_pos]
            return remote(src, buf.at[own(r), ring_pos], *sems, row_idx, tx_side[side])
        if part == 0:
            lanes = mlp.shape[-1] // 2
            block = mlp.at[own(r), from_side[side], :, pl.ds(side * lanes, lanes)]
        else:
            block = att.at[own(r), from_side[side], side]
        return remote(block, block, *sems, row_idx, tx_side[side])

    home, home_core = row_idx % half_ty, row_idx // half_ty

    def a2a(k):
        return remote(
            att_out.at[k], att.at[home, ring_pos, core], a2a_send.at[k], a2a_recv.at[home, core],
            k, ring_pos * 2 + home_core,
        )

    def a2a_self(k):
        return jnp.logical_and(k == row_idx, core == home_core)

    def attend(_):
        heads, lines, head_dim = q_f32.shape
        for load in qkv_loads:
            load.wait()
        for k in range(ty_size):
            for h in range(heads):
                lanes = slice(h * head_dim, (h + 1) * head_dim)
                q_f32[h, k * seq_block : (k + 1) * seq_block, :] = q_raw[k, :, lanes].astype(F32)
        kv_f32[...] = kvn[...].astype(F32)
        slots = lax.broadcasted_iota(jnp.int32, (heads * ty_size, kc.shape[1]), 1)

        def sequence(b, _):
            picked = pl.ds(b, ty_size, stride=seq_block)
            fresh = pl.ds(core * seq_block + b, 1)
            length = lens[(row_idx * TWO * RING + col_idx) * seq_block + b]
            keys = updated(kc[b], kv_f32[0, fresh, :], length)
            vals = updated(vc[b], kv_f32[1, fresh, :], length)
            queries = jnp.concatenate([q_f32[h, picked, :] for h in range(heads)]).astype(BF16)
            scores = lax.dot_general(
                queries, keys, (((1,), (1,)), ((), ())), preferred_element_type=F32
            ) * (head_dim**-0.5)
            scores = jnp.where(slots <= length, scores, -1e30)
            weights = jnp.exp(scores - jnp.max(scores, axis=1, keepdims=True))
            probs = (weights / jnp.sum(weights, axis=1, keepdims=True)).astype(BF16)
            mixed = jnp.dot(probs, vals, preferred_element_type=F32)
            for h in range(heads):
                o_f32[h, picked, :] = mixed[h * ty_size : (h + 1) * ty_size]
            return 0

        lax.fori_loop(0, seq_block, sequence, 0, unroll=8)
        for k in range(ty_size):
            for h in range(heads):
                lanes = slice(h * head_dim, (h + 1) * head_dim)
                att_out[k, :, lanes] = o_f32[h, k * seq_block : (k + 1) * seq_block, :].astype(BF16)
        for k in range(ty_size):
            @pl.when(a2a_self(k))
            def _():
                pltpu.make_async_copy(
                    att_out.at[k], att.at[home, ring_pos, core], a2a_recv.at[home, core]
                ).start()

            @pl.when(jnp.logical_not(a2a_self(k)))
            def _():
                a2a(k).start()

    for swap in w_swaps + x_swaps:
        swap.start()

    def att_ready(r):
        for g in range(begin[r], begin[r] + SIZES[r]):
            for cc in BOTH:
                remote(
                    att_out.at[0], att.at[g, ring_pos, cc], a2a_send.at[0], a2a_recv.at[g, cc], row_idx, tx_pair
                ).wait_recv()

    def own_att(r):
        att_ready(r)
        for side in BOTH:
            gather(r, 1, 0, side).start()

    def own_mlp(r):
        for side in BOTH:
            gather(r, 0, 0, side).start()

    def forward(part, r):
        for side in BOTH:
            gather(r, part, 0, side).wait_recv()
            gather(r, part, 1, side).start()

    def multiply(r):
        mlp_loads[r].wait()
        for part in BOTH:
            for side in BOTH:
                gather(r, part, 1, side).wait_recv()
        rows = SIZES[r] * RING * group

        def tile(n, _):
            lanes = pl.ds(pl.multiple_of(n * TILE, TILE), TILE)
            left_mlp = mlp[own(r)].reshape(rows, mlp.shape[-1])
            left_att = att[own(r)].reshape(rows, att.shape[-1])
            yp[pl.ds(begin[r] * RING * group, rows), lanes] = jnp.dot(
                left_mlp, wds[:, lanes], preferred_element_type=F32
            ) + jnp.dot(left_att, wos[:, lanes], preferred_element_type=F32)
            return 0

        lax.fori_loop(0, yp.shape[1] // TILE, tile, 0)

    bufs = ((p2_1, sd_1, sb_1, ra_1, rb_1), (p2_2, sd_2, sb_2, ra_2, rb_2))

    def block_rows(level, r):
        return (SIZES[r] * group, seq_block)[level]

    def hop(level, r, c, kind, side):
        p2, sd, sb, ra, rb = bufs[level]
        m = pl.ds(0, block_rows(level, r))
        src, dst = (
            (p2.at[r, c, m, pl.ds(side * hcols, hcols)], ra.at[r, c, side, m]),
            (sd.at[r, c, side, m], rb.at[r, c, side, 0, m]),
            (sb.at[r, c, side, m], rb.at[r, c, side, 1, m]),
        )[kind]
        return remote(
            src, dst, rs_send.at[level, r, c, kind, side], rs_recv.at[level, r, c, kind, side],
            sides[c][level][side], col_idx,
        )

    def part_of(level, r, c, b, half):
        size = block_rows(level, r)
        if level == 0:
            rows = pl.ds(pl.multiple_of(begin[r] * RING * group + b * size, 8), size)
            return yp[rows, c * cols + half * hcols : c * cols + (half + 1) * hcols]
        return t1[r, c, pl.ds(pl.multiple_of(b * size, 8), size), half * hcols : (half + 1) * hcols]

    def reduce_a(level, r):
        p2, sd = bufs[level][:2]
        m = block_rows(level, r)
        for c in BOTH:
            pos = places[c][level]
            for half in BOTH:
                p2[r, c, :m, half * hcols : (half + 1) * hcols] = part_of(level, r, c, (pos + 2) % RING, half).astype(BF16)
                hop(level, r, c, 0, half).start()
        for c in BOTH:
            pos = places[c][level]
            for side, b in enumerate((up(pos), down(pos))):
                sd[r, c, side, :m] = part_of(level, r, c, b, 1 - side).astype(BF16)
                hop(level, r, c, 1, side).start()

    def reduce_b(level, r):
        sb, ra = bufs[level][2:4]
        m = block_rows(level, r)
        for c in BOTH:
            pos = places[c][level]
            for side, b in enumerate((up(pos), down(pos))):
                hop(level, r, c, 0, side).wait_recv()
                sb[r, c, side, :m] = (part_of(level, r, c, b, side) + ra[r, c, side, :m].astype(F32)).astype(BF16)
                hop(level, r, c, 2, side).start()

    def reduce_c(level, r, finish):
        rb = bufs[level][4]
        m = block_rows(level, r)
        for c in BOTH:
            pos = places[c][level]
            for half in BOTH:
                hop(level, r, c, 1, 1 - half).wait_recv()
                hop(level, r, c, 2, half).wait_recv()
                finish(
                    c, half,
                    part_of(level, r, c, pos, half)
                    + rb[r, c, half, 1, :m].astype(F32) + rb[r, c, 1 - half, 0, :m].astype(F32),
                )

    def spread(level, r, c, stage, side):
        ring, (p1, p2) = sides[c][level], places[c]
        sems = ag_send.at[level, r, c, stage, side], ag_recv.at[level, r, c, stage, side]
        near = (down, up)[side]
        half = pl.ds(side * hcols, hcols)
        if level == 1 and exchange[r]:
            m = pl.ds(0, block_rows(0, r))
            block = ex.at[r, c, p2, m] if stage == 0 else ex.at[r, c, near(p2), m, half]
        elif level == 1:
            block = yf.at[c, unit(r, p1, p2)] if stage == 0 else yf.at[c, unit(r, p1, near(p2)), :, half]
        elif stage == 0:
            block = yf.at[c, block_units(r, p1)]
        else:
            block = yf.at[c, pl.ds(unit(r, near(p1), side * SIZES[r]), SIZES[r])]
        return remote(block, block, *sems, ring[side], col_idx)

    def spread_own(level, r):
        for c in BOTH:
            for side in BOTH:
                spread(level, r, c, 0, side).start()

    def spread_on(level, r):
        for c in BOTH:
            for side in BOTH:
                spread(level, r, c, 0, side).wait_recv()
                spread(level, r, c, 1, side).start()

    def spread_end(level, r):
        for c in BOTH:
            for side in BOTH:
                spread(level, r, c, 1, side).wait_recv()

    def s3(r):
        reduce_b(0, r)

    def s4(r):
        m = block_rows(0, r)

        def finish(c, half, vals):
            lanes = slice(half * hcols, (half + 1) * hcols)
            if exchange[r]:
                ex[r, c, places[c][1], :m, lanes] = vals.astype(BF16)
            else:
                t1[r, c, :m, lanes] = vals
        reduce_c(0, r, finish)
        if exchange[r]:
            spread_own(1, r)
        else:
            reduce_a(1, r)

    def s5(r):
        if exchange[r]:
            spread_on(1, r)
        else:
            reduce_b(1, r)

    def s6(r):
        x_loads[r].wait()
        remote(x_tile(other, r), x_slot(other, r), xp_send.at[r], xp_recv.at[r], row_idx, tx_pair).wait_recv()
        if exchange[r]:
            m = block_rows(0, r)
            spread_end(1, r)
            for c in BOTH:
                for n in range(2 * SIZES[r]):
                    rows = slice(n * seq_block, (n + 1) * seq_block)
                    first, second, third, fourth = (ex[r, c, p, rows].astype(F32) for p in range(RING))
                    total = (first + second) + (third + fourth)
                    yf[c, unit(r, places[c][0], n)] = (xr[c, r, n].astype(F32) + total).astype(BF16)
            spread_own(0, r)
        else:
            def finish(c, half, vals):
                lanes = slice(half * hcols, (half + 1) * hcols)
                yf[c, unit(r, *places[c]), :, lanes] = (xr[c, r, 0, :, lanes].astype(F32) + vals).astype(BF16)
            reduce_c(1, r, finish)
            spread_own(1, r)

    def s7(r):
        spread_on(1, r)

    def s8(r):
        spread_end(1, r)
        spread_own(0, r)

    def s9(r):
        spread_on(0, r)

    def out_copy(r):
        return pltpu.make_async_copy(yf.at[core, units(r)], y_out.at[core, units(r)], out_sem.at[r])

    def out_swap(r):
        return remote(
            yf.at[other, units(r)], y_out.at[core, units(r)], outp_send.at[r], outp_recv.at[r], row_idx, tx_pair
        )

    def s10(r):
        spread_end(0, r)
        out_swap(r).start()
        out_copy(r).start()

    def s2(r):
        multiply(r)
        reduce_a(0, r)

    stages = dict(zip("mAagh23456789t", (
        own_mlp, attend, own_att, functools.partial(forward, 0), functools.partial(forward, 1),
        s2, s3, s4, s5, s6, s7, s8, s9, s10,
    )))
    products = ORDER[::TWO].index("2") * TWO
    for n in range(0, len(ORDER), TWO):
        if n == products:
            for load, swap in zip(w_loads, w_swaps):
                load.wait()
                swap.wait_recv()
        stages[ORDER[n]](int(ORDER[n + 1]))

    for swap in w_swaps + x_swaps:
        swap.wait_send()
    for k in range(ty_size):
        @pl.when(jnp.logical_not(a2a_self(k)))
        def _():
            a2a(k).wait_send()
    for r in range(chunks):
        for a in BOTH:
            for b in BOTH:
                for side in BOTH:
                    gather(r, a, b, side).wait_send()
                    for level in BOTH:
                        spread(level, r, a, b, side).wait_send()
        for level in BOTH[: 2 - exchange[r]]:
            for c in BOTH:
                for kind in KINDS:
                    for side in BOTH:
                        hop(level, r, c, kind, side).wait_send()
        out_copy(r).wait()
        out_swap(r).wait()


def combine(q_owned, kv_new, k_blk, v_blk, lens_own, act_own, x_blk, w_out, w_down, ty_size):
    seq_block = q_owned.shape[1]
    head_dim = k_blk.shape[TWO]
    chunks, most = len(SIZES), max(SIZES)
    group, half_ty = TWO * seq_block, ty_size // TWO
    cols = w_out.shape[1]
    hcols = cols // TWO
    ffn, q_width = w_down.shape[0], w_out.shape[0]
    any_spec = pl.BlockSpec(memory_space=pl.ANY)
    ring_bufs = []
    for m in (most * group, seq_block):
        half = (chunks, TWO, TWO, m, hcols)
        both = (chunks, TWO, TWO, TWO, m, hcols)
        ring_bufs += [pltpu.VMEM(shape, BF16) for shape in ((chunks, TWO, m, cols), half, half, half, both)]
    dma = pltpu.SemaphoreType.DMA
    y_units = (TWO, half_ty * RING * TWO, seq_block, cols)
    y = pl.pallas_call(
        functools.partial(combine_kernel, ty_size),
        out_shape=jax.ShapeDtypeStruct(y_units, BF16),
        in_specs=[any_spec] * 8 + [pl.BlockSpec(memory_space=pltpu.SMEM)],
        out_specs=any_spec,
        scratch_shapes=[
            pltpu.VMEM(kv_new.shape, BF16),
            pltpu.VMEM(kv_new.shape, F32),
            pltpu.VMEM(k_blk.shape, BF16),
            pltpu.VMEM(v_blk.shape, BF16),
            pltpu.VMEM(q_owned.shape, BF16),
            pltpu.VMEM((q_width // head_dim, ty_size * seq_block, head_dim), F32),
            pltpu.VMEM((q_width // head_dim, ty_size * seq_block, head_dim), F32),
            pltpu.VMEM(q_owned.shape, BF16),
            pltpu.VMEM((half_ty, RING, TWO, seq_block, q_width), BF16),
            pltpu.VMEM((half_ty, RING, group, ffn), BF16),
            pltpu.VMEM((q_width, TWO * cols), BF16),
            pltpu.VMEM((ffn, TWO * cols), BF16),
            pltpu.VMEM((half_ty * RING * group, TWO * cols), F32),
            pltpu.VMEM((chunks, TWO, most * group, cols), F32),
            pltpu.VMEM((TWO, chunks, TWO * most, seq_block, cols), BF16),
            pltpu.VMEM(y_units, BF16),
            *ring_bufs,
            pltpu.VMEM((chunks, TWO, RING, most * group, cols), BF16),
            dma((RING,)), dma((CORES,)), dma((CORES,)), dma((CORES,)),
            dma((ty_size,)), dma((half_ty, TWO)),
            dma((chunks,)),
            dma((chunks, TWO, TWO, TWO)), dma((chunks, TWO, TWO, TWO)),
            dma((chunks,)), dma((chunks,)), dma((chunks,)),
            dma((TWO, chunks, TWO, len(KINDS), TWO)), dma((TWO, chunks, TWO, len(KINDS), TWO)),
            dma((TWO, chunks, TWO, TWO, TWO)), dma((TWO, chunks, TWO, TWO, TWO)),
            dma((chunks,)), dma((chunks,)), dma((chunks,)),
        ],
        compiler_params=pltpu.CompilerParams(
            collective_id=1, has_side_effects=True, vmem_limit_bytes=60 * MIB
        ),
        name="combine",
    )(q_owned, kv_new, k_blk, v_blk, act_own.reshape(half_ty, group, ffn), x_blk.reshape(y_units), w_out, w_down, lens_own)
    return y.reshape(x_blk.shape)


def emit_kernel(pieces, y_in, kv_in, k_in, v_in, lens, y_out, k_out, v_out, ys, kvn, kv_f32, kc, vc, load_sem, y_sem, out_sem, y_out_sem):
    core = lax.axis_index("tx") % CORES
    seq_block = kc.shape[0]
    size = ys.shape[0] // pieces
    base = (lax.axis_index("ty") * TWO * RING + lax.axis_index("tx")) * seq_block
    loads = [
        pltpu.make_async_copy(src, dst, load_sem.at[n]) for n, (src, dst) in enumerate(((kv_in, kvn), (k_in, kc), (v_in, vc)))
    ]
    part = [pl.ds(n * size, size) for n in range(pieces)]
    y_loads = [pltpu.make_async_copy(y_in.at[p], ys.at[p], y_sem.at[n]) for n, p in enumerate(part)]
    y_stores = [pltpu.make_async_copy(ys.at[p], y_out.at[p], y_out_sem.at[n]) for n, p in enumerate(part)]
    stores = [pltpu.make_async_copy(kc, k_out, out_sem.at[0]), pltpu.make_async_copy(vc, v_out, out_sem.at[1])]
    for load in y_loads + loads:
        load.start()
    for load, store in zip(y_loads, y_stores):
        load.wait()
        store.start()
    for load in loads:
        load.wait()
    kv_f32[...] = kvn[...].astype(F32)

    def sequence(b, _):
        fresh = pl.ds(core * seq_block + b, 1)
        length = lens[base + b]
        kc[b] = updated(kc[b], kv_f32[0, fresh, :], length)
        vc[b] = updated(vc[b], kv_f32[1, fresh, :], length)
        return 0

    lax.fori_loop(0, seq_block, sequence, 0, unroll=4)
    for store in stores:
        store.start()
    for store in y_stores + stores:
        store.wait()


def emit(y, kv_new, k_blk, v_blk, lens_own):
    pieces = 8
    any_spec = pl.BlockSpec(memory_space=pl.ANY)
    dma = pltpu.SemaphoreType.DMA
    return pl.pallas_call(
        functools.partial(emit_kernel, pieces),
        out_shape=tuple(jax.ShapeDtypeStruct(a.shape, BF16) for a in (y, k_blk, v_blk)),
        in_specs=[any_spec] * RING + [pl.BlockSpec(memory_space=pltpu.SMEM)],
        out_specs=(any_spec,) * len(KINDS),
        scratch_shapes=[
            pltpu.VMEM(y.shape, BF16),
            pltpu.VMEM(kv_new.shape, BF16),
            pltpu.VMEM(kv_new.shape, F32),
            pltpu.VMEM(k_blk.shape, BF16),
            pltpu.VMEM(v_blk.shape, BF16),
            dma((len(KINDS),)), dma((pieces,)), dma((TWO,)), dma((pieces,)),
        ],
        compiler_params=pltpu.CompilerParams(vmem_limit_bytes=60 * MIB),
        name="emit",
    )(y, kv_new, k_blk, v_blk, lens_own)


def solution(mesh):
    ty_size = mesh.shape["ty"]
    tx_size = mesh.shape["tx"]
    cache_spec = P(("dp", "ty", "tx"), None, None)

    def layer_shard(x_blk, lens_part, k_blk, v_blk, gamma_blk, w_query, w_key, w_value, w_gate, w_up, w_out, w_down):
        rows = x_blk.shape[0]
        d_model = x_blk.shape[1] * tx_size
        seq_block, _, head_dim = k_blk.shape
        tile = min(256, w_gate.shape[1])

        act_own, q_owned, kv_new = project(
            x_blk, gamma_blk, w_query, w_key, w_value, w_gate, w_up, lens_part, head_dim,
            ty_size, seq_block, d_model, tile,
        )
        y_raw = combine(q_owned, kv_new, k_blk, v_blk, lens_part, act_own, x_blk, w_out, w_down, ty_size)
        y_blk, k_out, v_out = emit(y_raw, kv_new, k_blk, v_blk, lens_part)
        return y_blk, k_out, v_out

    in_specs = (P("dp", "tx"), P("dp"), cache_spec, cache_spec, P("tx"), P("tx", "ty"), P("tx", None), P("tx", None), P("tx", "ty"), P("tx", "ty"), P("ty", "tx"), P("ty", "tx"))
    out_specs = (P("dp", "tx"), cache_spec, cache_spec)
    return jax.shard_map(layer_shard, mesh=mesh, in_specs=in_specs, out_specs=out_specs, check_vma=False)
```

```python
import functools

import jax
import jax.numpy as jnp
import numpy as np
from jax import lax
from jax.experimental import pallas as pl
from jax.experimental.pallas import tpu as pltpu
from jax.sharding import PartitionSpec as P

EPSILON = 1e-6
ROPE_BASE = 10000.0
MESH = pl.DeviceIdType.MESH
RING = 4
CORES = 2
TWO = 2
LANES = 128
TILE = 512
BOTH = (0, 1)
KINDS = (0, 1, 2)
MIB = 2**20
SIZES = (2, 2, 2, 1, 1)
ORDER = (
    "m2m1A0a0a1g1h1a2m021h2g2h031g0m4a4m3412251a320g4h43230h3g361"
    + "2442407123345250816044336270915472438053t182636490929394t2t0"
    + "t3t4"
)
F32 = jnp.float32
BF16 = jnp.bfloat16


def inverse_freqs(head_dim):
    powers = np.arange(head_dim // 2, dtype=np.float32) * np.float32(2.0) / np.float32(head_dim)
    freqs = np.float32(ROPE_BASE) ** -powers
    return jnp.asarray(np.concatenate([freqs, freqs])[None, :])


def updated(cache, row, length):
    slots = lax.broadcasted_iota(jnp.int32, cache.shape, 0)
    return jnp.where(slots == length, row, cache.astype(F32)).astype(BF16)


def remote(src, dst, send_sem, recv_sem, ty, tx):
    return pltpu.make_async_remote_copy(
        src_ref=src, dst_ref=dst, send_sem=send_sem, recv_sem=recv_sem,
        device_id={"ty": ty, "tx": tx}, device_id_type=MESH,
    )


def project_kernel(
    ty_size, tile, d_model,
    x_main, x_kv, wq, wk, wv, wg, wu, gamma, lens, freqs,
    act_out, q_out, kv_out,
    spots, xs, ws, wkvs, gam, st, sr, p2, sd, sb, ra, rb, act, kvs, kvr, kvf, qs, qr,
    load_sem, pair_send, pair_recv, st_send, st_recv, ssem, rsem, kv_ssem, kv_rsem, kvf_sem, q_ssem, q_rsem, act_sem, out_sem,
):
    row_idx = lax.axis_index("ty")
    col_idx = lax.axis_index("tx")
    ring_pos, core = col_idx // 2, col_idx % 2
    other = 1 - core
    half_ty = ty_size // 2
    group = xs.shape[1]
    seq_block = group // 2
    rows = half_ty * group
    hrows = rows // 2
    hg = half_ty // 2
    kdim = xs.shape[2]
    kblk = kdim // 2
    steps = wg.shape[1] // tile
    head_dim = freqs.shape[1]
    q_width = wq.shape[1]
    pos_p, pos_m, pos_o = (ring_pos + 1) % RING, (ring_pos + RING - 1) % RING, (ring_pos + 2) % RING
    tx_p, tx_m, tx_o = pos_p * 2 + core, pos_m * 2 + core, pos_o * 2 + core
    tx_pair = ring_pos * 2 + other
    lanes = pl.ds(pl.multiple_of(core * kblk, LANES), kblk)
    krows = pl.ds(pl.multiple_of(core * kblk, LANES), kblk)

    pieces = []
    for d in range(RING):
        pieces.append((lambda c, d=d: x_main.at[c, :, d], xs.at[pl.ds(d * half_ty, half_ty), :, lanes]))
    pieces.append((lambda c: x_kv.at[row_idx], xs.at[pl.ds(RING * half_ty, RING), :, lanes]))
    pieces.append((lambda c: gamma, gam.at[core]))
    pieces.append((lambda c: wq, ws.at[0, krows, pl.ds(0, q_width)]))
    kv_piece = len(pieces)
    pieces.append((lambda c: wk, wkvs.at[krows]))
    for t in range(steps):
        pieces.append((lambda c, t=t: wg.at[:, pl.ds(t * tile, tile)], ws.at[t + 1, krows, pl.ds(0, tile)]))
        pieces.append((lambda c, t=t: wu.at[:, pl.ds(t * tile, tile)], ws.at[t + 1, krows, pl.ds(tile, tile)]))
    loads = [pltpu.make_async_copy(src(core), dst, load_sem.at[n]) for n, (src, dst) in enumerate(pieces)]
    swaps = [remote(src(other), dst, pair_send.at[n], pair_recv.at[n], row_idx, tx_pair) for n, (src, dst) in enumerate(pieces)]
    def start(copies, kv_copies, wants, first):
        for n, copy in enumerate(copies):
            if n < first:
                continue
            if n != kv_piece:
                copy.start()
            else:
                for which in BOTH:
                    pl.when(wants == which)(kv_copies[which].start)

    start(loads, [pltpu.make_async_copy(w, wkvs.at[krows], load_sem.at[kv_piece]) for w in (wk, wv)], core, 0)
    st[...] = jnp.zeros_like(st)

    barrier = pltpu.get_barrier_semaphore()
    pl.semaphore_signal(barrier, device_id={"ty": row_idx, "tx": tx_pair}, device_id_type=MESH)
    for tx in (tx_p, tx_m, tx_o):
        pl.semaphore_signal(barrier, device_id={"ty": row_idx, "tx": tx}, device_id_type=MESH)
    for off in range(1, ty_size):
        for cc in BOTH:
            pl.semaphore_signal(
                barrier, device_id={"ty": (row_idx + off) % ty_size, "tx": ring_pos * 2 + cc}, device_id_type=MESH
            )
    pl.semaphore_wait(barrier, 4 + 2 * (ty_size - 1))
    kv_swaps = [
        remote(w, wkvs.at[krows], pair_send.at[kv_piece], pair_recv.at[kv_piece], row_idx, tx_pair) for w in (wk, wv)
    ]
    for swap in swaps[: kv_piece - 1]:
        swap.start()

    blk = 2 * group
    blocks = (RING * half_ty + RING) // 2
    per_dest = half_ty // 2
    lane_tiles, slab_tiles = kdim // LANES, kblk // LANES

    def add_stats(slab, first, count):
        def stat_block(b, _):
            def lane_tile(j, sums):
                tile_lanes = pl.ds(pl.multiple_of(slab * kblk + j * LANES, LANES), LANES)
                part = xs[pl.ds(2 * b, 2), :, tile_lanes].reshape(blk, LANES).astype(F32)
                return sums[0] + part, sums[1] + part * part
            zero = jnp.zeros((blk, LANES), F32)
            sums = lax.fori_loop(0, kblk // LANES, lane_tile, (zero, zero))
            for which in BOTH:
                line = pl.ds(b + which * (st.shape[0] // 2), 1)
                st[line, pl.ds(0, blk)] += jnp.sum(sums[which].T, axis=0, keepdims=True)
            return 0

        lax.fori_loop(first, first + count, stat_block, 0)

    for n in range(kv_piece - 1):
        loads[n].wait()
    add_stats(core, 0, blocks)
    for n in range(kv_piece - 1):
        swaps[n].wait_recv()
        if n <= RING:
            add_stats(other, n * per_dest, per_dest if n < RING else RING // 2)
    start(swaps, kv_swaps, other, kv_piece - 1)
    stat_copies = [
        remote(st, sr.at[n], st_send.at[n], st_recv.at[n], row_idx, tx) for n, tx in enumerate((tx_p, tx_m, tx_o))
    ]
    for copy in stat_copies:
        copy.start()
    for copy in stat_copies:
        copy.wait()
    total = ((st[...] + sr[0]) + (sr[1] + sr[2]))
    mean = total[: st.shape[0] // 2] / d_model
    var = total[st.shape[0] // 2 :] / d_model - mean * mean
    sr[0, : st.shape[0] // 2, :] = mean
    sr[1, : st.shape[0] // 2, :] = lax.rsqrt(var + EPSILON)

    def norm_block(b, _):
        mean_b = jnp.broadcast_to(sr[0, pl.ds(b, 1), :], (128, LANES)).T[:blk]
        rstd_b = jnp.broadcast_to(sr[1, pl.ds(b, 1), :], (128, LANES)).T[:blk]
        for j in range(lane_tiles):
            cols = slice(j * 128, (j + 1) * LANES)
            part = xs[pl.ds(2 * b, 2), :, cols].reshape(blk, LANES).astype(F32)
            normed = ((part - mean_b) * rstd_b * gam[j // slab_tiles, pl.ds(j % slab_tiles, 1), :]).astype(BF16)
            xs[pl.ds(2 * b, 2), :, cols] = normed.reshape(2, group, LANES)
        return 0


    def norm_dest(d, count):
        lax.fori_loop(d * per_dest, d * per_dest + count, norm_block, 0)


    def left(start, count):
        return xs[pl.ds(start, count)].reshape(count * group, kdim)

    def mm(start, count, w):
        return jnp.dot(left(start, count), w, preferred_element_type=F32)

    def hop(s, n, kind, side):
        cols = pl.ds(0, n)
        src, dst = (
            (p2.at[s, pl.ds(side * hrows, hrows), cols], ra.at[s, side, :, cols]),
            (sd.at[s, side, :, cols], rb.at[s, side, 0, :, cols]),
            (sb.at[s, side, :, cols], rb.at[s, side, 1, :, cols]),
        )[kind]
        return remote(src, dst, ssem.at[s, kind, side], rsem.at[s, kind, side], row_idx, (tx_p, tx_m)[side])

    def stage_far(s, n):
        w = ws[s, :, 0:n]
        p2[s, :, 0:n] = mm(pos_o * half_ty, half_ty, w).astype(BF16)
        hop(s, n, 0, 0).start()
        hop(s, n, 0, 1).start()

    def stage_near(s, n):
        w = ws[s, :, 0:n]
        sd[s, 0, :, 0:n] = mm(pos_p * half_ty + hg, hg, w).astype(BF16)
        hop(s, n, 1, 0).start()
        sd[s, 1, :, 0:n] = mm(pos_m * half_ty, hg, w).astype(BF16)
        hop(s, n, 1, 1).start()

    def stage_a(s, n):
        stage_far(s, n)
        stage_near(s, n)

    def stage_b(s, n):
        w = ws[s, :, 0:n]
        for side, start in ((0, pos_p * half_ty), (1, pos_m * half_ty + hg)):
            own = mm(start, hg, w)
            hop(s, n, 0, side).wait_recv()
            sb[s, side, :, 0:n] = (own + ra[s, side, :, 0:n].astype(F32)).astype(BF16)
            hop(s, n, 2, side).start()

    def stage_c(s, n, finish):
        w = ws[s, :, 0:n]
        for half in BOTH:
            own = mm(ring_pos * half_ty + half * hg, hg, w)
            hop(s, n, 2, half).wait_recv()
            hop(s, n, 1, 1 - half).wait_recv()
            finish(half, own + rb[s, half, 1, :, 0:n].astype(F32) + rb[s, 1 - half, 0, :, 0:n].astype(F32))

    low = lax.broadcasted_iota(jnp.int32, (group, head_dim), 1) < head_dim // 2

    def tables(index, turns):
        start = index * group
        line = start // LANES
        for n, at in enumerate((line, jnp.minimum(line + 1, lens.shape[0] - 1))):
            down_rows = jnp.broadcast_to(lens[pl.ds(at, 1), :].astype(F32), (LANES, LANES)).T
            spots[pl.ds(n * LANES, LANES), :] = down_rows
        angles = spots[pl.ds(pl.multiple_of(start % LANES, 8), group), :] * (freqs[...] * turns)
        sines = jnp.sin(angles)
        return jnp.cos(angles), jnp.where(low, -sines, sines)

    def turn(vals, cos2, sin2):
        return vals * cos2 + pltpu.roll(vals, head_dim // 2, 1) * sin2

    def finish_q(half, vals):
        for g in range(hg):
            cos2, sin2 = tables((core * half_ty + half * hg + g) * RING + ring_pos, 1.0)
            for h in range(q_width // head_dim):
                cols = slice(h * head_dim, (h + 1) * head_dim)
                turned = turn(vals[g * group : (g + 1) * group, cols], cos2, sin2).astype(BF16)
                for k in BOTH:
                    qs[2 * (half * hg + g) + k, :, cols] = turned[k * seq_block : (k + 1) * seq_block]

    def act_copy(s):
        tile_lanes = pl.ds(pl.multiple_of((s - 1) * tile, tile), tile)
        return pltpu.make_async_copy(act.at[:, tile_lanes], act_out.at[:, tile_lanes], act_sem.at[s])

    def finish_mlp(s):
        def finish(half, vals):
            gate = vals[:, :tile].astype(BF16).astype(F32)
            up = vals[:, tile:].astype(BF16).astype(F32)
            act[pl.ds(half * hrows, hrows), pl.ds(pl.multiple_of((s - 1) * tile, tile), tile)] = (
                gate * jax.nn.sigmoid(gate) * up
            ).astype(BF16)
            if half:
                act_copy(s).start()
        return finish

    def q_copy(k):
        return remote(
            qs.at[k], qr.at[row_idx], q_ssem.at[k], q_rsem.at[row_idx],
            core * half_ty + k // 2, ring_pos * 2 + k % 2,
        )

    def q_is_self(k):
        return jnp.logical_and(core * half_ty + k // 2 == row_idx, core == k % 2)

    def kv_copy(n, pos):
        return remote(kvs.at[pos], kvr.at[n], kv_ssem.at[n], kv_rsem.at[n], row_idx, pos * 2 + core)

    wide = 2 * tile
    norm_dest(pos_o, per_dest)
    for n in (kv_piece - 1, kv_piece):
        loads[n].wait()
        swaps[n].wait_recv()
    stage_far(0, q_width)
    norm_dest(pos_p, per_dest)
    norm_dest(pos_m, per_dest)
    stage_near(0, q_width)
    norm_dest(RING, 2)
    kvs[...] = mm(RING * half_ty, RING, wkvs[...]).reshape(kvs.shape)
    for n, pos in enumerate((pos_p, pos_m, pos_o)):
        kv_copy(n, pos).start()
    norm_dest(ring_pos, per_dest)

    def weights_here(first, last):
        for n in range(kv_piece + 2 * first - 1, kv_piece + 2 * last + 1):
            loads[n].wait()
            swaps[n].wait_recv()

    weights_here(1, 1)
    stage_a(1, wide)
    stage_b(0, q_width)
    for n, pos in enumerate((pos_p, pos_m, pos_o)):
        kv_copy(n, pos).wait_recv()
    new_row = (kvs[ring_pos] + kvr[0]) + (kvr[1] + kvr[2])
    kvf[core] = turn(new_row, *tables(row_idx * RING + ring_pos, other.astype(F32))).astype(BF16)
    kv_pair = remote(kvf.at[core], kvf.at[core], kvf_sem.at[0], kvf_sem.at[1], row_idx, tx_pair)
    kv_pair.start()
    weights_here(2, 2)
    stage_a(2, wide)
    stage_b(1, wide)
    stage_c(0, q_width, finish_q)
    for k in range(ty_size):
        @pl.when(q_is_self(k))
        def _():
            pltpu.make_async_copy(qs.at[k], qr.at[row_idx], q_rsem.at[row_idx]).start()

        @pl.when(jnp.logical_not(q_is_self(k)))
        def _():
            q_copy(k).start()

    def middle(s, _):
        stage_a(s, wide)
        stage_b(s - 1, wide)
        stage_c(s - 2, wide, finish_mlp(s - 2))
        return 0

    weights_here(3, steps)
    lax.fori_loop(3, steps + 1, middle, 0)
    stage_b(steps, wide)
    stage_c(steps - 1, wide, finish_mlp(steps - 1))
    stage_c(steps, wide, finish_mlp(steps))

    outs = [
        pltpu.make_async_copy(qr, q_out, out_sem.at[0]),
        pltpu.make_async_copy(kvf, kv_out, out_sem.at[1]),
    ]
    for k in range(ty_size):
        remote(qs.at[0], qr.at[k], q_ssem.at[0], q_rsem.at[k], row_idx, tx_pair).wait_recv()
    outs[0].start()
    kv_pair.wait_send()
    remote(kvf.at[other], kvf.at[other], kvf_sem.at[0], kvf_sem.at[1], row_idx, tx_pair).wait_recv()
    outs[1].start()
    for k in range(ty_size):
        @pl.when(jnp.logical_not(q_is_self(k)))
        def _():
            q_copy(k).wait_send()
    for n, pos in enumerate((pos_p, pos_m, pos_o)):
        kv_copy(n, pos).wait_send()
    for swap in swaps:
        swap.wait_send()
    for kind in KINDS:
        for side in BOTH:
            hop(0, q_width, kind, side).wait_send()

    def drain(s, _):
        act_copy(s).wait()
        for kind in KINDS:
            for side in BOTH:
                hop(s, wide, kind, side).wait_send()
        return 0

    lax.fori_loop(1, steps + 1, drain, 0)
    for out in outs:
        out.wait()


def project(x_blk, gamma_blk, wq, wk, wv, wg, wu, lens, head_dim, ty_size, seq_block, d_model, tile):
    rows_all, kblk = x_blk.shape
    half_ty, group = ty_size // TWO, TWO * seq_block
    rows = half_ty * group
    q_width, ffn = wq.shape[1], wg.shape[1]
    kv_width = wk.shape[1]
    steps = ffn // tile
    wide = 2 * tile
    kdim = 2 * kblk
    x_main = x_blk.reshape(TWO, half_ty, RING, group, kblk)
    x_kv = x_blk.reshape(ty_size, RING, group, kblk)
    pieces = RING + 4 + 2 * steps
    stat_lines = 2 * (-(-((RING * half_ty + RING) // TWO) // 8) * 8)
    any_spec = pl.BlockSpec(memory_space=pl.ANY)
    vmem_spec = pl.BlockSpec(memory_space=pltpu.VMEM)
    return pl.pallas_call(
        functools.partial(project_kernel, ty_size, tile, d_model),
        out_shape=(
            jax.ShapeDtypeStruct((rows, ffn), BF16),
            jax.ShapeDtypeStruct((ty_size, seq_block, q_width), BF16),
            jax.ShapeDtypeStruct((TWO, group, kv_width), BF16),
        ),
        in_specs=[any_spec] * 8 + [vmem_spec] * 2,
        out_specs=(any_spec,) * 3,
        scratch_shapes=[
            pltpu.VMEM((TWO * LANES, LANES), F32),
            pltpu.VMEM((RING * half_ty + RING, group, kdim), BF16),
            pltpu.VMEM((steps + 1, kdim, wide), BF16),
            pltpu.VMEM((kdim, kv_width), BF16),
            pltpu.VMEM((CORES, kblk // LANES, LANES), F32),
            pltpu.VMEM((stat_lines, LANES), F32),
            pltpu.VMEM((3, stat_lines, LANES), F32),
            pltpu.VMEM((steps + 1, rows, wide), BF16),
            pltpu.VMEM((steps + 1, TWO, rows // TWO, wide), BF16),
            pltpu.VMEM((steps + 1, TWO, rows // TWO, wide), BF16),
            pltpu.VMEM((steps + 1, TWO, rows // TWO, wide), BF16),
            pltpu.VMEM((steps + 1, TWO, TWO, rows // TWO, wide), BF16),
            pltpu.VMEM((rows, ffn), BF16),
            pltpu.VMEM((RING, group, kv_width), F32),
            pltpu.VMEM((3, group, kv_width), F32),
            pltpu.VMEM((TWO, group, kv_width), BF16),
            pltpu.VMEM((ty_size, seq_block, q_width), BF16),
            pltpu.VMEM((ty_size, seq_block, q_width), BF16),
            pltpu.SemaphoreType.DMA((pieces,)),
            pltpu.SemaphoreType.DMA((pieces,)),
            pltpu.SemaphoreType.DMA((pieces,)),
            pltpu.SemaphoreType.DMA((len(KINDS),)),
            pltpu.SemaphoreType.DMA((len(KINDS),)),
            pltpu.SemaphoreType.DMA((steps + 1, len(KINDS), TWO)),
            pltpu.SemaphoreType.DMA((steps + 1, len(KINDS), TWO)),
            pltpu.SemaphoreType.DMA((len(KINDS),)),
            pltpu.SemaphoreType.DMA((len(KINDS),)),
            pltpu.SemaphoreType.DMA((TWO,)),
            pltpu.SemaphoreType.DMA((ty_size,)),
            pltpu.SemaphoreType.DMA((ty_size,)),
            pltpu.SemaphoreType.DMA((steps + 1,)),
            pltpu.SemaphoreType.DMA((TWO,)),
        ],
        compiler_params=pltpu.CompilerParams(
            collective_id=0, has_side_effects=True, vmem_limit_bytes=56 * MIB
        ),
        name="project",
    )(
        x_main, x_kv, wq, wk, wv, wg, wu, gamma_blk.reshape(-1, LANES), lens.reshape(-1, LANES), inverse_freqs(head_dim)
    )


def combine_kernel(
    ty_size,
    q_in, kv_in, k_in, v_in, act_in, x_in, wo, wd, lens,
    y_out,
    kvn, kv_f32, kc, vc, q_raw, q_f32, o_f32, att_out, att, mlp, wos, wds, yp, t1, xr, yf, p2_1, sd_1, sb_1, ra_1, rb_1, p2_2, sd_2, sb_2, ra_2, rb_2, ex,
    qkv_sem, w_sem, wp_send, wp_recv, a2a_send, a2a_recv, mlp_sem, gx_send, gx_recv, x_sem, xp_send, xp_recv,
    rs_send, rs_recv, ag_send, ag_recv, out_sem, outp_send, outp_recv,
):
    row_idx = lax.axis_index("ty")
    col_idx = lax.axis_index("tx")
    ring_pos, core = col_idx // 2, col_idx % 2
    other = 1 - core
    half_ty = ty_size // 2
    chunks = len(SIZES)
    begin = [sum(SIZES[:r]) for r in range(chunks)]
    seq_block = q_in.shape[1]
    group = 2 * seq_block
    cols = wo.shape[1]
    hcols = cols // 2
    pos_p, pos_m = (ring_pos + 1) % RING, (ring_pos + RING - 1) % RING
    tx_side = (pos_p * 2 + core, pos_m * 2 + core)
    from_side = (pos_m, pos_p)
    tx_pair = ring_pos * 2 + other
    z_pos, y_pos = row_idx // RING, row_idx % RING
    up = lambda v: (v + 1) % RING
    down = lambda v: (v + RING - 1) % RING
    y_side = (z_pos * RING + up(y_pos), z_pos * RING + down(y_pos))
    z_side = (up(z_pos) * RING + y_pos, down(z_pos) * RING + y_pos)
    places = ((y_pos, z_pos), (z_pos, y_pos))
    sides = ((y_side, z_side), (z_side, y_side))
    exchange = [size == 1 for size in SIZES]
    mine = pl.ds(pl.multiple_of(core * cols, LANES), cols)

    def units(r):
        return pl.ds(begin[r] * 2 * RING, SIZES[r] * 2 * RING)

    def block_units(r, b):
        return pl.ds(begin[r] * 2 * RING + b * 2 * SIZES[r], 2 * SIZES[r])

    def unit(r, b1, b2):
        return begin[r] * 2 * RING + b1 * 2 * SIZES[r] + b2

    def x_tile(c, r):
        b1, b2 = jnp.where(core == 0, y_pos, z_pos), jnp.where(core == 0, z_pos, y_pos)
        return x_in.at[c, block_units(r, b1) if exchange[r] else pl.ds(unit(r, b1, b2), 1)]

    def x_slot(c, r):
        return xr.at[c, r, pl.ds(0, 2 * SIZES[r] if exchange[r] else 1)]

    def own(r):
        return pl.ds(begin[r], SIZES[r])

    w_loads = [pltpu.make_async_copy(wd, wds.at[:, mine], w_sem.at[0]), pltpu.make_async_copy(wo, wos.at[:, mine], w_sem.at[1])]
    w_swaps = [
        remote(wd, wds.at[:, mine], wp_send.at[0], wp_recv.at[0], row_idx, tx_pair),
        remote(wo, wos.at[:, mine], wp_send.at[1], wp_recv.at[1], row_idx, tx_pair),
    ]
    mlp_loads = [pltpu.make_async_copy(act_in.at[own(r)], mlp.at[own(r), ring_pos], mlp_sem.at[r]) for r in range(chunks)]
    x_loads = [pltpu.make_async_copy(x_tile(core, r), x_slot(core, r), x_sem.at[r]) for r in range(chunks)]
    x_swaps = [remote(x_tile(other, r), x_slot(core, r), xp_send.at[r], xp_recv.at[r], row_idx, tx_pair) for r in range(chunks)]
    qkv_loads = [
        pltpu.make_async_copy(src, dst, qkv_sem.at[n])
        for n, (src, dst) in enumerate(((q_in, q_raw), (kv_in, kvn), (k_in, kc), (v_in, vc)))
    ]
    for load in qkv_loads + w_loads + mlp_loads + x_loads:
        load.start()

    barrier = pltpu.get_barrier_semaphore()
    pl.semaphore_signal(barrier, device_id={"ty": row_idx, "tx": tx_pair}, device_id_type=MESH)
    for tx in tx_side:
        pl.semaphore_signal(barrier, device_id={"ty": row_idx, "tx": tx}, device_id_type=MESH)
    for off in range(1, ty_size):
        for cc in BOTH:
            pl.semaphore_signal(
                barrier, device_id={"ty": (row_idx + off) % ty_size, "tx": ring_pos * 2 + cc}, device_id_type=MESH
            )
    pl.semaphore_wait(barrier, 3 + 2 * (ty_size - 1))

    def gather(r, part, stage, side):
        sems = gx_send.at[r, part, stage, side], gx_recv.at[r, part, stage, side]
        buf = (mlp, att)[part]
        if stage == 0:
            src = act_in.at[own(r)] if part == 0 else att.at[own(r), ring_pos]
            return remote(src, buf.at[own(r), ring_pos], *sems, row_idx, tx_side[side])
        if part == 0:
            lanes = mlp.shape[-1] // 2
            block = mlp.at[own(r), from_side[side], :, pl.ds(side * lanes, lanes)]
        else:
            block = att.at[own(r), from_side[side], side]
        return remote(block, block, *sems, row_idx, tx_side[side])

    home, home_core = row_idx % half_ty, row_idx // half_ty

    def a2a(k):
        return remote(
            att_out.at[k], att.at[home, ring_pos, core], a2a_send.at[k], a2a_recv.at[home, core],
            k, ring_pos * 2 + home_core,
        )

    def a2a_self(k):
        return jnp.logical_and(k == row_idx, core == home_core)

    def attend(_):
        heads, lines, head_dim = q_f32.shape
        for load in qkv_loads:
            load.wait()
        for k in range(ty_size):
            for h in range(heads):
                lanes = slice(h * head_dim, (h + 1) * head_dim)
                q_f32[h, k * seq_block : (k + 1) * seq_block, :] = q_raw[k, :, lanes].astype(F32)
        kv_f32[...] = kvn[...].astype(F32)
        slots = lax.broadcasted_iota(jnp.int32, (heads * ty_size, kc.shape[1]), 1)

        def sequence(b, _):
            picked = pl.ds(b, ty_size, stride=seq_block)
            fresh = pl.ds(core * seq_block + b, 1)
            length = lens[(row_idx * TWO * RING + col_idx) * seq_block + b]
            keys = updated(kc[b], kv_f32[0, fresh, :], length)
            vals = updated(vc[b], kv_f32[1, fresh, :], length)
            queries = jnp.concatenate([q_f32[h, picked, :] for h in range(heads)]).astype(BF16)
            scores = lax.dot_general(
                queries, keys, (((1,), (1,)), ((), ())), preferred_element_type=F32
            ) * (head_dim**-0.5)
            scores = jnp.where(slots <= length, scores, -1e30)
            weights = jnp.exp(scores - jnp.max(scores, axis=1, keepdims=True))
            probs = (weights / jnp.sum(weights, axis=1, keepdims=True)).astype(BF16)
            mixed = jnp.dot(probs, vals, preferred_element_type=F32)
            for h in range(heads):
                o_f32[h, picked, :] = mixed[h * ty_size : (h + 1) * ty_size]
            return 0

        lax.fori_loop(0, seq_block, sequence, 0, unroll=8)
        for k in range(ty_size):
            for h in range(heads):
                lanes = slice(h * head_dim, (h + 1) * head_dim)
                att_out[k, :, lanes] = o_f32[h, k * seq_block : (k + 1) * seq_block, :].astype(BF16)
        for k in range(ty_size):
            @pl.when(a2a_self(k))
            def _():
                pltpu.make_async_copy(
                    att_out.at[k], att.at[home, ring_pos, core], a2a_recv.at[home, core]
                ).start()

            @pl.when(jnp.logical_not(a2a_self(k)))
            def _():
                a2a(k).start()

    for swap in w_swaps + x_swaps:
        swap.start()

    def att_ready(r):
        for g in range(begin[r], begin[r] + SIZES[r]):
            for cc in BOTH:
                remote(
                    att_out.at[0], att.at[g, ring_pos, cc], a2a_send.at[0], a2a_recv.at[g, cc], row_idx, tx_pair
                ).wait_recv()

    def own_att(r):
        att_ready(r)
        for side in BOTH:
            gather(r, 1, 0, side).start()

    def own_mlp(r):
        for side in BOTH:
            gather(r, 0, 0, side).start()

    def forward(part, r):
        for side in BOTH:
            gather(r, part, 0, side).wait_recv()
            gather(r, part, 1, side).start()

    def multiply(r):
        mlp_loads[r].wait()
        for part in BOTH:
            for side in BOTH:
                gather(r, part, 1, side).wait_recv()
        rows = SIZES[r] * RING * group

        def tile(n, _):
            lanes = pl.ds(pl.multiple_of(n * TILE, TILE), TILE)
            left_mlp = mlp[own(r)].reshape(rows, mlp.shape[-1])
            left_att = att[own(r)].reshape(rows, att.shape[-1])
            yp[pl.ds(begin[r] * RING * group, rows), lanes] = jnp.dot(
                left_mlp, wds[:, lanes], preferred_element_type=F32
            ) + jnp.dot(left_att, wos[:, lanes], preferred_element_type=F32)
            return 0

        lax.fori_loop(0, yp.shape[1] // TILE, tile, 0)

    bufs = ((p2_1, sd_1, sb_1, ra_1, rb_1), (p2_2, sd_2, sb_2, ra_2, rb_2))

    def block_rows(level, r):
        return (SIZES[r] * group, seq_block)[level]

    def hop(level, r, c, kind, side):
        p2, sd, sb, ra, rb = bufs[level]
        m = pl.ds(0, block_rows(level, r))
        src, dst = (
            (p2.at[r, c, m, pl.ds(side * hcols, hcols)], ra.at[r, c, side, m]),
            (sd.at[r, c, side, m], rb.at[r, c, side, 0, m]),
            (sb.at[r, c, side, m], rb.at[r, c, side, 1, m]),
        )[kind]
        return remote(
            src, dst, rs_send.at[level, r, c, kind, side], rs_recv.at[level, r, c, kind, side],
            sides[c][level][side], col_idx,
        )

    def part_of(level, r, c, b, half):
        size = block_rows(level, r)
        if level == 0:
            rows = pl.ds(pl.multiple_of(begin[r] * RING * group + b * size, 8), size)
            return yp[rows, c * cols + half * hcols : c * cols + (half + 1) * hcols]
        return t1[r, c, pl.ds(pl.multiple_of(b * size, 8), size), half * hcols : (half + 1) * hcols]

    def reduce_a(level, r):
        p2, sd = bufs[level][:2]
        m = block_rows(level, r)
        for c in BOTH:
            pos = places[c][level]
            for half in BOTH:
                p2[r, c, :m, half * hcols : (half + 1) * hcols] = part_of(level, r, c, (pos + 2) % RING, half).astype(BF16)
                hop(level, r, c, 0, half).start()
        for c in BOTH:
            pos = places[c][level]
            for side, b in enumerate((up(pos), down(pos))):
                sd[r, c, side, :m] = part_of(level, r, c, b, 1 - side).astype(BF16)
                hop(level, r, c, 1, side).start()

    def reduce_b(level, r):
        sb, ra = bufs[level][2:4]
        m = block_rows(level, r)
        for c in BOTH:
            pos = places[c][level]
            for side, b in enumerate((up(pos), down(pos))):
                hop(level, r, c, 0, side).wait_recv()
                sb[r, c, side, :m] = (part_of(level, r, c, b, side) + ra[r, c, side, :m].astype(F32)).astype(BF16)
                hop(level, r, c, 2, side).start()

    def reduce_c(level, r, finish):
        rb = bufs[level][4]
        m = block_rows(level, r)
        for c in BOTH:
            pos = places[c][level]
            for half in BOTH:
                hop(level, r, c, 1, 1 - half).wait_recv()
                hop(level, r, c, 2, half).wait_recv()
                finish(
                    c, half,
                    part_of(level, r, c, pos, half)
                    + rb[r, c, half, 1, :m].astype(F32) + rb[r, c, 1 - half, 0, :m].astype(F32),
                )

    def spread(level, r, c, stage, side):
        ring, (p1, p2) = sides[c][level], places[c]
        sems = ag_send.at[level, r, c, stage, side], ag_recv.at[level, r, c, stage, side]
        near = (down, up)[side]
        half = pl.ds(side * hcols, hcols)
        if level == 1 and exchange[r]:
            m = pl.ds(0, block_rows(0, r))
            block = ex.at[r, c, p2, m] if stage == 0 else ex.at[r, c, near(p2), m, half]
        elif level == 1:
            block = yf.at[c, unit(r, p1, p2)] if stage == 0 else yf.at[c, unit(r, p1, near(p2)), :, half]
        elif stage == 0:
            block = yf.at[c, block_units(r, p1)]
        else:
            block = yf.at[c, pl.ds(unit(r, near(p1), side * SIZES[r]), SIZES[r])]
        return remote(block, block, *sems, ring[side], col_idx)

    def spread_own(level, r):
        for c in BOTH:
            for side in BOTH:
                spread(level, r, c, 0, side).start()

    def spread_on(level, r):
        for c in BOTH:
            for side in BOTH:
                spread(level, r, c, 0, side).wait_recv()
                spread(level, r, c, 1, side).start()

    def spread_end(level, r):
        for c in BOTH:
            for side in BOTH:
                spread(level, r, c, 1, side).wait_recv()

    def s3(r):
        reduce_b(0, r)

    def s4(r):
        m = block_rows(0, r)

        def finish(c, half, vals):
            lanes = slice(half * hcols, (half + 1) * hcols)
            if exchange[r]:
                ex[r, c, places[c][1], :m, lanes] = vals.astype(BF16)
            else:
                t1[r, c, :m, lanes] = vals
        reduce_c(0, r, finish)
        if exchange[r]:
            spread_own(1, r)
        else:
            reduce_a(1, r)

    def s5(r):
        if exchange[r]:
            spread_on(1, r)
        else:
            reduce_b(1, r)

    def s6(r):
        x_loads[r].wait()
        remote(x_tile(other, r), x_slot(other, r), xp_send.at[r], xp_recv.at[r], row_idx, tx_pair).wait_recv()
        if exchange[r]:
            m = block_rows(0, r)
            spread_end(1, r)
            for c in BOTH:
                for n in range(2 * SIZES[r]):
                    rows = slice(n * seq_block, (n + 1) * seq_block)
                    first, second, third, fourth = (ex[r, c, p, rows].astype(F32) for p in range(RING))
                    total = (first + second) + (third + fourth)
                    yf[c, unit(r, places[c][0], n)] = (xr[c, r, n].astype(F32) + total).astype(BF16)
            spread_own(0, r)
        else:
            def finish(c, half, vals):
                lanes = slice(half * hcols, (half + 1) * hcols)
                yf[c, unit(r, *places[c]), :, lanes] = (xr[c, r, 0, :, lanes].astype(F32) + vals).astype(BF16)
            reduce_c(1, r, finish)
            spread_own(1, r)

    def s7(r):
        spread_on(1, r)

    def s8(r):
        spread_end(1, r)
        spread_own(0, r)

    def s9(r):
        spread_on(0, r)

    def out_copy(r):
        return pltpu.make_async_copy(yf.at[core, units(r)], y_out.at[core, units(r)], out_sem.at[r])

    def out_swap(r):
        return remote(
            yf.at[other, units(r)], y_out.at[core, units(r)], outp_send.at[r], outp_recv.at[r], row_idx, tx_pair
        )

    def s10(r):
        spread_end(0, r)
        out_swap(r).start()
        out_copy(r).start()

    def s2(r):
        multiply(r)
        reduce_a(0, r)

    stages = dict(zip("mAagh23456789t", (
        own_mlp, attend, own_att, functools.partial(forward, 0), functools.partial(forward, 1),
        s2, s3, s4, s5, s6, s7, s8, s9, s10,
    )))
    products = ORDER[::TWO].index("2") * TWO
    for n in range(0, len(ORDER), TWO):
        if n == products:
            for load, swap in zip(w_loads, w_swaps):
                load.wait()
                swap.wait_recv()
        stages[ORDER[n]](int(ORDER[n + 1]))

    for swap in w_swaps + x_swaps:
        swap.wait_send()
    for k in range(ty_size):
        @pl.when(jnp.logical_not(a2a_self(k)))
        def _():
            a2a(k).wait_send()
    for r in range(chunks):
        for a in BOTH:
            for b in BOTH:
                for side in BOTH:
                    gather(r, a, b, side).wait_send()
                    for level in BOTH:
                        spread(level, r, a, b, side).wait_send()
        for level in BOTH[: 2 - exchange[r]]:
            for c in BOTH:
                for kind in KINDS:
                    for side in BOTH:
                        hop(level, r, c, kind, side).wait_send()
        out_copy(r).wait()
        out_swap(r).wait()


def combine(q_owned, kv_new, k_blk, v_blk, lens_own, act_own, x_blk, w_out, w_down, ty_size):
    seq_block = q_owned.shape[1]
    head_dim = k_blk.shape[TWO]
    chunks, most = len(SIZES), max(SIZES)
    group, half_ty = TWO * seq_block, ty_size // TWO
    cols = w_out.shape[1]
    hcols = cols // TWO
    ffn, q_width = w_down.shape[0], w_out.shape[0]
    any_spec = pl.BlockSpec(memory_space=pl.ANY)
    ring_bufs = []
    for m in (most * group, seq_block):
        half = (chunks, TWO, TWO, m, hcols)
        both = (chunks, TWO, TWO, TWO, m, hcols)
        ring_bufs += [pltpu.VMEM(shape, BF16) for shape in ((chunks, TWO, m, cols), half, half, half, both)]
    dma = pltpu.SemaphoreType.DMA
    y_units = (TWO, half_ty * RING * TWO, seq_block, cols)
    y = pl.pallas_call(
        functools.partial(combine_kernel, ty_size),
        out_shape=jax.ShapeDtypeStruct(y_units, BF16),
        in_specs=[any_spec] * 8 + [pl.BlockSpec(memory_space=pltpu.SMEM)],
        out_specs=any_spec,
        scratch_shapes=[
            pltpu.VMEM(kv_new.shape, BF16),
            pltpu.VMEM(kv_new.shape, F32),
            pltpu.VMEM(k_blk.shape, BF16),
            pltpu.VMEM(v_blk.shape, BF16),
            pltpu.VMEM(q_owned.shape, BF16),
            pltpu.VMEM((q_width // head_dim, ty_size * seq_block, head_dim), F32),
            pltpu.VMEM((q_width // head_dim, ty_size * seq_block, head_dim), F32),
            pltpu.VMEM(q_owned.shape, BF16),
            pltpu.VMEM((half_ty, RING, TWO, seq_block, q_width), BF16),
            pltpu.VMEM((half_ty, RING, group, ffn), BF16),
            pltpu.VMEM((q_width, TWO * cols), BF16),
            pltpu.VMEM((ffn, TWO * cols), BF16),
            pltpu.VMEM((half_ty * RING * group, TWO * cols), F32),
            pltpu.VMEM((chunks, TWO, most * group, cols), F32),
            pltpu.VMEM((TWO, chunks, TWO * most, seq_block, cols), BF16),
            pltpu.VMEM(y_units, BF16),
            *ring_bufs,
            pltpu.VMEM((chunks, TWO, RING, most * group, cols), BF16),
            dma((RING,)), dma((CORES,)), dma((CORES,)), dma((CORES,)),
            dma((ty_size,)), dma((half_ty, TWO)),
            dma((chunks,)),
            dma((chunks, TWO, TWO, TWO)), dma((chunks, TWO, TWO, TWO)),
            dma((chunks,)), dma((chunks,)), dma((chunks,)),
            dma((TWO, chunks, TWO, len(KINDS), TWO)), dma((TWO, chunks, TWO, len(KINDS), TWO)),
            dma((TWO, chunks, TWO, TWO, TWO)), dma((TWO, chunks, TWO, TWO, TWO)),
            dma((chunks,)), dma((chunks,)), dma((chunks,)),
        ],
        compiler_params=pltpu.CompilerParams(
            collective_id=1, has_side_effects=True, vmem_limit_bytes=60 * MIB
        ),
        name="combine",
    )(q_owned, kv_new, k_blk, v_blk, act_own.reshape(half_ty, group, ffn), x_blk.reshape(y_units), w_out, w_down, lens_own)
    return y.reshape(x_blk.shape)


def emit_kernel(pieces, y_in, kv_in, k_in, v_in, lens, y_out, k_out, v_out, ys, kvn, kv_f32, kc, vc, load_sem, y_sem, out_sem, y_out_sem):
    core = lax.axis_index("tx") % CORES
    seq_block = kc.shape[0]
    size = ys.shape[0] // pieces
    base = (lax.axis_index("ty") * TWO * RING + lax.axis_index("tx")) * seq_block
    loads = [
        pltpu.make_async_copy(src, dst, load_sem.at[n]) for n, (src, dst) in enumerate(((kv_in, kvn), (k_in, kc), (v_in, vc)))
    ]
    part = [pl.ds(n * size, size) for n in range(pieces)]
    y_loads = [pltpu.make_async_copy(y_in.at[p], ys.at[p], y_sem.at[n]) for n, p in enumerate(part)]
    y_stores = [pltpu.make_async_copy(ys.at[p], y_out.at[p], y_out_sem.at[n]) for n, p in enumerate(part)]
    stores = [pltpu.make_async_copy(kc, k_out, out_sem.at[0]), pltpu.make_async_copy(vc, v_out, out_sem.at[1])]
    for load in y_loads + loads:
        load.start()
    for load, store in zip(y_loads, y_stores):
        load.wait()
        store.start()
    for load in loads:
        load.wait()
    kv_f32[...] = kvn[...].astype(F32)

    def sequence(b, _):
        fresh = pl.ds(core * seq_block + b, 1)
        length = lens[base + b]
        kc[b] = updated(kc[b], kv_f32[0, fresh, :], length)
        vc[b] = updated(vc[b], kv_f32[1, fresh, :], length)
        return 0

    lax.fori_loop(0, seq_block, sequence, 0, unroll=4)
    for store in stores:
        store.start()
    for store in y_stores + stores:
        store.wait()


def emit(y, kv_new, k_blk, v_blk, lens_own):
    pieces = 8
    any_spec = pl.BlockSpec(memory_space=pl.ANY)
    dma = pltpu.SemaphoreType.DMA
    return pl.pallas_call(
        functools.partial(emit_kernel, pieces),
        out_shape=tuple(jax.ShapeDtypeStruct(a.shape, BF16) for a in (y, k_blk, v_blk)),
        in_specs=[any_spec] * RING + [pl.BlockSpec(memory_space=pltpu.SMEM)],
        out_specs=(any_spec,) * len(KINDS),
        scratch_shapes=[
            pltpu.VMEM(y.shape, BF16),
            pltpu.VMEM(kv_new.shape, BF16),
            pltpu.VMEM(kv_new.shape, F32),
            pltpu.VMEM(k_blk.shape, BF16),
            pltpu.VMEM(v_blk.shape, BF16),
            dma((len(KINDS),)), dma((pieces,)), dma((TWO,)), dma((pieces,)),
        ],
        compiler_params=pltpu.CompilerParams(vmem_limit_bytes=60 * MIB),
        name="emit",
    )(y, kv_new, k_blk, v_blk, lens_own)


def solution(mesh):
    ty_size = mesh.shape["ty"]
    tx_size = mesh.shape["tx"]
    cache_spec = P(("dp", "ty", "tx"), None, None)

    def layer_shard(x_blk, lens_part, k_blk, v_blk, gamma_blk, w_query, w_key, w_value, w_gate, w_up, w_out, w_down):
        rows = x_blk.shape[0]
        d_model = x_blk.shape[1] * tx_size
        seq_block, _, head_dim = k_blk.shape
        tile = min(256, w_gate.shape[1])

        act_own, q_owned, kv_new = project(
            x_blk, gamma_blk, w_query, w_key, w_value, w_gate, w_up, lens_part, head_dim,
            ty_size, seq_block, d_model, tile,
        )
        y_raw = combine(q_owned, kv_new, k_blk, v_blk, lens_part, act_own, x_blk, w_out, w_down, ty_size)
        y_blk, k_out, v_out = emit(y_raw, kv_new, k_blk, v_blk, lens_part)
        return y_blk, k_out, v_out

    in_specs = (P("dp", "tx"), P("dp"), cache_spec, cache_spec, P("tx"), P("tx", "ty"), P("tx", None), P("tx", None), P("tx", "ty"), P("tx", "ty"), P("ty", "tx"), P("ty", "tx"))
    out_specs = (P("dp", "tx"), cache_spec, cache_spec)
    return jax.shard_map(layer_shard, mesh=mesh, in_specs=in_specs, out_specs=out_specs, check_vma=False)
```
